32 devices in a mesh: dp: 8 (over z, y), seq: 4 (over x, core).
Axes of the slice: x: 2, y: 2, z: 4, core: 2. Of those that a mesh axis runs over, the one named last changes fastest.
Arguments:
- tokens: bfloat16 [3, 8, 2048, 768], P(None, 'dp', 'seq'), may hold values from -6 to 6
- norm_gain: float32 [768], P(('dp', 'seq')), may hold values from 0.1 to 1.9
- w_in: float32 [768, 3352], P(('dp', 'seq')), may hold values from -0.21875 to 0.21875
- conv_weight: float32 [4, 1792], P(None, ('dp', 'seq')), may hold values from -3 to 3
- conv_bias: float32 [1792], P(('dp', 'seq')), may hold values from -3 to 3
- dt_bias: float32 [24], replicated, may hold values from -3 to 0.5
- a_log: float32 [24], replicated, may hold values from -6 to 0
- d_skip: float32 [24], replicated, may hold values from -3 to 3
- gated_gain: float32 [1536], P(('dp', 'seq')), may hold values from 0.1 to 1.9
- w_out: float32 [1536, 768], P(('dp', 'seq')), may hold values from -0.15625 to 0.15625
- lengths: int32 [3, 8], P(None, 'dp'), may hold values from 1024 to 2048, as said below
- cotangent: bfloat16 [3, 8, 2048, 768], P(None, 'dp', 'seq'), may hold values from -6 to 6
Outputs:
- block_out: bfloat16 [3, 8, 2048, 768], P(None, 'dp', 'seq')
- tokens_grad: bfloat16 [3, 8, 2048, 768], P(None, 'dp', 'seq')
- norm_gain_grad: float32 [768], P(('dp', 'seq'))
- w_in_grad: float32 [768, 3352], P(('dp', 'seq'))
- conv_weight_grad: float32 [4, 1792], P(None, ('dp', 'seq'))
- conv_bias_grad: float32 [1792], P(('dp', 'seq'))
- dt_bias_grad: float32 [24], replicated
- a_log_grad: float32 [24], replicated
- d_skip_grad: float32 [24], replicated
- gated_gain_grad: float32 [1536], P(('dp', 'seq'))
- w_out_grad: float32 [1536, 768], P(('dp', 'seq'))
The draws below stay inside these ranges and needn't reach their ends.
Inputs may be any that keep to these rules, and one draw needn't show every extreme that they name: `lengths`: one sequence of the draw has length exactly 2048.
All inputs are finite; a program needn't handle non-finite values.
Results may differ from the reference program's by a relative error of at most 0.0085.
The reference program's roundings to bfloat16 on the way count: a program that leaves them out, or rounds other values in their place, can miss the bound.
Values may be sent and summed in bfloat16 or wider, within the bound.
A program may use at most 320 MiB of HBM per device.

```python
import jax
import jax.numpy as jnp
from jax import lax

D = 768
NH = 24
HD = 64
NS = 128
DCONV = 4
CH = 256
MB = 3
DI = 1536
XBC = 1792
PROJ = 3352
SEQ_LEN = 2048
SEQS = 8


def draw_lengths(key, part):
    first_key, second_key = jax.random.split(jax.random.fold_in(key, 11))
    values = jax.random.randint(first_key, (MB * SEQS,), SEQ_LEN // 2, SEQ_LEN + 1)
    longest = jax.random.randint(second_key, (), 0, MB * SEQS)
    values = values.at[longest].set(SEQ_LEN)
    return values.reshape(MB, SEQS).astype(jnp.int32)


def block_scale(rng, shape, cuts, least, top_value):
    loudness = 1.0
    for axis_at, blocks in cuts:
        draws = jax.random.uniform(jax.random.fold_in(jax.random.fold_in(rng, 6), axis_at), (blocks,), jnp.float32, least / len(cuts), top_value / len(cuts))
        loudness = loudness * jnp.repeat(jnp.exp(draws), shape[axis_at] // blocks).reshape((-1,) + (1,) * (len(shape) - 1 - axis_at))
    return loudness


def centred(stream_key, dims, width, reach, cuts=(), kind=jnp.bfloat16):
    drawn = width * jax.random.normal(stream_key, dims, jnp.float32)
    if cuts:
        drawn = drawn * block_scale(stream_key, dims, cuts, -0.22, 0.18)
    return jnp.clip(drawn, -reach, reach).astype(kind)


def setup_inputs(seed: int = 0) -> dict:
    key_list = jax.random.split(jax.random.key(seed), 13)
    tokens = centred(key_list[0], (MB, SEQS, SEQ_LEN, D), 1.0, 6.0, ((1, 8), (2, 4)))
    norm_gain = jnp.clip(1.0 + 0.18 * jax.random.normal(key_list[1], (D,), jnp.float32), 0.1, 1.9)
    w_in = centred(key_list[2], (D, PROJ), D ** -0.5, 0.21875, ((0, 32),), jnp.float32)
    conv_weight = centred(key_list[3], (DCONV, XBC), DCONV ** -0.5, 3.0, ((1, 32),), jnp.float32)
    conv_bias = centred(key_list[4], (XBC,), 0.5, 3.0, ((0, 32),), jnp.float32)
    dt_bias = jnp.clip(jax.random.uniform(key_list[5], (NH,), jnp.float32, -3.0, 0.5), -3.0, 0.5)
    a_log = jnp.clip(jax.random.uniform(key_list[6], (NH,), jnp.float32, -6.0, 0.0), -6.0, 0.0)
    d_skip = centred(key_list[7], (NH,), 1.0, 3.0, (), jnp.float32)
    gated_gain = jnp.clip(1.0 + 0.18 * jax.random.normal(key_list[8], (DI,), jnp.float32), 0.1, 1.9)
    w_out = centred(key_list[9], (DI, D), DI ** -0.5, 0.15625, ((0, 32),), jnp.float32)
    lengths = draw_lengths(jax.random.fold_in(key_list[12], 71), 0)
    cotangent = centred(key_list[11], (MB, SEQS, SEQ_LEN, D), 1.0, 6.0, ((1, 8), (2, 4)))
    return {"tokens": tokens, "norm_gain": norm_gain, "w_in": w_in, "conv_weight": conv_weight, "conv_bias": conv_bias, "dt_bias": dt_bias, "a_log": a_log, "d_skip": d_skip, "gated_gain": gated_gain, "w_out": w_out, "lengths": lengths, "cotangent": cotangent}


@jax.custom_vjp
def low(v):
    return lax.optimization_barrier(v.astype(jnp.bfloat16)).astype(jnp.float32)

@jax.custom_vjp
def low_back(v):
    return v

def low_keep(v):
    return (low(v), None)

def low_pass(kept, grad):
    return (grad,)

def back_keep(v):
    return (v, None)

def back_low(kept, grad):
    return (low(grad),)
low.defvjp(low_keep, low_pass)
low_back.defvjp(back_keep, back_low)
EPSILON = 1e-05
PRECISE = lax.Precision.HIGHEST

def rms_scale(values, scale_gain):
    return values * lax.rsqrt(lax.optimization_barrier(jnp.mean(values * values, axis=-1, keepdims=True)) + EPSILON) * scale_gain

def conv_silu(conv_input, conv_weight, conv_bias):
    row_count = conv_input.shape[0]
    padded = jnp.concatenate([jnp.zeros((DCONV - 1, conv_input.shape[1]), jnp.float32), conv_input], axis=0)
    running = conv_bias + jnp.zeros_like(conv_input)
    for tap_index in range(DCONV):
        running = running + padded[tap_index:tap_index + row_count] * conv_weight[tap_index]
    return jax.nn.silu(running)

def block_update(decay_rate, states, inputs_ssm, b_rows, c_rows, step_size):
    log_decay = jnp.cumsum(step_size * decay_rate, axis=0)
    causal = lax.broadcasted_iota(jnp.int32, (CH, CH), 0) >= lax.broadcasted_iota(jnp.int32, (CH, CH), 1)
    log_gaps = log_decay.T[:, :, None] - log_decay.T[:, None, :]
    weights = jnp.where(causal, jnp.exp(jnp.where(causal, log_gaps, 0.0)), 0.0)
    scores = jnp.dot(c_rows, b_rows.T, precision=PRECISE)
    mixing = weights * scores[None] * step_size.T[:, None, :]
    y_diag = jnp.einsum('hts,shp->thp', mixing, inputs_ssm, precision=PRECISE)
    y_off = jnp.einsum('tn,hpn->thp', c_rows, states, precision=PRECISE) * jnp.exp(log_decay)[:, :, None]
    tail_weight = jnp.exp(log_decay[-1][None, :] - log_decay) * step_size
    weighted = inputs_ssm * tail_weight[:, :, None]
    local_state = jnp.einsum('shp,sn->hpn', weighted, b_rows, precision=PRECISE)
    block_decay = jnp.exp(log_decay[-1])
    return (block_decay[:, None, None] * states + local_state, y_diag + y_off)

def sequence_forward(params, token_rows, validity):
    norm_gain, w_in, conv_weight, conv_bias, dt_bias, a_log, d_skip, gated_gain, w_out = params
    normed = low(rms_scale(token_rows, norm_gain))
    projected = low_back(jnp.dot(normed, low(w_in), precision=PRECISE))
    gate_part = projected[:, :DI]
    conv_input = projected[:, DI:DI + XBC]
    dt_raw = projected[:, DI + XBC:]
    activated = conv_silu(conv_input, conv_weight, conv_bias)
    inputs_ssm = activated[:, :DI].reshape(SEQ_LEN, NH, HD)
    b_rows = activated[:, DI:DI + NS]
    c_rows = activated[:, DI + NS:]
    step_size = jax.nn.softplus(dt_raw + dt_bias) * validity[:, None]
    decay_rate = -jnp.exp(a_log)

    def advance(states, block_data):
        return block_update(decay_rate, states, *block_data)
    block_total = SEQ_LEN // CH
    block_data = (inputs_ssm.reshape(block_total, CH, NH, HD), b_rows.reshape(block_total, CH, NS), c_rows.reshape(block_total, CH, NS), step_size.reshape(block_total, CH, NH))
    final_state, outputs = lax.scan(jax.checkpoint(advance), jnp.zeros((NH, HD, NS), jnp.float32), block_data)
    y_full = outputs.reshape(SEQ_LEN, NH, HD) + d_skip[:, None] * inputs_ssm
    gated_rows = y_full.reshape(SEQ_LEN, DI) * jax.nn.silu(gate_part)
    gated_norm = low(rms_scale(gated_rows, gated_gain))
    branch = low_back(jnp.dot(gated_norm, low(w_out), precision=PRECISE))
    return validity[:, None] * (token_rows + branch)

def reference(tokens, norm_gain, w_in, conv_weight, conv_bias, dt_bias, a_log, d_skip, gated_gain, w_out, lengths, cotangent):
    params = (norm_gain, w_in, conv_weight, conv_bias, dt_bias, a_log, d_skip, gated_gain, w_out)
    positions = jnp.arange(SEQ_LEN, dtype=jnp.int32)
    flat_tokens = tokens.reshape(MB * SEQS, SEQ_LEN, D)
    flat_cot = cotangent.reshape(MB * SEQS, SEQ_LEN, D)
    flat_len = lengths.reshape(MB * SEQS).astype(jnp.int32)

    def per_sequence(gradients, sequence_item):
        token_seq, cot_seq, length = sequence_item
        validity = (positions < length).astype(jnp.float32)

        def forward(param_set, token_rows):
            return sequence_forward(param_set, token_rows, validity)
        result, pullback = jax.vjp(forward, params, token_seq.astype(jnp.float32))
        param_grads, token_grads = pullback(cot_seq.astype(jnp.float32))
        gradients = jax.tree.map(jnp.add, gradients, param_grads)
        return (gradients, (result.astype(jnp.bfloat16), token_grads.astype(jnp.bfloat16)))
    zero_grads = jax.tree.map(jnp.zeros_like, params)
    gradients, (results, token_grads) = lax.scan(per_sequence, zero_grads, (flat_tokens, flat_cot, flat_len))
    return (results.reshape(tokens.shape), token_grads.reshape(tokens.shape), gradients[0], gradients[1], gradients[2], gradients[3], gradients[4], gradients[5], gradients[6], gradients[7], gradients[8])
```

```python
from functools import partial

import jax
import jax.numpy as jnp
from jax import lax
from jax.experimental import pallas as pl
from jax.experimental.pallas import tpu as pltpu
from jax.sharding import PartitionSpec as P

D = 768
NH = 24
HD = 64
NS = 128
DCONV = 4
CL = 128
DI = 1536
XBC = 1792
PROJ = 3352
XD = 1920
LN = 128
EPSILON = 1e-05

F32 = jnp.float32
BF = jnp.bfloat16
SROWS = 144


def nn(a, b):
    return lax.dot_general(a, b, (((1,), (0,)), ((), ())), preferred_element_type=F32)


def nt(a, b):
    return lax.dot_general(a, b, (((1,), (1,)), ((), ())), preferred_element_type=F32)


def tn(a, b):
    return lax.dot_general(a, b, (((0,), (0,)), ((), ())), preferred_element_type=F32)


def exact_nn(a, b):
    return lax.dot_general(
        a, b, (((1,), (0,)), ((), ())), precision=lax.Precision.HIGHEST, preferred_element_type=F32
    )


def sigmoid(v):
    return 0.5 * jnp.tanh(0.5 * v) + 0.5


def halves(v):
    top = v.astype(BF)
    return top, (v - top.astype(F32)).astype(BF)


def three(op, a, b):
    ah, al = halves(a)
    bh, bl = halves(b)
    return op(ah, bh) + op(al, bh) + op(ah, bl)


def expander():
    head = lax.broadcasted_iota(jnp.int32, (LN, DI), 0)
    lane = lax.broadcasted_iota(jnp.int32, (LN, DI), 1)
    return jnp.where(head == lane // HD, 1.0, 0.0).astype(BF)


def expand(v, e):
    top, low = halves(v)
    return nn(top, e) + nn(low, e)


def lower_mask(strict):
    row = lax.broadcasted_iota(jnp.int32, (CL, CL), 0)
    col = lax.broadcasted_iota(jnp.int32, (CL, CL), 1)
    return row > col if strict else row >= col


def half_masks():
    lane = lax.broadcasted_iota(jnp.int32, (1, 2 * HD), 1)
    left = jnp.where(lane < HD, 1.0, 0.0).astype(BF)
    right = jnp.where(lane < HD, 0.0, 1.0).astype(BF)
    return left, right


def lanes(j):
    return slice(j * LN, (j + 1) * LN)


def conv_running(ext, cw, cb):
    total = cb
    for tap in range(DCONV):
        total = total + ext[5 + tap : 5 + tap + CL] * cw[tap : tap + 1]
    return total


def project_kernel(
    vlen_ref,
    x_ref,
    xh_ref,
    g_ref,
    w_ref,
    cw_ref,
    cb_ref,
    dtb_ref,
    rate_ref,
    nrm_ref,
    ci_ref,
    act_ref,
    step_ref,
    l_ref,
    sig_ref,
    sloc_ref,
    s_ref,
    nx,
    xw,
    state,
    *,
    first,
):
    piece = x_ref.shape[0]
    chunks = piece // CL
    valid = vlen_ref[first + pl.program_id(0)]

    def norm(v):
        v = v.astype(F32)
        r = lax.rsqrt(jnp.mean(v * v, axis=-1, keepdims=True) + EPSILON)
        return (v * r * g_ref[...]).astype(BF)

    nx[0:16] = norm(xh_ref[...])

    def norm_rows(i, c):
        rows = pl.ds(pl.multiple_of(i * 64, 64), 64)
        v = norm(x_ref[rows, :])
        nx[pl.ds(pl.multiple_of(i * 64 + 16, 16), 64), :] = v
        nrm_ref[rows, :] = v
        return c

    lax.fori_loop(0, piece // 64, norm_rows, 0)

    for j in range(XBC // 256):
        cols = slice(j * 256, (j + 1) * 256)
        ci_ref[:, cols] = nn(nx[...], w_ref[:, cols])[8:]
    dt_raw = nn(nx[16:], w_ref[:, XBC:]) + dtb_ref[...]
    row = lax.broadcasted_iota(jnp.int32, (piece, LN), 0)
    mask = jnp.where(row < valid, 1.0, 0.0)
    step_ref[...] = (jnp.maximum(dt_raw, 0.0) + jnp.log1p(jnp.exp(-jnp.abs(dt_raw)))) * mask
    sig_ref[...] = mask / (1.0 + jnp.exp(-dt_raw))

    e = expander()
    tri = jnp.where(lower_mask(False), 1.0, 0.0)
    state[...] = jnp.zeros_like(state)

    def chunk(k, total):
        base = pl.multiple_of(k * CL, CL)
        rows = pl.ds(base, CL)
        step = step_ref[rows, :]
        ld = exact_nn(tri, step * rate_ref[...])
        l_ref[rows, :] = ld
        end = ld[CL - 1 :]
        tail = expand(step * jnp.exp(end - ld), e)
        for j in range(XBC // LN):
            ext = ci_ref[pl.ds(base, CL + 8), lanes(j)]
            run = conv_running(ext, cw_ref[:, lanes(j)], cb_ref[:, lanes(j)])
            act = run * sigmoid(run)
            act_ref[rows, lanes(j)] = act
            if j < DI // LN:
                xw[:, lanes(j)] = (act * tail[:, lanes(j)]).astype(BF)
        b = act_ref[rows, DI : DI + NS].astype(BF)
        sloc_ref[k] = state[...].astype(BF)
        keep = expand(jnp.exp(jnp.broadcast_to(end, (8, LN))), e)[0:1]
        state[...] = keep * state[...] + tn(b, xw[...])
        return total + end

    total = lax.fori_loop(0, chunks, chunk, jnp.zeros((1, LN), F32))
    s_ref[0:NS] = state[...].astype(BF)
    keep = expand(jnp.exp(jnp.broadcast_to(total, (8, LN))), e)[0:1]
    top, low = halves(keep)
    s_ref[NS : NS + 16] = jnp.concatenate([top, low, jnp.zeros((14, DI), BF)], axis=0)


def whole(shape):
    return pl.BlockSpec(shape, lambda i: (0,) * len(shape))


def kept(shape):
    return pl.BlockSpec(shape, lambda i: (0,) * len(shape), pipeline_mode=pl.Buffered(1))


def per(shape, first=0, **mode):
    rest = (0,) * len(shape)
    return pl.BlockSpec((None,) + shape, lambda i: (first + i,) + rest, **mode)


ONE = dict(pipeline_mode=pl.Buffered(1))


SMEM = pl.BlockSpec(memory_space=pltpu.SMEM)
LIMIT = 67_000_000


def project(first, count, valid, tokens, halo, gain, w_xd, cw, cb, dtb, rate):
    piece = tokens.shape[1]
    chunks = piece // CL
    sds = jax.ShapeDtypeStruct
    return pl.pallas_call(
        partial(project_kernel, first=first),
        grid=(count,),
        in_specs=[
            SMEM,
            per((piece, D), first),
            per((16, D), first),
            whole((1, D)),
            kept((D, XD)),
            whole((DCONV, XBC)),
            whole((1, XBC)),
            whole((1, LN)),
            whole((1, LN)),
        ],
        out_specs=[
            per((piece, D)),
            per((piece + 8, XBC)),
            per((piece, XBC)),
            per((piece, LN)),
            per((piece, LN)),
            per((piece, LN)),
            per((chunks, NS, DI)),
            per((SROWS, DI)),
        ],
        out_shape=[
            sds((count, piece, D), BF),
            sds((count, piece + 8, XBC), F32),
            sds((count, piece, XBC), F32),
            sds((count, piece, LN), F32),
            sds((count, piece, LN), F32),
            sds((count, piece, LN), F32),
            sds((count, chunks, NS, DI), BF),
            sds((count, SROWS, DI), BF),
        ],
        scratch_shapes=[
            pltpu.VMEM((piece + 16, D), BF),
            pltpu.VMEM((CL, DI), BF),
            pltpu.VMEM((NS, DI), F32),
        ],
        compiler_params=pltpu.CompilerParams(vmem_limit_bytes=LIMIT),
        name="project",
    )(valid, tokens, halo, gain, w_xd, cw, cb, dtb, rate)


def mix_kernel(
    vlen_ref,
    place_ref,
    x_ref,
    cot_ref,
    nrm_ref,
    act_ref,
    step_ref,
    l_ref,
    sloc_ref,
    sg_ref,
    wz_ref,
    wo_ref,
    gg_ref,
    dsk_ref,
    out_ref,
    gn_ref,
    dbr_ref,
    dz_ref,
    dy_ref,
    y_ref,
    sst_ref,
    dsin_ref,
    ggrad_ref,
    zs,
    dgn,
    incoming,
    dsacc,
    yf,
    work,
    *,
    first,
    places,
):
    piece = x_ref.shape[0]
    chunks = piece // CL
    valid = vlen_ref[first + pl.program_id(0)]
    place = place_ref[0]

    @pl.when(pl.program_id(0) == 0)
    def _():
        ggrad_ref[...] = jnp.zeros_like(ggrad_ref)

    incoming[...] = jnp.zeros_like(incoming)
    for j in range(places - 1):

        @pl.when(j < place)
        def _():
            keep = sg_ref[j, NS : NS + 1].astype(F32) + sg_ref[j, NS + 1 : NS + 2].astype(F32)
            incoming[...] = keep * incoming[...] + sg_ref[j, 0:NS].astype(F32)

    row = lax.broadcasted_iota(jnp.int32, (piece, 1), 0)
    live = row < valid
    dbr_ref[...] = jnp.where(live, cot_ref[...].astype(F32), 0.0).astype(BF)
    for j in range(DI // 256):
        cols = slice(j * 256, (j + 1) * 256)
        zs[:, cols] = nn(nrm_ref[...], wz_ref[:, cols])
        dgn[:, cols] = nt(dbr_ref[...], wo_ref[cols, :])

    e = expander()
    low = lower_mask(False)
    left, right = half_masks()
    dsacc[...] = jnp.zeros_like(dsacc)

    def chunk(k, prefix):
        base = pl.multiple_of(k * CL, CL)
        rows = pl.ds(base, CL)
        step = step_ref[rows, :]
        ld = l_ref[rows, :]
        ldt = ld.T
        end = ld[CL - 1 :]
        before = expand(jnp.exp(jnp.broadcast_to(prefix, (8, LN))), e)[0:1]
        startf = before * incoming[...] + sloc_ref[k].astype(F32)
        start = startf.astype(BF)
        sst_ref[k] = startf
        step_e = expand(step, e)
        grow = expand(jnp.exp(ld), e)
        b = act_ref[rows, DI : DI + NS].astype(BF)
        c, c_low = halves(act_ref[rows, DI + NS :])
        scores = jnp.where(low, nt(c, b), 0.0)
        squares = jnp.zeros((CL, LN), F32)
        for j in range(DI // LN):
            x = act_ref[rows, lanes(j)]
            xd = (x * step_e[:, lanes(j)]).astype(BF)
            mixes = []
            for h in (2 * j, 2 * j + 1):
                gap = jnp.minimum(ld[:, h : h + 1] - ldt[h : h + 1, :], 0.0)
                mixes.append((jnp.exp(gap) * scores).astype(BF))
            block = jnp.concatenate([xd * left, xd * right], axis=0)
            st = start[:, lanes(j)]
            y = nn(jnp.concatenate(mixes, axis=1), block) + (nn(c, st) + nn(c_low, st)) * grow[:, lanes(j)]
            y_ref[rows, lanes(j)] = y
            full = y + dsk_ref[:, lanes(j)] * x
            yf[:, lanes(j)] = full
            z = zs[rows, lanes(j)]
            u = full * (z * sigmoid(z))
            squares = squares + u * u
        r = lax.rsqrt(jnp.sum(squares, axis=-1, keepdims=True) * (1.0 / DI) + EPSILON)
        inner = jnp.zeros((CL, LN), F32)
        for j in range(DI // LN):
            z = zs[rows, lanes(j)]
            v = yf[:, lanes(j)] * (z * sigmoid(z)) * r
            gain = gg_ref[:, lanes(j)]
            gn_ref[rows, lanes(j)] = (v * gain).astype(BF)
            dg = dgn[rows, lanes(j)]
            gv = dg * v
            ggrad_ref[:, lanes(j)] += jnp.sum(gv.reshape(CL // 8, 8, LN), axis=0)
            inner = inner + gv * gain
        q = jnp.sum(inner, axis=-1, keepdims=True) * (1.0 / DI)
        for j in range(DI // LN):
            z = zs[rows, lanes(j)]
            s = sigmoid(z)
            sz = z * s
            full = yf[:, lanes(j)]
            v = full * sz * r
            du = r * (dgn[rows, lanes(j)] * gg_ref[:, lanes(j)] - v * q)
            dy = du * sz
            dy_ref[rows, lanes(j)] = dy
            dz_ref[rows, lanes(j)] = (du * full * (s + sz * (1.0 - s))).astype(BF)
            work[:, lanes(j)] = (dy * grow[:, lanes(j)]).astype(BF)
        dsacc[...] += before * tn(c, work[...])
        return prefix + end

    lax.fori_loop(0, chunks, chunk, jnp.zeros((1, LN), F32))
    dsin_ref[...] = dsacc[...].astype(BF)
    for j in range(D // 256):
        cols = slice(j * 256, (j + 1) * 256)
        branch = nn(gn_ref[...], wo_ref[:, cols])
        out_ref[:, cols] = jnp.where(live, x_ref[:, cols].astype(F32) + branch, 0.0).astype(BF)


def mix(first, count, valid, place, tokens, cot, normed, act, step, ld, sloc, gathered, w_z, w_o, gg, dsk):
    piece = tokens.shape[1]
    chunks = piece // CL
    places = gathered.shape[0]
    sds = jax.ShapeDtypeStruct
    return pl.pallas_call(
        partial(mix_kernel, first=first, places=places),
        grid=(count,),
        in_specs=[
            SMEM,
            SMEM,
            per((piece, D), first),
            per((piece, D), first),
            per((piece, D)),
            per((piece, XBC), **ONE),
            per((piece, LN)),
            per((piece, LN)),
            per((chunks, NS, DI), **ONE),
            pl.BlockSpec((places, None, SROWS, DI), lambda i: (0, i, 0, 0), **ONE),
            kept((D, DI)),
            kept((DI, D)),
            whole((1, DI)),
            whole((1, DI)),
        ],
        out_specs=[
            per((piece, D)),
            per((piece, DI)),
            per((piece, D)),
            per((piece, DI)),
            per((piece, DI)),
            per((piece, DI)),
            per((chunks, NS, DI)),
            per((NS, DI)),
            whole((8, DI)),
        ],
        out_shape=[
            sds((count, piece, D), BF),
            sds((count, piece, DI), BF),
            sds((count, piece, D), BF),
            sds((count, piece, DI), BF),
            sds((count, piece, DI), F32),
            sds((count, piece, DI), F32),
            sds((count, chunks, NS, DI), F32),
            sds((count, NS, DI), BF),
            sds((8, DI), F32),
        ],
        scratch_shapes=[
            pltpu.VMEM((piece, DI), F32),
            pltpu.VMEM((piece, DI), F32),
            pltpu.VMEM((NS, DI), F32),
            pltpu.VMEM((NS, DI), F32),
            pltpu.VMEM((CL, DI), F32),
            pltpu.VMEM((CL, DI), BF),
        ],
        compiler_params=pltpu.CompilerParams(vmem_limit_bytes=LIMIT),
        name="mix",
    )(valid, place, tokens, cot, normed, act, step, ld, sloc, gathered, w_z, w_o, gg, dsk)


def scan_back_kernel(
    place_ref,
    ci_ref,
    step_ref,
    l_ref,
    sig_ref,
    dy_ref,
    y_ref,
    sst_ref,
    dsg_ref,
    keep_ref,
    cw_ref,
    cb_ref,
    rate_ref,
    dsk_ref,
    dxd_ref,
    fix_ref,
    edge_ref,
    cgrad_ref,
    hgrad_ref,
    skip_ref,
    ds,
    xa,
    dsl,
    dact,
    xdt,
    xt,
    dr,
    *,
    places,
):
    piece = dy_ref.shape[0]
    chunks = piece // CL
    place = place_ref[0]

    @pl.when(pl.program_id(0) == 0)
    def _():
        cgrad_ref[...] = jnp.zeros_like(cgrad_ref)
        hgrad_ref[...] = jnp.zeros_like(hgrad_ref)
        skip_ref[...] = jnp.zeros_like(skip_ref)

    ds[...] = jnp.zeros_like(ds)
    for j in reversed(range(1, places)):

        @pl.when(j > place)
        def _():
            keep = keep_ref[j, 0:1].astype(F32) + keep_ref[j, 1:2].astype(F32)
            ds[...] = keep * ds[...] + dsg_ref[j].astype(F32)

    e = expander()
    upper = jnp.logical_not(lower_mask(True))
    upper_one = jnp.where(upper, 1.0, 0.0)
    before_one = jnp.where(lower_mask(True), 1.0, 0.0)
    left, right = half_masks()
    dr[CL:] = jnp.zeros((8, XBC), F32)

    def chunk(i, carry):
        k = chunks - 1 - i
        base = pl.multiple_of(k * CL, CL)
        rows = pl.ds(base, CL)
        step = step_ref[rows, :]
        ld = l_ref[rows, :]
        ldt = ld.T
        end = ld[CL - 1 :]
        step_e = expand(step, e)
        grow = expand(jnp.exp(ld), e)
        tail = expand(jnp.exp(end - ld), e)
        keep = expand(jnp.exp(jnp.broadcast_to(end, (8, LN))), e)[0:1]
        for j in range(XBC // LN):
            ext = ci_ref[pl.ds(base, CL + 8), lanes(j)]
            run = conv_running(ext, cw_ref[:, lanes(j)], cb_ref[:, lanes(j)])
            s = sigmoid(run)
            a = run * s
            xa[:, lanes(j)] = a
            dsl[:, lanes(j)] = s + a * (1.0 - s)
            if j < DI // LN:
                xd = a * step_e[:, lanes(j)]
                xdt[:, lanes(j)] = xd
                xt[:, lanes(j)] = xd * tail[:, lanes(j)]
        b = xa[:, DI : DI + NS].astype(BF)
        c = xa[:, DI + NS :].astype(BF)
        scores = jnp.where(upper, nt(b, c), 0.0)
        dsb = ds[...].astype(BF)
        start = sst_ref[k]
        dscores = jnp.zeros((CL, CL), F32)
        db = three(nt, xt[...], ds[...])
        dc = jnp.zeros((CL, NS), F32)
        r_u = jnp.zeros((CL, LN), F32)
        r_f = jnp.zeros((CL, LN), F32)
        r_v = jnp.zeros((CL, LN), F32)
        r_c = jnp.zeros((8, LN), F32)
        for j in range(DI // LN):
            et = e[:, lanes(j)]
            dyf = dy_ref[rows, lanes(j)]
            dyb, dyl = halves(dyf)
            block = jnp.concatenate([dyb * left, dyb * right], axis=0)
            xdb, xdl = halves(xdt[:, lanes(j)])
            dmix = nt(xdb, block)
            dmix = dmix + nt(xdl, block) + nt(xdb, jnp.concatenate([dyl * left, dyl * right], axis=0))
            mixes = []
            for p, h in enumerate((2 * j, 2 * j + 1)):
                gap = jnp.minimum(ldt[h : h + 1, :] - ld[:, h : h + 1], 0.0)
                w = jnp.exp(gap)
                mixes.append((w * scores).astype(BF))
                dscores = dscores + dmix[:, lanes(p)] * w
            diag = nn(jnp.concatenate(mixes, axis=1), block)
            far = nn(b, dsb[:, lanes(j)]) * tail[:, lanes(j)]
            xdf = xdb.astype(F32)
            u_top, u_low = halves(dyb.astype(F32) * y_ref[rows, lanes(j)] - xdf * diag)
            r_u = r_u + nt(u_top, et) + nt(u_low, et)
            r_f = r_f + nt((xdf * far).astype(BF), et)
            dxd = diag + far
            x = xa[:, lanes(j)]
            r_v = r_v + nt((x * dxd).astype(BF), et)
            dact[:, lanes(j)] = dxd * step_e[:, lanes(j)] + dsk_ref[:, lanes(j)] * dyf
            skip_ref[:, lanes(j)] += jnp.sum((dyf * x).reshape(CL // 8, 8, LN), axis=0)
            dygf = dyf * grow[:, lanes(j)]
            dyg = dygf.astype(BF)
            st = start[:, lanes(j)]
            dc = dc + three(nt, dygf, st)
            dsj = ds[:, lanes(j)]
            const = jnp.sum((st * dsj).reshape(NS // 8, 8, LN), axis=0) * keep[:, lanes(j)]
            c_top, c_low = halves(const)
            r_c = r_c + nt(c_top, et) + nt(c_low, et)
            ds[:, lanes(j)] = keep[:, lanes(j)] * dsj + tn(c, dyg)
        dsc = jnp.where(upper, dscores, 0.0).astype(BF)
        dact[:, DI : DI + NS] = db + nn(dsc, c)
        dact[:, DI + NS :] = dc + tn(dsc, b)
        da = exact_nn(upper_one, r_u) + exact_nn(before_one, r_f) + jnp.sum(r_c, axis=0, keepdims=True)
        dstep = r_v + rate_ref[...] * da
        ddt = dstep * sig_ref[rows, :]
        hgrad_ref[0:8] += jnp.sum(ddt.reshape(CL // 8, 8, LN), axis=0)
        hgrad_ref[8:16] += jnp.sum((da * step).reshape(CL // 8, 8, LN), axis=0)
        dxd_ref[rows, XBC:] = ddt.astype(BF)
        for j in range(XBC // LN):
            g = dact[:, lanes(j)] * dsl[:, lanes(j)]
            dr[0:CL, lanes(j)] = g
            ext = ci_ref[pl.ds(base, CL + 8), lanes(j)]
            gext = dr[:, lanes(j)]
            total = jnp.zeros((CL, LN), F32)
            for tap in range(DCONV):
                total = total + gext[DCONV - 1 - tap : DCONV - 1 - tap + CL] * cw_ref[tap : tap + 1, lanes(j)]
                part = g * ext[5 + tap : 5 + tap + CL]
                cgrad_ref[8 * tap : 8 * tap + 8, lanes(j)] += jnp.sum(part.reshape(CL // 8, 8, LN), axis=0)
            cgrad_ref[32:40, lanes(j)] += jnp.sum(g.reshape(CL // 8, 8, LN), axis=0)
            dxd_ref[rows, lanes(j)] = total.astype(BF)

            @pl.when(i == 0)
            def _():
                fix_ref[:, lanes(j)] = total[CL - 16 :]

            dr[CL:, lanes(j)] = g[0:8]
        return carry

    lax.fori_loop(0, chunks, chunk, 0)
    edge_ref[...] = dr[CL:]


def scan_back(count, place, ci, step, ld, sig, dy, y, sst, dsg, gathered, cw, cb, rate, dsk):
    piece = dy.shape[1]
    chunks = piece // CL
    places = gathered.shape[0]
    sds = jax.ShapeDtypeStruct
    return pl.pallas_call(
        partial(scan_back_kernel, places=places),
        grid=(count,),
        in_specs=[
            SMEM,
            per((piece + 8, XBC)),
            per((piece, LN)),
            per((piece, LN)),
            per((piece, LN)),
            per((piece, DI)),
            per((piece, DI)),
            per((chunks, NS, DI)),
            pl.BlockSpec((places, None, NS, DI), lambda i: (0, i, 0, 0), **ONE),
            pl.BlockSpec((places, None, 16, DI), lambda i: (0, i, NS // 16, 0)),
            whole((DCONV, XBC)),
            whole((1, XBC)),
            whole((1, LN)),
            whole((1, DI)),
        ],
        out_specs=[
            per((piece, XD)),
            per((16, XBC)),
            per((8, XBC)),
            whole((40, XBC)),
            whole((16, LN)),
            whole((8, DI)),
        ],
        out_shape=[
            sds((count, piece, XD), BF),
            sds((count, 16, XBC), F32),
            sds((count, 8, XBC), F32),
            sds((40, XBC), F32),
            sds((16, LN), F32),
            sds((8, DI), F32),
        ],
        scratch_shapes=[
            pltpu.VMEM((NS, DI), F32),
            pltpu.VMEM((CL, XBC), F32),
            pltpu.VMEM((CL, XBC), F32),
            pltpu.VMEM((CL, XBC), F32),
            pltpu.VMEM((CL, DI), F32),
            pltpu.VMEM((CL, DI), F32),
            pltpu.VMEM((CL + 8, XBC), F32),
        ],
        compiler_params=pltpu.CompilerParams(vmem_limit_bytes=LIMIT),
        name="scan_back",
    )(place, ci, step, ld, sig, dy, y, sst, dsg, gathered, cw, cb, rate, dsk)


def input_grad_kernel(x_ref, dbr_ref, g_ref, dz_ref, dxd_ref, wz_ref, wx_ref, out_ref, gain_ref, dn):
    piece = x_ref.shape[0]

    @pl.when(pl.program_id(0) == 0)
    def _():
        gain_ref[...] = jnp.zeros_like(gain_ref)

    for j in range(D // 256):
        cols = slice(j * 256, (j + 1) * 256)
        dn[:, cols] = nt(dz_ref[...], wz_ref[cols, :]) + nt(dxd_ref[...], wx_ref[cols, :])

    def rows_of(i, c):
        rows = pl.ds(pl.multiple_of(i * 64, 64), 64)
        x = x_ref[rows, :].astype(F32)
        d = dn[rows, :]
        r = lax.rsqrt(jnp.mean(x * x, axis=-1, keepdims=True) + EPSILON)
        v = x * r
        gain_ref[...] += jnp.sum((d * v).reshape(8, 8, D), axis=0)
        dv = d * g_ref[...]
        q = jnp.mean(dv * v, axis=-1, keepdims=True)
        out_ref[rows, :] = (dbr_ref[rows, :].astype(F32) + r * (dv - v * q)).astype(BF)
        return c

    lax.fori_loop(0, piece // 64, rows_of, 0)


def input_grad(first, count, tokens, dbr, gain, dz, dxd, w_z, w_xd):
    piece = tokens.shape[1]
    sds = jax.ShapeDtypeStruct
    return pl.pallas_call(
        input_grad_kernel,
        grid=(count,),
        in_specs=[
            per((piece, D), first),
            per((piece, D)),
            whole((1, D)),
            per((piece, DI)),
            per((piece, XD)),
            kept((D, DI)),
            kept((D, XD)),
        ],
        out_specs=[per((piece, D)), whole((8, D))],
        out_shape=[sds((count, piece, D), BF), sds((8, D), F32)],
        scratch_shapes=[pltpu.VMEM((piece, D), F32)],
        compiler_params=pltpu.CompilerParams(vmem_limit_bytes=LIMIT),
        name="input_grad",
    )(tokens, dbr, gain, dz, dxd, w_z, w_xd)


MESH_ID = pl.DeviceIdType.MESH


class Here:
    def __init__(self, depth):
        dp, seq = lax.axis_index("dp"), lax.axis_index("seq")
        self.depth = depth
        self.levels = depth.bit_length() - 1
        self.z, self.y = dp // 2, dp % 2
        self.x, self.c = seq // 2, seq % 2
        self.rank = dp * 4 + seq

    def device(self, z=None, y=None, x=None, c=None):
        z = self.z if z is None else z
        y = self.y if y is None else y
        x = self.x if x is None else x
        c = self.c if c is None else c
        return (z * 2 + y, x * 2 + c)

    def across(self, level):
        size = 1 << level
        return self.z + size * (1 - 2 * ((self.z // size) % 2))

    def block(self, level):
        size = 1 << level
        return (self.z // size) * size, size

    def block_across(self, level):
        size = 1 << level
        return (self.z // size) * size + size * (1 - 2 * ((self.z // size) % 2)), size

    def greet(self, ranks):
        barrier = pltpu.get_barrier_semaphore()

        def hail(i, carry):
            other = (self.rank + i) % ranks
            pl.semaphore_signal(
                barrier, inc=1, device_id=(other // 4, other % 4), device_id_type=MESH_ID
            )
            return carry

        lax.fori_loop(1, ranks, hail, 0)
        pl.semaphore_wait(barrier, ranks - 1)


class Copies:
    def __init__(self, send, recv):
        self.send, self.recv, self.made = send, recv, []

    def start(self, pairs, device):
        waits = []
        for source, target, landing in pairs:
            i = len(self.made)
            copy = pltpu.make_async_remote_copy(
                src_ref=source,
                dst_ref=target,
                send_sem=self.send.at[i],
                recv_sem=self.recv.at[i],
                device_id=device,
                device_id_type=MESH_ID,
            )
            copy.start()
            self.made.append(copy)
            waits.append(
                pltpu.make_async_remote_copy(
                    src_ref=source,
                    dst_ref=landing,
                    send_sem=self.send.at[i],
                    recv_sem=self.recv.at[i],
                    device_id=device,
                    device_id_type=MESH_ID,
                )
            )
        return waits

    def finish(self):
        for copy in self.made:
            copy.wait_send()


def arrived(waits):
    for w in waits:
        w.wait_recv()


BOTH = slice(None)


def at(item, z, y, x, c):
    ref, half = item
    index = (z, y, x, c)
    return ref.at[index if half is None else index + (half,)]


def everyone(rank, ranks, source, target, send, recv, own):
    def one(i, starting):
        other = (rank + i) % ranks
        copy = pltpu.make_async_remote_copy(
            src_ref=source(other),
            dst_ref=target(rank),
            send_sem=send.at[i],
            recv_sem=recv.at[i],
            device_id=(other // 4, other % 4),
            device_id_type=MESH_ID,
        )
        return copy

    def begin(i, carry):
        one(i, True).start()
        return carry

    def end(i, carry):
        copy = one(i, False)
        copy.wait_send()
        copy.wait_recv()
        return carry

    def start():
        lax.fori_loop(1, ranks, begin, 0)

    def finish():
        lax.fori_loop(1, ranks, end, 0)

    return start, finish


def gather_stream(here, copies, items, first):
    z, y, x, c = here.z, here.y, here.x, here.c
    a_dev = here.device(x=1 - x) if first == "x" else here.device(y=1 - y)
    b_dev = here.device(y=1 - y) if first == "x" else here.device(x=1 - x)
    sibling = here.device(c=1 - c)
    cores = []

    def a_there(item, zs, core):
        return at(item, zs, y, 1 - x, core) if first == "x" else at(item, zs, 1 - y, x, core)

    def line(item, zs, core):
        return at(item, zs, y, BOTH, core) if first == "x" else at(item, zs, BOTH, x, core)

    def line_there(item, zs, core):
        return at(item, zs, 1 - y, BOTH, core) if first == "x" else at(item, zs, BOTH, 1 - x, core)

    def same(where, zs):
        return [(where(i, zs, c), where(i, zs, c), where(i, zs, 1 - c)) for i in items]

    def to_core(where, zs):
        cores.extend(copies.start(same(where, zs), sibling))

    def mine(item, zs, core):
        return at(item, zs, y, x, core)

    def start_a(zs):
        waits = copies.start([(mine(i, zs, c), mine(i, zs, c), a_there(i, zs, c)) for i in items], a_dev)
        to_core(mine, zs)
        return waits

    def start_b(zs, waits):
        arrived(waits)
        out = copies.start([(line(i, zs, c), line(i, zs, c), line_there(i, zs, c)) for i in items], b_dev)
        to_core(a_there, zs)
        return out

    def end_b(zs, waits):
        arrived(waits)
        to_core(line_there, zs)

    sets = [pl.ds(z, 1)]
    waiting_a, waiting_b = [], []
    for level in range(here.levels):
        base, size = here.block(level)
        far, _ = here.block_across(level)
        own, theirs = pl.ds(base, size), pl.ds(far, size)
        zwait = copies.start(
            [(mine(i, own, c), mine(i, own, c), mine(i, theirs, c)) for i in items],
            here.device(z=here.across(level)),
        )
        waiting_a.append((sets[-1], start_a(sets[-1])))
        sets.append(theirs)
        yield
        if level:
            zs, w = waiting_a.pop(0)
            waiting_b.append((zs, start_b(zs, w)))
            yield
        arrived(zwait)
    waiting_a.append((sets[-1], start_a(sets[-1])))
    while waiting_a:
        yield
        zs, w = waiting_a.pop(0)
        waiting_b.append((zs, start_b(zs, w)))
    while waiting_b:
        yield
        zs, w = waiting_b.pop(0)
        end_b(zs, w)
    yield
    arrived(cores)


def side_by_side(streams):
    streams = list(streams)
    while streams:
        for s in list(streams):
            try:
                next(s)
            except StopIteration:
                streams.remove(s)


def gather_kernel(
    xd_in, z_in, o_in, small_in, xd_out, z_out, o_out, small_out, send, recv, ssend, srecv, place_sem, *, depth, ranks
):
    here = Here(depth)
    z, y, x, c = here.z, here.y, here.x, here.c
    own = []
    for i, (source, target) in enumerate(((xd_in, xd_out), (z_in, z_out), (o_in, o_out))):
        own.append(pltpu.make_async_copy(source, target.at[z, y, x, c], place_sem.at[i]))
    own.append(pltpu.make_async_copy(small_in, small_out.at[here.rank], place_sem.at[3]))
    for copy in own:
        copy.start()
    here.greet(ranks)
    start, finish = everyone(
        here.rank, ranks, lambda other: small_in, lambda rank: small_out.at[rank], ssend, srecv, None
    )
    for copy in own:
        copy.wait()
    copies = Copies(send, recv)
    streams = [
        gather_stream(here, copies, [(xd_out, None), (o_out, 0)], "x"),
        gather_stream(here, copies, [(z_out, None), (o_out, 1)], "y"),
    ]
    start()
    side_by_side(streams)
    finish()
    copies.finish()


def copies_needed(levels):
    return 2 * 2 * (levels + 5 * (levels + 1))


def gather(xd, wz, wo, small, depth):
    ranks = depth * 8
    lead = (depth, 2, 2, 2)
    sds = jax.ShapeDtypeStruct
    n = copies_needed(depth.bit_length() - 1)
    any_space = pl.BlockSpec(memory_space=pl.ANY)
    in_vmem = pl.BlockSpec(memory_space=pltpu.VMEM)
    dma = pltpu.SemaphoreType.DMA
    return pl.pallas_call(
        partial(gather_kernel, depth=depth, ranks=ranks),
        in_specs=[in_vmem] * 4,
        out_specs=[any_space] * 4,
        out_shape=[sds(lead + a.shape, a.dtype) for a in (xd, wz, wo)] + [sds((ranks,) + small.shape, small.dtype)],
        scratch_shapes=[dma((n,)), dma((n,)), dma((ranks,)), dma((ranks,)), dma((4,))],
        compiler_params=pltpu.CompilerParams(collective_id=0, has_side_effects=True),
        name="gather",
    )(xd, wz, wo, small)


def reduce_stream(here, copies, items, first):
    z, y, x, c = here.z, here.y, here.x, here.c
    one_dev = here.device(y=1 - y) if first == "y" else here.device(x=1 - x)
    two_dev = here.device(x=1 - x) if first == "y" else here.device(y=1 - y)
    sibling = here.device(c=1 - c)

    def part(item, zs, core):
        return at((item[0], item[1]), zs, BOTH, BOTH, core)

    def keep_line(zs):
        return (zs, y, BOTH) if first == "y" else (zs, BOTH, x)

    def give_line(zs):
        return (zs, 1 - y, BOTH) if first == "y" else (zs, BOTH, 1 - x)

    def give_one(zs):
        return (zs, y, 1 - x) if first == "y" else (zs, 1 - y, x)

    def keep_one(zs):
        return (zs, y, x)

    sets = []
    for level in reversed(range(here.levels)):
        far, size = here.block_across(level)
        sets.append((far, size))
    sets.append((z, 1))

    def slots(zs):
        return pl.ds(zs[0], zs[1])

    def over(zs, body):
        for k in range(zs[1]):
            body(zs[0] + k)

    def core_phase(zs):
        s = slots(zs)
        return copies.start([(part(i, s, 1 - c), i[3].at[s], i[3].at[s]) for i in items], sibling)

    def line_phase(zs, waits):
        arrived(waits)

        def add(k):
            for item in items:
                for a in range(2):
                    for b in range(2):
                        index = (k, a, b, c) if item[1] is None else (k, a, b, c, item[1])
                        item[2][k, a, b] = (item[0][index].astype(F32) + item[3][k, a, b].astype(F32)).astype(BF)

        over(zs, add)
        s = slots(zs)
        return copies.start([(i[2].at[give_line(s)], i[4].at[s], i[4].at[s]) for i in items], one_dev)

    def side_phase(zs, waits):
        arrived(waits)

        def add(k):
            for item in items:
                for a in range(2):
                    index = (k, y, a) if first == "y" else (k, a, x)
                    item[2][index] = (item[2][index].astype(F32) + item[4][k, a].astype(F32)).astype(BF)

        over(zs, add)
        s = slots(zs)
        return copies.start([(i[2].at[give_one(s)], i[5].at[s], i[5].at[s]) for i in items], two_dev)

    def last_phase(zs, waits):
        arrived(waits)

        def add(k):
            for item in items:
                item[2][k, y, x] = (item[2][k, y, x].astype(F32) + item[5][k].astype(F32)).astype(BF)

        over(zs, add)

    cores = [core_phase(zs) for zs in sets]
    yield
    lines, sides = [], []
    n = len(sets)
    for step in range(n + 2):
        if step < n:
            lines.append(line_phase(sets[step], cores[step]))
            yield
        if 1 <= step <= n:
            sides.append(side_phase(sets[step - 1], lines[step - 1]))
            yield
        if step >= 2:
            last_phase(sets[step - 2], sides[step - 2])
            if step == 2:
                level = here.levels - 1
                far, size = here.block_across(level)
                base, _ = here.block(level)
                s, own = pl.ds(far, size), pl.ds(base, size)
                zwait = copies.start(
                    [(i[2].at[s, y, x], i[6][0].at[0:size], i[6][0].at[0:size]) for i in items],
                    here.device(z=here.across(level)),
                )
            yield
    for depth_at, level in enumerate(reversed(range(here.levels))):
        size = 1 << level
        base, _ = here.block(level)
        arrived(zwait)
        for k in range(size):
            for item in items:
                got = item[6][depth_at][k].astype(F32) + item[2][base + k, y, x].astype(F32)
                if level:
                    item[2][base + k, y, x] = got.astype(BF)
                else:
                    item[7](got)
        if level:
            size = 1 << (level - 1)
            far, _ = here.block_across(level - 1)
            zwait = copies.start(
                [
                    (i[2].at[pl.ds(far, size), y, x], i[6][depth_at + 1].at[0:size], i[6][depth_at + 1].at[0:size])
                    for i in items
                ],
                here.device(z=here.across(level - 1)),
            )
            yield


def reduce_kernel(*refs, depth, ranks, names):
    here = Here(depth)
    levels = here.levels
    count = len(names)
    parts = refs[:count]
    small_in = refs[count]
    outs = refs[count + 1 : 2 * count + 1]
    small_out = refs[2 * count + 1]
    scratch = list(refs[2 * count + 2 :])
    send, recv, ssend, srecv, small_got = scratch[:5]
    scratch = scratch[5:]
    here.greet(ranks)
    start, finish = everyone(
        here.rank, ranks, lambda other: small_in.at[other], lambda rank: small_got.at[rank], ssend, srecv, None
    )
    start()
    copies = Copies(send, recv)
    streams = []
    at_scratch = 0
    for first, members in (("y", [m for m in STREAM_Y if m[0] in names]), ("x", [m for m in STREAM_X if m[0] in names])):
        items = []
        for name, half in members:
            k = names.index(name)
            acc, core_in, line_in, side_in = scratch[at_scratch : at_scratch + 4]
            z_in = scratch[at_scratch + 4 : at_scratch + 4 + levels]
            at_scratch += 4 + levels

            def put(v, k=k, half=half):
                if half is None:
                    outs[k][...] = v
                else:
                    outs[k][half] = v

            items.append((parts[k], half, acc, core_in, line_in, side_in, z_in, put))
        if items:
            streams.append(reduce_stream(here, copies, items, first))
    side_by_side(streams)
    finish()

    def add(i, total):
        return total + jnp.where(i == here.rank, small_in[i], small_got[i])

    small_out[...] = lax.fori_loop(0, ranks, add, jnp.zeros(small_out.shape, F32))
    copies.finish()


STREAM_Y = [("xd", None), ("o", 0)]
STREAM_X = [("z", None), ("o", 1)]


def reduce(parts, small, depth, ident):
    ranks = depth * 8
    levels = depth.bit_length() - 1
    names = list(parts)
    arrays = [parts[n] for n in names]
    sds = jax.ShapeDtypeStruct
    dma = pltpu.SemaphoreType.DMA
    in_vmem = pl.BlockSpec(memory_space=pltpu.VMEM)
    n = 2 * 2 * (3 * (levels + 1) + levels)
    scratch = [dma((n,)), dma((n,)), dma((ranks,)), dma((ranks,)), pltpu.VMEM(small.shape, F32)]
    for name, half in [m for m in STREAM_Y + STREAM_X if m[0] in names]:
        tile = parts[name].shape[-2:]
        scratch.append(pltpu.VMEM((depth, 2, 2) + tile, BF))
        scratch.append(pltpu.VMEM((depth, 2, 2) + tile, BF))
        scratch.append(pltpu.VMEM((depth, 2) + tile, BF))
        scratch.append(pltpu.VMEM((depth,) + tile, BF))
        for level in reversed(range(levels)):
            scratch.append(pltpu.VMEM((1 << level,) + tile, BF))
    return pl.pallas_call(
        partial(reduce_kernel, depth=depth, ranks=ranks, names=names),
        in_specs=[in_vmem] * (len(arrays) + 1),
        out_specs=[in_vmem] * (len(arrays) + 1),
        out_shape=[sds(a.shape[4:], F32) for a in arrays] + [sds(small.shape[1:], F32)],
        scratch_shapes=scratch,
        compiler_params=pltpu.CompilerParams(collective_id=ident, has_side_effects=True, vmem_limit_bytes=LIMIT),
        name="reduce",
    )(*arrays, small)


def pass_on(block, axis, distance):
    devices = range(lax.axis_size(axis))
    route = [(i - distance, i) for i in devices if i - distance in devices]
    return lax.ppermute(block, axis, route)


def contract_rows(left, right):
    return lax.dot_general(left, right, (((0, 1), (0, 1)), ((), ())), preferred_element_type=F32)


def local(
    tokens,
    norm_gain,
    w_in,
    conv_weight,
    conv_bias,
    dt_bias,
    a_log,
    d_skip,
    gated_gain,
    w_out,
    lengths,
    cotangent,
):
    ranks = lax.axis_size("dp") * lax.axis_size("seq")
    place = lax.axis_index("seq")
    tokens = tokens[:, 0]
    cot = cotangent[:, 0]
    batches, piece, _ = tokens.shape
    rows = w_in.shape[0]

    depth = lax.axis_size("dp") // 2
    n0, n1, n2 = norm_gain.shape[0], gated_gain.shape[0], conv_bias.shape[0]
    small = jnp.concatenate([norm_gain, gated_gain, conv_bias, conv_weight.reshape(-1)])
    small = jnp.pad(small, (0, 8 * LN - small.shape[0])).reshape(8, LN)
    w_low = w_in.astype(BF)
    w_xd = jnp.pad(w_low[:, DI:], ((0, 0), (0, XD - (PROJ - DI))))
    w_xd, w_z, w_o, small = gather(w_xd, w_low[:, :DI], w_out.astype(BF).reshape(2, n1 // 2, D), small, depth)
    w_xd, w_z, w_o = w_xd.reshape(D, XD), w_z.reshape(D, DI), w_o.reshape(DI, D)
    small = small.reshape(ranks, 8 * LN)
    gain = small[:, :n0].reshape(1, D)
    gg = small[:, n0 : n0 + n1].reshape(1, DI)
    cb = small[:, n0 + n1 : n0 + n1 + n2].reshape(1, XBC)
    cw = small[:, n0 + n1 + n2 : n0 + n1 + 5 * n2].reshape(ranks, DCONV, n2).transpose(1, 0, 2).reshape(DCONV, XBC)

    halo = pass_on(tokens[:, piece - 16 :], "seq", 1)
    valid = lengths[:, 0].astype(jnp.int32) - place.astype(jnp.int32) * piece
    where_am_i = place.astype(jnp.int32).reshape(1)
    lane_pad = ((0, 0), (0, LN - NH))
    dtb = jnp.pad(dt_bias[None], lane_pad)
    rate = -jnp.exp(a_log)
    rate_row = jnp.pad(rate[None], lane_pad)
    dsk = jnp.repeat(d_skip, HD)[None]

    first, count = 0, batches
    normed, ci, act, step, ld, sig, sloc, s = project(
        first, count, valid, tokens, halo, gain, w_xd, cw, cb, dtb, rate_row
    )
    gathered = lax.all_gather(s, "seq")
    out, gn, dbr, dz, dy, y, sst, dsin, ggrad = mix(
        first, count, valid, where_am_i, tokens, cot, normed, act, step, ld, sloc, gathered, w_z, w_o, gg, dsk
    )
    dsg = lax.all_gather(dsin, "seq")
    dxd, fix, edge, cgrad, hgrad, skip = scan_back(
        count, where_am_i, ci, step, ld, sig, dy, y, sst, dsg, gathered, cw, cb, rate_row, dsk
    )
    next_edge = pass_on(edge, "seq", -1)[:, : DCONV - 1]
    late = []
    for j in range(DCONV - 1):
        late.append(sum(cw[t][None] * next_edge[:, j - t] for t in range(j + 1)))
    late = jnp.stack(late, axis=1)
    fixed = fix.at[:, 16 - (DCONV - 1) :].add(late).astype(BF)
    dxd = dxd.at[:, piece - 16 :, :XBC].set(fixed)
    tgrad, gain_grad = input_grad(first, count, tokens, dbr, gain, dz, dxd, w_z, w_xd)

    grad_wo = contract_rows(gn, dbr)
    grad_wz = contract_rows(normed, dz)
    grad_wx = contract_rows(normed, dxd)
    lead = (depth, 2, 2, 2)
    grad_cw = cgrad[:32].reshape(DCONV, 8, XBC).sum(1)
    heads = hgrad.reshape(2, 8, LN).sum(1)[:, :NH]
    heads = jnp.concatenate([heads[0], heads[1] * rate, skip.sum(0).reshape(NH, HD).sum(1)])
    packed = jnp.concatenate(
        [
            gain_grad.sum(0).reshape(ranks, n0),
            ggrad.sum(0).reshape(ranks, n1),
            cgrad[32:].sum(0).reshape(ranks, n2),
            grad_cw.reshape(DCONV, ranks, n2).transpose(1, 0, 2).reshape(ranks, DCONV * n2),
            jnp.broadcast_to(heads[None], (ranks, 3 * NH)),
        ],
        axis=1,
    )
    used = packed.shape[1]
    packed = jnp.pad(packed, ((0, 0), (0, 8 * LN - used))).reshape(ranks, 8, LN)
    parts = {
        "xd": grad_wx.astype(BF).reshape(lead + (rows, XD)),
        "z": grad_wz.astype(BF).reshape(lead + (rows, DI)),
        "o": grad_wo.astype(BF).reshape(lead + (2, n1 // 2, D)),
    }
    shard_wx, shard_wz, shard_wo, total = reduce(parts, packed, depth, 1)
    shard_win = jnp.concatenate([shard_wz, shard_wx[:, : PROJ - DI]], axis=1)
    total = total.reshape(-1)[:used]
    sizes = [n0, n1, n2, DCONV * n2, NH, NH, NH]
    starts = [sum(sizes[:i]) for i in range(len(sizes))]
    mine = [total[a : a + n] for a, n in zip(starts, sizes)]
    return (
        out[:, None],
        tgrad[:, None],
        mine[0],
        shard_win,
        mine[3].reshape(DCONV, n2),
        mine[2],
        mine[4],
        mine[5],
        mine[6],
        mine[1],
        shard_wo.reshape(n1, D),
    )


def solution(mesh):
    shard = P(("dp", "seq"))
    row_shard = P(("dp", "seq"), None)
    col_shard = P(None, ("dp", "seq"))
    acts = P(None, "dp", "seq", None)
    return jax.shard_map(
        local,
        mesh=mesh,
        in_specs=(
            acts,
            shard,
            row_shard,
            col_shard,
            shard,
            P(),
            P(),
            P(),
            shard,
            row_shard,
            P(None, "dp"),
            acts,
        ),
        out_specs=(
            acts,
            acts,
            shard,
            row_shard,
            col_shard,
            shard,
            P(),
            P(),
            P(),
            shard,
            row_shard,
        ),
        check_vma=False,
    )
```

```python
from functools import partial

import jax
import jax.numpy as jnp
from jax import lax
from jax.experimental import pallas as pl
from jax.experimental.pallas import tpu as pltpu
from jax.sharding import PartitionSpec as P

D = 768
NH = 24
HD = 64
NS = 128
DCONV = 4
CL = 128
DI = 1536
XBC = 1792
PROJ = 3352
XD = 1920
LN = 128
EPSILON = 1e-05

F32 = jnp.float32
BF = jnp.bfloat16
SROWS = 144


def nn(a, b):
    return lax.dot_general(a, b, (((1,), (0,)), ((), ())), preferred_element_type=F32)


def nt(a, b):
    return lax.dot_general(a, b, (((1,), (1,)), ((), ())), preferred_element_type=F32)


def tn(a, b):
    return lax.dot_general(a, b, (((0,), (0,)), ((), ())), preferred_element_type=F32)


def exact_nn(a, b):
    return lax.dot_general(
        a, b, (((1,), (0,)), ((), ())), precision=lax.Precision.HIGHEST, preferred_element_type=F32
    )


def sigmoid(v):
    return 0.5 * jnp.tanh(0.5 * v) + 0.5


def halves(v):
    top = v.astype(BF)
    return top, (v - top.astype(F32)).astype(BF)


def three(op, a, b):
    ah, al = halves(a)
    bh, bl = halves(b)
    return op(ah, bh) + op(al, bh) + op(ah, bl)


def fill_expander(ref):
    head = lax.broadcasted_iota(jnp.int32, (LN, DI), 0)
    lane = lax.broadcasted_iota(jnp.int32, (LN, DI), 1)
    e = jnp.where(head == lane // HD, 1.0, 0.0).astype(BF)
    ref[0:LN] = e
    ref[LN:] = e


def expand(v, e2):
    return nn(jnp.concatenate(halves(v), axis=1), e2[...])


def lower_mask(strict):
    row = lax.broadcasted_iota(jnp.int32, (CL, CL), 0)
    col = lax.broadcasted_iota(jnp.int32, (CL, CL), 1)
    return row > col if strict else row >= col


def half_masks():
    lane = lax.broadcasted_iota(jnp.int32, (1, 2 * HD), 1)
    left = jnp.where(lane < HD, 1.0, 0.0).astype(BF)
    right = jnp.where(lane < HD, 0.0, 1.0).astype(BF)
    return left, right


def lanes(j):
    return slice(j * LN, (j + 1) * LN)


def conv_running(ext, cw, cb):
    total = cb
    for tap in range(DCONV):
        total = total + ext[5 + tap : 5 + tap + CL] * cw[tap : tap + 1]
    return total


def project_kernel(
    vlen_ref,
    x_ref,
    xh_ref,
    g_ref,
    w_ref,
    cw_ref,
    cb_ref,
    dtb_ref,
    rate_ref,
    nrm_ref,
    ci_ref,
    act_ref,
    step_ref,
    l_ref,
    sig_ref,
    sloc_ref,
    s_ref,
    nx,
    xw,
    state,
    e2,
    *,
    first,
):
    piece = x_ref.shape[0]
    chunks = piece // CL
    valid = vlen_ref[first + pl.program_id(0)]

    def norm(v):
        v = v.astype(F32)
        r = lax.rsqrt(jnp.mean(v * v, axis=-1, keepdims=True) + EPSILON)
        return (v * r * g_ref[...]).astype(BF)

    nx[0:16] = norm(xh_ref[...])

    def norm_rows(i, c):
        rows = pl.ds(pl.multiple_of(i * 64, 64), 64)
        v = norm(x_ref[rows, :])
        nx[pl.ds(pl.multiple_of(i * 64 + 16, 16), 64), :] = v
        nrm_ref[rows, :] = v
        return c

    lax.fori_loop(0, piece // 64, norm_rows, 0)

    for j in range(XBC // 256):
        cols = slice(j * 256, (j + 1) * 256)
        ci_ref[:, cols] = nn(nx[...], w_ref[:, cols])[8:]
    dt_raw = nn(nx[16:], w_ref[:, XBC:]) + dtb_ref[...]
    row = lax.broadcasted_iota(jnp.int32, (piece, LN), 0)
    mask = jnp.where(row < valid, 1.0, 0.0)
    step_ref[...] = (jnp.maximum(dt_raw, 0.0) + jnp.log1p(jnp.exp(-jnp.abs(dt_raw)))) * mask
    sig_ref[...] = mask / (1.0 + jnp.exp(-dt_raw))

    @pl.when(pl.program_id(0) == 0)
    def _():
        fill_expander(e2)

    tri = jnp.where(lower_mask(False), 1.0, 0.0)
    state[...] = jnp.zeros_like(state)

    def chunk(k, total):
        base = pl.multiple_of(k * CL, CL)
        rows = pl.ds(base, CL)
        step = step_ref[rows, :]
        ld = exact_nn(tri, step * rate_ref[...])
        l_ref[rows, :] = ld
        end = ld[CL - 1 :]
        tail = expand(step * jnp.exp(end - ld), e2)
        for j in range(XBC // LN):
            ext = ci_ref[pl.ds(base, CL + 8), lanes(j)]
            run = conv_running(ext, cw_ref[:, lanes(j)], cb_ref[:, lanes(j)])
            act = run * sigmoid(run)
            act_ref[rows, lanes(j)] = act
            if j < DI // LN:
                xw[:, lanes(j)] = (act * tail[:, lanes(j)]).astype(BF)
        b = act_ref[rows, DI : DI + NS].astype(BF)
        sloc_ref[k] = state[...].astype(BF)
        keep = expand(jnp.exp(jnp.broadcast_to(end, (8, LN))), e2)[0:1]
        state[...] = keep * state[...] + tn(b, xw[...])
        return total + end

    total = lax.fori_loop(0, chunks, chunk, jnp.zeros((1, LN), F32))
    s_ref[0:NS] = state[...].astype(BF)
    keep = expand(jnp.exp(jnp.broadcast_to(total, (8, LN))), e2)[0:1]
    top, low = halves(keep)
    s_ref[NS : NS + 16] = jnp.concatenate([top, low, jnp.zeros((14, DI), BF)], axis=0)


def whole(shape):
    return pl.BlockSpec(shape, lambda i: (0,) * len(shape))


def kept(shape):
    return pl.BlockSpec(shape, lambda i: (0,) * len(shape), pipeline_mode=pl.Buffered(1))


def per(shape, first=0, **mode):
    rest = (0,) * len(shape)
    return pl.BlockSpec((None,) + shape, lambda i: (first + i,) + rest, **mode)


ONE = dict(pipeline_mode=pl.Buffered(1))


SMEM = pl.BlockSpec(memory_space=pltpu.SMEM)
LIMIT = 67_000_000


def project(first, count, valid, tokens, halo, gain, w_xd, cw, cb, dtb, rate):
    piece = tokens.shape[1]
    chunks = piece // CL
    sds = jax.ShapeDtypeStruct
    return pl.pallas_call(
        partial(project_kernel, first=first),
        grid=(count,),
        in_specs=[
            SMEM,
            per((piece, D), first),
            per((16, D), first),
            whole((1, D)),
            kept((D, XD)),
            whole((DCONV, XBC)),
            whole((1, XBC)),
            whole((1, LN)),
            whole((1, LN)),
        ],
        out_specs=[
            per((piece, D)),
            per((piece + 8, XBC)),
            per((piece, XBC)),
            per((piece, LN)),
            per((piece, LN)),
            per((piece, LN)),
            per((chunks, NS, DI)),
            per((SROWS, DI)),
        ],
        out_shape=[
            sds((count, piece, D), BF),
            sds((count, piece + 8, XBC), F32),
            sds((count, piece, XBC), F32),
            sds((count, piece, LN), F32),
            sds((count, piece, LN), F32),
            sds((count, piece, LN), F32),
            sds((count, chunks, NS, DI), BF),
            sds((count, SROWS, DI), BF),
        ],
        scratch_shapes=[
            pltpu.VMEM((piece + 16, D), BF),
            pltpu.VMEM((CL, DI), BF),
            pltpu.VMEM((NS, DI), F32),
            pltpu.VMEM((2 * LN, DI), BF),
        ],
        compiler_params=pltpu.CompilerParams(vmem_limit_bytes=LIMIT),
        name="project",
    )(valid, tokens, halo, gain, w_xd, cw, cb, dtb, rate)


class Exchange:
    def __init__(self, own, sib, out, got, swap_send, swap_recv, far_send, far_recv, giver):
        dp, seq = lax.axis_index("dp"), lax.axis_index("seq")
        self.x, self.c = seq // 2, seq % 2
        self.sibling = (dp, self.x * 2 + 1 - self.c)
        self.across = (dp, (1 - self.x) * 2 + self.c)
        self.own, self.sib, self.out, self.got = own, sib, out, got
        self.sems = (swap_send, swap_recv, far_send, far_recv)
        self.giver = giver

    def greet(self):
        barrier = pltpu.get_barrier_semaphore()
        for other in (self.sibling, self.across):
            pl.semaphore_signal(barrier, inc=1, device_id=other, device_id_type=pl.DeviceIdType.MESH)
        pl.semaphore_wait(barrier, 2)

    def swap(self, i):
        return pltpu.make_async_remote_copy(
            src_ref=self.own.at[i],
            dst_ref=self.sib.at[i],
            send_sem=self.sems[0].at[i],
            recv_sem=self.sems[1].at[i],
            device_id=self.sibling,
            device_id_type=pl.DeviceIdType.MESH,
        )

    def far(self, i):
        return pltpu.make_async_remote_copy(
            src_ref=self.out.at[i],
            dst_ref=self.got.at[i],
            send_sem=self.sems[2].at[i],
            recv_sem=self.sems[3].at[i],
            device_id=self.across,
            device_id_type=pl.DeviceIdType.MESH,
        )

    def decay(self, ref, i):
        return ref[i, NS : NS + 1].astype(F32) + ref[i, NS + 1 : NS + 2].astype(F32)

    def begin(self, count, coefficients):
        self.greet()
        for i in range(count):
            self.swap(i).start()
        for i in range(count):
            self.swap(i).wait_recv()

            @pl.when(self.x == self.giver)
            def _():
                f, g = coefficients(self.decay(self.own, i), self.decay(self.sib, i))
                self.out[i] = (f * self.own[i, 0:NS].astype(F32) + g * self.sib[i, 0:NS].astype(F32)).astype(BF)
                self.far(i).start()

    def end(self, count):
        for i in range(count):
            self.swap(i).wait_send()

            @pl.when(self.x == self.giver)
            def _():
                self.far(i).wait_send()


def exchange_scratch(count):
    dma = pltpu.SemaphoreType.DMA((count,))
    return [
        pltpu.VMEM((count, SROWS, DI), BF),
        pltpu.VMEM((count, NS, DI), BF),
        pltpu.VMEM((count, NS, DI), BF),
        dma,
        dma,
        dma,
        dma,
    ]


def mix_kernel(
    vlen_ref,
    x_ref,
    cot_ref,
    nrm_ref,
    act_ref,
    step_ref,
    l_ref,
    sloc_ref,
    s_ref,
    wz_ref,
    wo_ref,
    gg_ref,
    dsk_ref,
    out_ref,
    gn_ref,
    dbr_ref,
    dz_ref,
    dy_ref,
    y_ref,
    incoming,
    dsin_ref,
    ggrad_ref,
    zs,
    dgn,
    dsacc,
    yf,
    work,
    e2,
    sib,
    out,
    got,
    *sems,
    first,
    count,
):
    piece = x_ref.shape[0]
    chunks = piece // CL
    section = pl.program_id(0)
    valid = vlen_ref[first + section]
    states = Exchange(s_ref, sib, out, got, *sems, giver=0)
    even = states.c == 0

    @pl.when(section == 0)
    def _():
        ggrad_ref[...] = jnp.zeros_like(ggrad_ref)
        fill_expander(e2)
        states.begin(count, lambda own, sibs: (jnp.where(even, sibs, 1.0), jnp.where(even, 1.0, own)))

    row = lax.broadcasted_iota(jnp.int32, (piece, 1), 0)
    live = row < valid
    dbr_ref[...] = jnp.where(live, cot_ref[...].astype(F32), 0.0).astype(BF)
    for j in range(DI // 256):
        cols = slice(j * 256, (j + 1) * 256)
        zs[:, cols] = nn(nrm_ref[...], wz_ref[:, cols])
        dgn[:, cols] = nt(dbr_ref[...], wo_ref[cols, :])

    @pl.when(states.x == 0)
    def _():
        incoming[...] = jnp.where(even, 0.0, 1.0) * sib[section, 0:NS].astype(F32)

    @pl.when(states.x == 1)
    def _():
        states.far(section).wait_recv()
        f = jnp.where(even, 1.0, states.decay(sib, section))
        incoming[...] = f * got[section].astype(F32) + jnp.where(even, 0.0, 1.0) * sib[section, 0:NS].astype(F32)

    low = lower_mask(False)
    left, right = half_masks()
    dsacc[...] = jnp.zeros_like(dsacc)

    def chunk(k, before):
        base = pl.multiple_of(k * CL, CL)
        rows = pl.ds(base, CL)
        step = step_ref[rows, :]
        ld = l_ref[rows, :]
        ldt = ld.T
        start = (before * incoming[...] + sloc_ref[k].astype(F32)).astype(BF)
        step_e = expand(step, e2)
        grow = expand(jnp.exp(ld), e2)
        b = act_ref[rows, DI : DI + NS].astype(BF)
        c, c_low = halves(act_ref[rows, DI + NS :])
        scores = jnp.where(low, nt(c, b), 0.0)
        squares = jnp.zeros((CL, LN), F32)
        for j in range(DI // LN):
            x = act_ref[rows, lanes(j)]
            xd = (x * step_e[:, lanes(j)]).astype(BF)
            mixes = []
            for h in (2 * j, 2 * j + 1):
                gap = jnp.minimum(ld[:, h : h + 1] - ldt[h : h + 1, :], 0.0)
                mixes.append((jnp.exp(gap) * scores).astype(BF))
            block = jnp.concatenate([xd * left, xd * right], axis=0)
            st = start[:, lanes(j)]
            y = nn(jnp.concatenate(mixes, axis=1), block) + (nn(c, st) + nn(c_low, st)) * grow[:, lanes(j)]
            y_ref[rows, lanes(j)] = y
            full = y + dsk_ref[:, lanes(j)] * x
            yf[:, lanes(j)] = full
            z = zs[rows, lanes(j)]
            u = full * (z * sigmoid(z))
            squares = squares + u * u
        r = lax.rsqrt(jnp.sum(squares, axis=-1, keepdims=True) * (1.0 / DI) + EPSILON)
        inner = jnp.zeros((CL, LN), F32)
        for j in range(DI // LN):
            z = zs[rows, lanes(j)]
            v = yf[:, lanes(j)] * (z * sigmoid(z)) * r
            gain = gg_ref[:, lanes(j)]
            gn_ref[rows, lanes(j)] = (v * gain).astype(BF)
            dg = dgn[rows, lanes(j)]
            gv = dg * v
            ggrad_ref[:, lanes(j)] += jnp.sum(gv.reshape(CL // 8, 8, LN), axis=0)
            inner = inner + gv * gain
        q = jnp.sum(inner, axis=-1, keepdims=True) * (1.0 / DI)
        for j in range(DI // LN):
            z = zs[rows, lanes(j)]
            s = sigmoid(z)
            sz = z * s
            full = yf[:, lanes(j)]
            v = full * sz * r
            du = r * (dgn[rows, lanes(j)] * gg_ref[:, lanes(j)] - v * q)
            dy = du * sz
            dy_ref[rows, lanes(j)] = dy
            dz_ref[rows, lanes(j)] = (du * full * (s + sz * (1.0 - s))).astype(BF)
            work[:, lanes(j)] = (dy * grow[:, lanes(j)]).astype(BF)
        dsacc[...] += before * tn(c, work[...])
        return before * grow[CL - 1 :]

    lax.fori_loop(0, chunks, chunk, jnp.ones((1, DI), F32))
    dsin_ref[0:NS] = dsacc[...].astype(BF)
    dsin_ref[NS:] = s_ref[section, NS:]
    for j in range(D // 256):
        cols = slice(j * 256, (j + 1) * 256)
        branch = nn(gn_ref[...], wo_ref[:, cols])
        out_ref[:, cols] = jnp.where(live, x_ref[:, cols].astype(F32) + branch, 0.0).astype(BF)

    @pl.when(section == count - 1)
    def _():
        states.end(count)


def mix(first, count, valid, tokens, cot, normed, act, step, ld, sloc, s, w_z, w_o, gg, dsk):
    piece = tokens.shape[1]
    chunks = piece // CL
    sds = jax.ShapeDtypeStruct
    return pl.pallas_call(
        partial(mix_kernel, first=first, count=count),
        grid=(count,),
        in_specs=[
            SMEM,
            per((piece, D), first),
            per((piece, D), first),
            per((piece, D)),
            per((piece, XBC)),
            per((piece, LN)),
            per((piece, LN)),
            per((chunks, NS, DI)),
            kept((count, SROWS, DI)),
            kept((D, DI)),
            kept((DI, D)),
            whole((1, DI)),
            whole((1, DI)),
        ],
        out_specs=[
            per((piece, D)),
            per((piece, DI)),
            per((piece, D)),
            per((piece, DI)),
            per((piece, DI)),
            per((piece, DI)),
            per((NS, DI)),
            per((SROWS, DI)),
            whole((8, DI)),
        ],
        out_shape=[
            sds((count, piece, D), BF),
            sds((count, piece, DI), BF),
            sds((count, piece, D), BF),
            sds((count, piece, DI), BF),
            sds((count, piece, DI), F32),
            sds((count, piece, DI), F32),
            sds((count, NS, DI), F32),
            sds((count, SROWS, DI), BF),
            sds((8, DI), F32),
        ],
        scratch_shapes=[
            pltpu.VMEM((piece, DI), F32),
            pltpu.VMEM((piece, DI), F32),
            pltpu.VMEM((NS, DI), F32),
            pltpu.VMEM((CL, DI), F32),
            pltpu.VMEM((CL, DI), BF),
            pltpu.VMEM((2 * LN, DI), BF),
        ]
        + exchange_scratch(count),
        compiler_params=pltpu.CompilerParams(vmem_limit_bytes=LIMIT, collective_id=2, has_side_effects=True),
        name="mix",
    )(valid, tokens, cot, normed, act, step, ld, sloc, s, w_z, w_o, gg, dsk)


def scan_back_kernel(
    ci_ref,
    step_ref,
    l_ref,
    sig_ref,
    dy_ref,
    y_ref,
    inc_ref,
    sloc_ref,
    dsin_ref,
    cw_ref,
    cb_ref,
    rate_ref,
    dsk_ref,
    dxd_ref,
    fix_ref,
    edge_ref,
    cgrad_ref,
    hgrad_ref,
    skip_ref,
    ds,
    xa,
    dsl,
    dact,
    xdt,
    xt,
    dr,
    e2,
    u_top,
    u_low,
    fs,
    vs,
    dyg,
    start,
    sib,
    out,
    got,
    *sems,
    count,
):
    piece = dy_ref.shape[0]
    chunks = piece // CL
    section = pl.program_id(0)
    states = Exchange(dsin_ref, sib, out, got, *sems, giver=1)
    even = states.c == 0
    one_if_even = jnp.where(even, 1.0, 0.0)

    @pl.when(section == 0)
    def _():
        cgrad_ref[...] = jnp.zeros_like(cgrad_ref)
        hgrad_ref[...] = jnp.zeros_like(hgrad_ref)
        skip_ref[...] = jnp.zeros_like(skip_ref)
        fill_expander(e2)
        states.begin(count, lambda own, sibs: (jnp.where(even, 1.0, sibs), jnp.where(even, own, 1.0)))

    @pl.when(states.x == 1)
    def _():
        ds[...] = one_if_even * sib[section, 0:NS].astype(F32)

    @pl.when(states.x == 0)
    def _():
        states.far(section).wait_recv()
        f = jnp.where(even, states.decay(sib, section), 1.0)
        ds[...] = f * got[section].astype(F32) + one_if_even * sib[section, 0:NS].astype(F32)

    upper = jnp.logical_not(lower_mask(True))
    upper_one = jnp.where(upper, 1.0, 0.0)
    before_one = jnp.where(lower_mask(True), 1.0, 0.0)
    left, right = half_masks()
    dr[CL:] = jnp.zeros((8, XBC), F32)

    def chunk(i, carry):
        k = chunks - 1 - i
        base = pl.multiple_of(k * CL, CL)
        rows = pl.ds(base, CL)
        step = step_ref[rows, :]
        ld = l_ref[rows, :]
        ldt = ld.T
        end = ld[CL - 1 :]
        prefix = jnp.zeros((8, LN), F32)
        for j in range(chunks - 1):
            prefix = prefix + jnp.where(j < k, 1.0, 0.0) * l_ref[j * CL + CL - 1 : j * CL + CL, :]
        before = expand(jnp.exp(prefix), e2)[0:1]
        start[...] = before * inc_ref[...] + sloc_ref[k].astype(F32)
        step_e = expand(step, e2)
        grow = expand(jnp.exp(ld), e2)
        tail = expand(jnp.exp(end - ld), e2)
        keep = grow[CL - 1 :]
        for j in range(XBC // LN):
            ext = ci_ref[pl.ds(base, CL + 8), lanes(j)]
            run = conv_running(ext, cw_ref[:, lanes(j)], cb_ref[:, lanes(j)])
            s = sigmoid(run)
            a = run * s
            xa[:, lanes(j)] = a
            dsl[:, lanes(j)] = s + a * (1.0 - s)
            if j < DI // LN:
                xd = a * step_e[:, lanes(j)]
                xdt[:, lanes(j)] = xd
                xt[:, lanes(j)] = xd * tail[:, lanes(j)]
        b = xa[:, DI : DI + NS].astype(BF)
        c = xa[:, DI + NS :].astype(BF)
        scores = jnp.where(upper, nt(b, c), 0.0)
        dact[:, 0:DI] = nn(b, ds[...].astype(BF)) * tail
        dscores = jnp.zeros((CL, CL), F32)
        for j in range(DI // LN):
            dyf = dy_ref[rows, lanes(j)]
            dyb, dyl = halves(dyf)
            block = jnp.concatenate([dyb * left, dyb * right], axis=0)
            block_low = jnp.concatenate([dyl * left, dyl * right], axis=0)
            xdb, xdl = halves(xdt[:, lanes(j)])
            dmix = nt(jnp.concatenate([xdb, xdl], axis=1), jnp.concatenate([block, block], axis=1)) + nt(xdb, block_low)
            mixes = []
            for p, h in enumerate((2 * j, 2 * j + 1)):
                gap = jnp.minimum(ldt[h : h + 1, :] - ld[:, h : h + 1], 0.0)
                w = jnp.exp(gap)
                mixes.append((w * scores).astype(BF))
                dscores = dscores + dmix[:, lanes(p)] * w
            diag = nn(jnp.concatenate(mixes, axis=1), block)
            far = dact[:, lanes(j)]
            xdf = xdb.astype(F32)
            u_top[:, lanes(j)], u_low[:, lanes(j)] = halves(dyb.astype(F32) * y_ref[rows, lanes(j)] - xdf * diag)
            fs[:, lanes(j)] = (xdf * far).astype(BF)
            dxd = diag + far
            x = xa[:, lanes(j)]
            vs[:, lanes(j)] = (x * dxd).astype(BF)
            dact[:, lanes(j)] = dxd * step_e[:, lanes(j)] + dsk_ref[:, lanes(j)] * dyf
            skip_ref[:, lanes(j)] += jnp.sum((dyf * x).reshape(CL // 8, 8, LN), axis=0)
            dyg[:, lanes(j)] = dyf * grow[:, lanes(j)]
        e = e2[0:LN]
        const = jnp.sum((start[...] * ds[...]).reshape(NS // 8, 8, DI), axis=0) * keep
        c_top, c_low = halves(const)
        r_c = jnp.sum(nt(c_top, e) + nt(c_low, e), axis=0, keepdims=True)
        r_u = nt(u_top[...], e) + nt(u_low[...], e)
        r_f = nt(fs[...], e)
        r_v = nt(vs[...], e)
        db = three(nt, xt[...], ds[...])
        dc = three(nt, dyg[...], start[...])
        ds[...] = keep * ds[...] + tn(c, dyg[...].astype(BF))
        dsc = jnp.where(upper, dscores, 0.0).astype(BF)
        dact[:, DI : DI + NS] = db + nn(dsc, c)
        dact[:, DI + NS :] = dc + tn(dsc, b)
        da = exact_nn(upper_one, r_u) + exact_nn(before_one, r_f) + r_c
        dstep = r_v + rate_ref[...] * da
        ddt = dstep * sig_ref[rows, :]
        hgrad_ref[0:8] += jnp.sum(ddt.reshape(CL // 8, 8, LN), axis=0)
        hgrad_ref[8:16] += jnp.sum((da * step).reshape(CL // 8, 8, LN), axis=0)
        dxd_ref[rows, XBC:] = ddt.astype(BF)
        for j in range(XBC // LN):
            g = dact[:, lanes(j)] * dsl[:, lanes(j)]
            dr[0:CL, lanes(j)] = g
            ci = ci_ref[pl.ds(base + 8, CL), lanes(j)]
            gext = dr[:, lanes(j)]
            total = jnp.zeros((CL, LN), F32)
            for tap in range(DCONV):
                later = DCONV - 1 - tap
                shifted = gext[later : later + CL] if later else g
                total = total + shifted * cw_ref[tap : tap + 1, lanes(j)]
                cgrad_ref[8 * tap : 8 * tap + 8, lanes(j)] += jnp.sum((shifted * ci).reshape(CL // 8, 8, LN), axis=0)
            cgrad_ref[32:40, lanes(j)] += jnp.sum(g.reshape(CL // 8, 8, LN), axis=0)
            dxd_ref[rows, lanes(j)] = total.astype(BF)

            @pl.when(i == 0)
            def _():
                fix_ref[:, lanes(j)] = total[CL - 16 :]

            dr[CL:, lanes(j)] = g[0:8]
        return carry

    lax.fori_loop(0, chunks, chunk, 0)
    edge_ref[...] = dr[CL:]
    for tap in range(DCONV - 1):
        later = DCONV - 1 - tap
        part = dr[CL : CL + later] * ci_ref[8 - later : 8]
        cgrad_ref[8 * tap : 8 * tap + 1] += jnp.sum(part, axis=0, keepdims=True)

    @pl.when(section == count - 1)
    def _():
        states.end(count)


def scan_back(count, ci, step, ld, sig, dy, y, inc, sloc, dsin, cw, cb, rate, dsk):
    piece = dy.shape[1]
    chunks = piece // CL
    sds = jax.ShapeDtypeStruct
    return pl.pallas_call(
        partial(scan_back_kernel, count=count),
        grid=(count,),
        in_specs=[
            per((piece + 8, XBC)),
            per((piece, LN)),
            per((piece, LN)),
            per((piece, LN)),
            per((piece, DI)),
            per((piece, DI)),
            per((NS, DI)),
            per((chunks, NS, DI)),
            kept((count, SROWS, DI)),
            whole((DCONV, XBC)),
            whole((1, XBC)),
            whole((1, LN)),
            whole((1, DI)),
        ],
        out_specs=[
            per((piece, XD)),
            per((16, XBC)),
            per((8, XBC)),
            whole((40, XBC)),
            whole((16, LN)),
            whole((8, DI)),
        ],
        out_shape=[
            sds((count, piece, XD), BF),
            sds((count, 16, XBC), F32),
            sds((count, 8, XBC), F32),
            sds((40, XBC), F32),
            sds((16, LN), F32),
            sds((8, DI), F32),
        ],
        scratch_shapes=[
            pltpu.VMEM((NS, DI), F32),
            pltpu.VMEM((CL, XBC), F32),
            pltpu.VMEM((CL, XBC), F32),
            pltpu.VMEM((CL, XBC), F32),
            pltpu.VMEM((CL, DI), F32),
            pltpu.VMEM((CL, DI), F32),
            pltpu.VMEM((CL + 8, XBC), F32),
            pltpu.VMEM((2 * LN, DI), BF),
            pltpu.VMEM((CL, DI), BF),
            pltpu.VMEM((CL, DI), BF),
            pltpu.VMEM((CL, DI), BF),
            pltpu.VMEM((CL, DI), BF),
            pltpu.VMEM((CL, DI), F32),
            pltpu.VMEM((NS, DI), F32),
        ]
        + exchange_scratch(count),
        compiler_params=pltpu.CompilerParams(vmem_limit_bytes=LIMIT, collective_id=3, has_side_effects=True),
        name="scan_back",
    )(ci, step, ld, sig, dy, y, inc, sloc, dsin, cw, cb, rate, dsk)


def input_grad_kernel(x_ref, dbr_ref, g_ref, dz_ref, dxd_ref, wz_ref, wx_ref, out_ref, gain_ref, dn):
    piece = x_ref.shape[0]

    @pl.when(pl.program_id(0) == 0)
    def _():
        gain_ref[...] = jnp.zeros_like(gain_ref)

    for j in range(D // 256):
        cols = slice(j * 256, (j + 1) * 256)
        dn[:, cols] = nt(dz_ref[...], wz_ref[cols, :]) + nt(dxd_ref[...], wx_ref[cols, :])

    def rows_of(i, c):
        rows = pl.ds(pl.multiple_of(i * 64, 64), 64)
        x = x_ref[rows, :].astype(F32)
        d = dn[rows, :]
        r = lax.rsqrt(jnp.mean(x * x, axis=-1, keepdims=True) + EPSILON)
        v = x * r
        gain_ref[...] += jnp.sum((d * v).reshape(8, 8, D), axis=0)
        dv = d * g_ref[...]
        q = jnp.mean(dv * v, axis=-1, keepdims=True)
        out_ref[rows, :] = (dbr_ref[rows, :].astype(F32) + r * (dv - v * q)).astype(BF)
        return c

    lax.fori_loop(0, piece // 64, rows_of, 0)


def input_grad(first, count, tokens, dbr, gain, dz, dxd, w_z, w_xd):
    piece = tokens.shape[1]
    sds = jax.ShapeDtypeStruct
    return pl.pallas_call(
        input_grad_kernel,
        grid=(count,),
        in_specs=[
            per((piece, D), first),
            per((piece, D)),
            whole((1, D)),
            per((piece, DI)),
            per((piece, XD)),
            kept((D, DI)),
            kept((D, XD)),
        ],
        out_specs=[per((piece, D)), whole((8, D))],
        out_shape=[sds((count, piece, D), BF), sds((8, D), F32)],
        scratch_shapes=[pltpu.VMEM((piece, D), F32)],
        compiler_params=pltpu.CompilerParams(vmem_limit_bytes=LIMIT),
        name="input_grad",
    )(tokens, dbr, gain, dz, dxd, w_z, w_xd)


MESH_ID = pl.DeviceIdType.MESH


class Here:
    def __init__(self, depth):
        dp, seq = lax.axis_index("dp"), lax.axis_index("seq")
        self.depth = depth
        self.levels = depth.bit_length() - 1
        self.z, self.y = dp // 2, dp % 2
        self.x, self.c = seq // 2, seq % 2
        self.rank = dp * 4 + seq

    def device(self, z=None, y=None, x=None, c=None):
        z = self.z if z is None else z
        y = self.y if y is None else y
        x = self.x if x is None else x
        c = self.c if c is None else c
        return (z * 2 + y, x * 2 + c)

    def across(self, level):
        size = 1 << level
        return self.z + size * (1 - 2 * ((self.z // size) % 2))

    def block(self, level):
        size = 1 << level
        return (self.z // size) * size, size

    def block_across(self, level):
        size = 1 << level
        return (self.z // size) * size + size * (1 - 2 * ((self.z // size) % 2)), size

    def greet(self, ranks):
        barrier = pltpu.get_barrier_semaphore()

        def hail(i, carry):
            other = (self.rank + i) % ranks
            pl.semaphore_signal(
                barrier, inc=1, device_id=(other // 4, other % 4), device_id_type=MESH_ID
            )
            return carry

        lax.fori_loop(1, ranks, hail, 0)
        pl.semaphore_wait(barrier, ranks - 1)


class Copies:
    def __init__(self, send, recv):
        self.send, self.recv, self.made = send, recv, []

    def start(self, pairs, device):
        waits = []
        for source, target, landing in pairs:
            i = len(self.made)
            copy = pltpu.make_async_remote_copy(
                src_ref=source,
                dst_ref=target,
                send_sem=self.send.at[i],
                recv_sem=self.recv.at[i],
                device_id=device,
                device_id_type=MESH_ID,
            )
            copy.start()
            self.made.append(copy)
            waits.append(
                pltpu.make_async_remote_copy(
                    src_ref=source,
                    dst_ref=landing,
                    send_sem=self.send.at[i],
                    recv_sem=self.recv.at[i],
                    device_id=device,
                    device_id_type=MESH_ID,
                )
            )
        return waits

    def finish(self):
        for copy in self.made:
            copy.wait_send()


def arrived(waits):
    for w in waits:
        w.wait_recv()


BOTH = slice(None)


def at(item, z, y, x, c):
    ref, half = item
    index = (z, y, x, c)
    return ref.at[index if half is None else index + (half,)]


def everyone(rank, ranks, source, target, send, recv, own):
    def one(i, starting):
        other = (rank + i) % ranks
        copy = pltpu.make_async_remote_copy(
            src_ref=source(other),
            dst_ref=target(rank),
            send_sem=send.at[i],
            recv_sem=recv.at[i],
            device_id=(other // 4, other % 4),
            device_id_type=MESH_ID,
        )
        return copy

    def begin(i, carry):
        one(i, True).start()
        return carry

    def end(i, carry):
        copy = one(i, False)
        copy.wait_send()
        copy.wait_recv()
        return carry

    def start():
        lax.fori_loop(1, ranks, begin, 0)

    def finish():
        lax.fori_loop(1, ranks, end, 0)

    return start, finish


def gather_stream(here, copies, items, first):
    z, y, x, c = here.z, here.y, here.x, here.c
    a_dev = here.device(x=1 - x) if first == "x" else here.device(y=1 - y)
    b_dev = here.device(y=1 - y) if first == "x" else here.device(x=1 - x)
    sibling = here.device(c=1 - c)
    cores = []

    def a_there(item, zs, core):
        return at(item, zs, y, 1 - x, core) if first == "x" else at(item, zs, 1 - y, x, core)

    def line(item, zs, core):
        return at(item, zs, y, BOTH, core) if first == "x" else at(item, zs, BOTH, x, core)

    def line_there(item, zs, core):
        return at(item, zs, 1 - y, BOTH, core) if first == "x" else at(item, zs, BOTH, 1 - x, core)

    def same(where, zs):
        return [(where(i, zs, c), where(i, zs, c), where(i, zs, 1 - c)) for i in items]

    def to_core(where, zs):
        cores.extend(copies.start(same(where, zs), sibling))

    def mine(item, zs, core):
        return at(item, zs, y, x, core)

    def start_a(zs):
        waits = copies.start([(mine(i, zs, c), mine(i, zs, c), a_there(i, zs, c)) for i in items], a_dev)
        to_core(mine, zs)
        return waits

    def start_b(zs, waits):
        arrived(waits)
        out = copies.start([(line(i, zs, c), line(i, zs, c), line_there(i, zs, c)) for i in items], b_dev)
        to_core(a_there, zs)
        return out

    def end_b(zs, waits):
        arrived(waits)
        to_core(line_there, zs)

    sets = [pl.ds(z, 1)]
    waiting_a, waiting_b = [], []
    for level in range(here.levels):
        base, size = here.block(level)
        far, _ = here.block_across(level)
        own, theirs = pl.ds(base, size), pl.ds(far, size)
        zwait = copies.start(
            [(mine(i, own, c), mine(i, own, c), mine(i, theirs, c)) for i in items],
            here.device(z=here.across(level)),
        )
        waiting_a.append((sets[-1], start_a(sets[-1])))
        sets.append(theirs)
        yield
        if level:
            zs, w = waiting_a.pop(0)
            waiting_b.append((zs, start_b(zs, w)))
            yield
        arrived(zwait)
    waiting_a.append((sets[-1], start_a(sets[-1])))
    while waiting_a:
        yield
        zs, w = waiting_a.pop(0)
        waiting_b.append((zs, start_b(zs, w)))
    while waiting_b:
        yield
        zs, w = waiting_b.pop(0)
        end_b(zs, w)
    yield
    arrived(cores)


def side_by_side(streams):
    streams = list(streams)
    while streams:
        for s in list(streams):
            try:
                next(s)
            except StopIteration:
                streams.remove(s)


def gather_kernel(
    xd_in, z_in, o_in, small_in, xd_out, z_out, o_out, small_out, send, recv, ssend, srecv, place_sem, *, depth, ranks
):
    here = Here(depth)
    z, y, x, c = here.z, here.y, here.x, here.c
    own = []
    for i, (source, target) in enumerate(((xd_in, xd_out), (z_in, z_out), (o_in, o_out))):
        own.append(pltpu.make_async_copy(source, target.at[z, y, x, c], place_sem.at[i]))
    own.append(pltpu.make_async_copy(small_in, small_out.at[here.rank], place_sem.at[3]))
    for copy in own:
        copy.start()
    here.greet(ranks)
    start, finish = everyone(
        here.rank, ranks, lambda other: small_in, lambda rank: small_out.at[rank], ssend, srecv, None
    )
    for copy in own:
        copy.wait()
    copies = Copies(send, recv)
    streams = [
        gather_stream(here, copies, [(xd_out, None), (o_out, 0)], "x"),
        gather_stream(here, copies, [(z_out, None), (o_out, 1)], "y"),
    ]
    start()
    side_by_side(streams)
    finish()
    copies.finish()


def copies_needed(levels):
    return 2 * 2 * (levels + 5 * (levels + 1))


def gather(xd, wz, wo, small, depth):
    ranks = depth * 8
    lead = (depth, 2, 2, 2)
    sds = jax.ShapeDtypeStruct
    n = copies_needed(depth.bit_length() - 1)
    any_space = pl.BlockSpec(memory_space=pl.ANY)
    in_vmem = pl.BlockSpec(memory_space=pltpu.VMEM)
    dma = pltpu.SemaphoreType.DMA
    return pl.pallas_call(
        partial(gather_kernel, depth=depth, ranks=ranks),
        in_specs=[in_vmem] * 4,
        out_specs=[any_space] * 4,
        out_shape=[sds(lead + a.shape, a.dtype) for a in (xd, wz, wo)] + [sds((ranks,) + small.shape, small.dtype)],
        scratch_shapes=[dma((n,)), dma((n,)), dma((ranks,)), dma((ranks,)), dma((4,))],
        compiler_params=pltpu.CompilerParams(collective_id=0, has_side_effects=True),
        name="gather",
    )(xd, wz, wo, small)


def reduce_stream(here, copies, items, first):
    z, y, x, c = here.z, here.y, here.x, here.c
    one_dev = here.device(y=1 - y) if first == "y" else here.device(x=1 - x)
    two_dev = here.device(x=1 - x) if first == "y" else here.device(y=1 - y)
    sibling = here.device(c=1 - c)

    def part(item, zs, core):
        return at((item[0], item[1]), zs, BOTH, BOTH, core)

    def keep_line(zs):
        return (zs, y, BOTH) if first == "y" else (zs, BOTH, x)

    def give_line(zs):
        return (zs, 1 - y, BOTH) if first == "y" else (zs, BOTH, 1 - x)

    def give_one(zs):
        return (zs, y, 1 - x) if first == "y" else (zs, 1 - y, x)

    def keep_one(zs):
        return (zs, y, x)

    sets = []
    for level in reversed(range(here.levels)):
        far, size = here.block_across(level)
        sets.append((far, size))
    sets.append((z, 1))

    def slots(zs):
        return pl.ds(zs[0], zs[1])

    def over(zs, body):
        for k in range(zs[1]):
            body(zs[0] + k)

    def core_phase(zs):
        s = slots(zs)
        return copies.start([(part(i, s, 1 - c), i[3].at[s], i[3].at[s]) for i in items], sibling)

    def line_phase(zs, waits):
        arrived(waits)

        def add(k):
            for item in items:
                for a in range(2):
                    for b in range(2):
                        index = (k, a, b, c) if item[1] is None else (k, a, b, c, item[1])
                        item[2][k, a, b] = (item[0][index].astype(F32) + item[3][k, a, b].astype(F32)).astype(BF)

        over(zs, add)
        s = slots(zs)
        return copies.start([(i[2].at[give_line(s)], i[4].at[s], i[4].at[s]) for i in items], one_dev)

    def side_phase(zs, waits):
        arrived(waits)

        def add(k):
            for item in items:
                for a in range(2):
                    index = (k, y, a) if first == "y" else (k, a, x)
                    item[2][index] = (item[2][index].astype(F32) + item[4][k, a].astype(F32)).astype(BF)

        over(zs, add)
        s = slots(zs)
        return copies.start([(i[2].at[give_one(s)], i[5].at[s], i[5].at[s]) for i in items], two_dev)

    def last_phase(zs, waits):
        arrived(waits)

        def add(k):
            for item in items:
                item[2][k, y, x] = (item[2][k, y, x].astype(F32) + item[5][k].astype(F32)).astype(BF)

        over(zs, add)

    cores = [core_phase(zs) for zs in sets]
    yield
    lines, sides = [], []
    n = len(sets)
    for step in range(n + 2):
        if step < n:
            lines.append(line_phase(sets[step], cores[step]))
            yield
        if 1 <= step <= n:
            sides.append(side_phase(sets[step - 1], lines[step - 1]))
            yield
        if step >= 2:
            last_phase(sets[step - 2], sides[step - 2])
            if step == 2:
                level = here.levels - 1
                far, size = here.block_across(level)
                base, _ = here.block(level)
                s, own = pl.ds(far, size), pl.ds(base, size)
                zwait = copies.start(
                    [(i[2].at[s, y, x], i[6][0].at[0:size], i[6][0].at[0:size]) for i in items],
                    here.device(z=here.across(level)),
                )
            yield
    for depth_at, level in enumerate(reversed(range(here.levels))):
        size = 1 << level
        base, _ = here.block(level)
        arrived(zwait)
        for k in range(size):
            for item in items:
                got = item[6][depth_at][k].astype(F32) + item[2][base + k, y, x].astype(F32)
                if level:
                    item[2][base + k, y, x] = got.astype(BF)
                else:
                    item[7](got)
        if level:
            size = 1 << (level - 1)
            far, _ = here.block_across(level - 1)
            zwait = copies.start(
                [
                    (i[2].at[pl.ds(far, size), y, x], i[6][depth_at + 1].at[0:size], i[6][depth_at + 1].at[0:size])
                    for i in items
                ],
                here.device(z=here.across(level - 1)),
            )
            yield


def reduce_kernel(*refs, depth, ranks, names):
    here = Here(depth)
    levels = here.levels
    count = len(names)
    parts = refs[:count]
    small_in = refs[count]
    outs = refs[count + 1 : 2 * count + 1]
    small_out = refs[2 * count + 1]
    scratch = list(refs[2 * count + 2 :])
    send, recv, ssend, srecv, small_got = scratch[:5]
    scratch = scratch[5:]
    here.greet(ranks)
    start, finish = everyone(
        here.rank, ranks, lambda other: small_in.at[other], lambda rank: small_got.at[rank], ssend, srecv, None
    )
    start()
    copies = Copies(send, recv)
    streams = []
    at_scratch = 0
    for first, members in (("y", [m for m in STREAM_Y if m[0] in names]), ("x", [m for m in STREAM_X if m[0] in names])):
        items = []
        for name, half in members:
            k = names.index(name)
            acc, core_in, line_in, side_in = scratch[at_scratch : at_scratch + 4]
            z_in = scratch[at_scratch + 4 : at_scratch + 4 + levels]
            at_scratch += 4 + levels

            def put(v, k=k, half=half):
                if half is None:
                    outs[k][...] = v
                else:
                    outs[k][half] = v

            items.append((parts[k], half, acc, core_in, line_in, side_in, z_in, put))
        if items:
            streams.append(reduce_stream(here, copies, items, first))
    side_by_side(streams)
    finish()

    def add(i, total):
        return total + jnp.where(i == here.rank, small_in[i], small_got[i])

    small_out[...] = lax.fori_loop(0, ranks, add, jnp.zeros(small_out.shape, F32))
    copies.finish()


STREAM_Y = [("xd", None), ("o", 0)]
STREAM_X = [("z", None), ("o", 1)]


def reduce(parts, small, depth, ident):
    ranks = depth * 8
    levels = depth.bit_length() - 1
    names = list(parts)
    arrays = [parts[n] for n in names]
    sds = jax.ShapeDtypeStruct
    dma = pltpu.SemaphoreType.DMA
    in_vmem = pl.BlockSpec(memory_space=pltpu.VMEM)
    n = 2 * 2 * (3 * (levels + 1) + levels)
    scratch = [dma((n,)), dma((n,)), dma((ranks,)), dma((ranks,)), pltpu.VMEM(small.shape, F32)]
    for name, half in [m for m in STREAM_Y + STREAM_X if m[0] in names]:
        tile = parts[name].shape[-2:]
        scratch.append(pltpu.VMEM((depth, 2, 2) + tile, BF))
        scratch.append(pltpu.VMEM((depth, 2, 2) + tile, BF))
        scratch.append(pltpu.VMEM((depth, 2) + tile, BF))
        scratch.append(pltpu.VMEM((depth,) + tile, BF))
        for level in reversed(range(levels)):
            scratch.append(pltpu.VMEM((1 << level,) + tile, BF))
    return pl.pallas_call(
        partial(reduce_kernel, depth=depth, ranks=ranks, names=names),
        in_specs=[in_vmem] * (len(arrays) + 1),
        out_specs=[in_vmem] * (len(arrays) + 1),
        out_shape=[sds(a.shape[4:], F32) for a in arrays] + [sds(small.shape[1:], F32)],
        scratch_shapes=scratch,
        compiler_params=pltpu.CompilerParams(collective_id=ident, has_side_effects=True, vmem_limit_bytes=LIMIT),
        name="reduce",
    )(*arrays, small)


def pass_on(block, axis, distance):
    devices = range(lax.axis_size(axis))
    route = [(i - distance, i) for i in devices if i - distance in devices]
    return lax.ppermute(block, axis, route)


def contract_rows(left, right):
    return lax.dot_general(left, right, (((0, 1), (0, 1)), ((), ())), preferred_element_type=F32)


def local(
    tokens,
    norm_gain,
    w_in,
    conv_weight,
    conv_bias,
    dt_bias,
    a_log,
    d_skip,
    gated_gain,
    w_out,
    lengths,
    cotangent,
):
    ranks = lax.axis_size("dp") * lax.axis_size("seq")
    place = lax.axis_index("seq")
    tokens = tokens[:, 0]
    cot = cotangent[:, 0]
    batches, piece, _ = tokens.shape
    rows = w_in.shape[0]

    depth = lax.axis_size("dp") // 2
    n0, n1, n2 = norm_gain.shape[0], gated_gain.shape[0], conv_bias.shape[0]
    small = jnp.concatenate([norm_gain, gated_gain, conv_bias, conv_weight.reshape(-1)])
    small = jnp.pad(small, (0, 8 * LN - small.shape[0])).reshape(8, LN)
    w_low = w_in.astype(BF)
    w_xd = jnp.pad(w_low[:, DI:], ((0, 0), (0, XD - (PROJ - DI))))
    w_xd, w_z, w_o, small = gather(w_xd, w_low[:, :DI], w_out.astype(BF).reshape(2, n1 // 2, D), small, depth)
    w_xd, w_z, w_o = w_xd.reshape(D, XD), w_z.reshape(D, DI), w_o.reshape(DI, D)
    small = small.reshape(ranks, 8 * LN)
    gain = small[:, :n0].reshape(1, D)
    gg = small[:, n0 : n0 + n1].reshape(1, DI)
    cb = small[:, n0 + n1 : n0 + n1 + n2].reshape(1, XBC)
    cw = small[:, n0 + n1 + n2 : n0 + n1 + 5 * n2].reshape(ranks, DCONV, n2).transpose(1, 0, 2).reshape(DCONV, XBC)

    halo = pass_on(tokens[:, piece - 16 :], "seq", 1)
    valid = lengths[:, 0].astype(jnp.int32) - place.astype(jnp.int32) * piece
    lane_pad = ((0, 0), (0, LN - NH))
    dtb = jnp.pad(dt_bias[None], lane_pad)
    rate = -jnp.exp(a_log)
    rate_row = jnp.pad(rate[None], lane_pad)
    dsk = jnp.repeat(d_skip, HD)[None]

    first, count = 0, batches
    normed, ci, act, step, ld, sig, sloc, s = project(
        first, count, valid, tokens, halo, gain, w_xd, cw, cb, dtb, rate_row
    )
    out, gn, dbr, dz, dy, y, inc, dsin, ggrad = mix(
        first, count, valid, tokens, cot, normed, act, step, ld, sloc, s, w_z, w_o, gg, dsk
    )
    dxd, fix, edge, cgrad, hgrad, skip = scan_back(
        count, ci, step, ld, sig, dy, y, inc, sloc, dsin, cw, cb, rate_row, dsk
    )
    next_edge = pass_on(edge, "seq", -1)[:, : DCONV - 1]
    late = []
    for j in range(DCONV - 1):
        late.append(sum(cw[t][None] * next_edge[:, j - t] for t in range(j + 1)))
    late = jnp.stack(late, axis=1)
    fixed = fix.at[:, 16 - (DCONV - 1) :].add(late).astype(BF)
    dxd = dxd.at[:, piece - 16 :, :XBC].set(fixed)
    tgrad, gain_grad = input_grad(first, count, tokens, dbr, gain, dz, dxd, w_z, w_xd)

    grad_wo = contract_rows(gn, dbr)
    grad_wz = contract_rows(normed, dz)
    grad_wx = contract_rows(normed, dxd)
    lead = (depth, 2, 2, 2)
    grad_cw = cgrad[:32].reshape(DCONV, 8, XBC).sum(1)
    heads = hgrad.reshape(2, 8, LN).sum(1)[:, :NH]
    heads = jnp.concatenate([heads[0], heads[1] * rate, skip.sum(0).reshape(NH, HD).sum(1)])
    packed = jnp.concatenate(
        [
            gain_grad.sum(0).reshape(ranks, n0),
            ggrad.sum(0).reshape(ranks, n1),
            cgrad[32:].sum(0).reshape(ranks, n2),
            grad_cw.reshape(DCONV, ranks, n2).transpose(1, 0, 2).reshape(ranks, DCONV * n2),
            jnp.broadcast_to(heads[None], (ranks, 3 * NH)),
        ],
        axis=1,
    )
    used = packed.shape[1]
    packed = jnp.pad(packed, ((0, 0), (0, 8 * LN - used))).reshape(ranks, 8, LN)
    parts = {
        "xd": grad_wx.astype(BF).reshape(lead + (rows, XD)),
        "z": grad_wz.astype(BF).reshape(lead + (rows, DI)),
        "o": grad_wo.astype(BF).reshape(lead + (2, n1 // 2, D)),
    }
    shard_wx, shard_wz, shard_wo, total = reduce(parts, packed, depth, 1)
    shard_win = jnp.concatenate([shard_wz, shard_wx[:, : PROJ - DI]], axis=1)
    total = total.reshape(-1)[:used]
    sizes = [n0, n1, n2, DCONV * n2, NH, NH, NH]
    starts = [sum(sizes[:i]) for i in range(len(sizes))]
    mine = [total[a : a + n] for a, n in zip(starts, sizes)]
    return (
        out[:, None],
        tgrad[:, None],
        mine[0],
        shard_win,
        mine[3].reshape(DCONV, n2),
        mine[2],
        mine[4],
        mine[5],
        mine[6],
        mine[1],
        shard_wo.reshape(n1, D),
    )


def solution(mesh):
    shard = P(("dp", "seq"))
    row_shard = P(("dp", "seq"), None)
    col_shard = P(None, ("dp", "seq"))
    acts = P(None, "dp", "seq", None)
    return jax.shard_map(
        local,
        mesh=mesh,
        in_specs=(
            acts,
            shard,
            row_shard,
            col_shard,
            shard,
            P(),
            P(),
            P(),
            shard,
            row_shard,
            P(None, "dp"),
            acts,
        ),
        out_specs=(
            acts,
            acts,
            shard,
            row_shard,
            col_shard,
            shard,
            P(),
            P(),
            P(),
            shard,
            row_shard,
        ),
        check_vma=False,
    )
```

```python
from functools import partial

import jax
import jax.numpy as jnp
from jax import lax
from jax.experimental import pallas as pl
from jax.experimental.pallas import tpu as pltpu
from jax.sharding import PartitionSpec as P

D = 768
NH = 24
HD = 64
NS = 128
DCONV = 4
CL = 128
DI = 1536
XBC = 1792
PROJ = 3352
XD = 1920
XA = 1024
LN = 128
EPSILON = 1e-05

F32 = jnp.float32
BF = jnp.bfloat16
SROWS = 144


def nn(a, b):
    return lax.dot_general(a, b, (((1,), (0,)), ((), ())), preferred_element_type=F32)


def nt(a, b):
    return lax.dot_general(a, b, (((1,), (1,)), ((), ())), preferred_element_type=F32)


def tn(a, b):
    return lax.dot_general(a, b, (((0,), (0,)), ((), ())), preferred_element_type=F32)


def exact_nn(a, b):
    return lax.dot_general(
        a, b, (((1,), (0,)), ((), ())), precision=lax.Precision.HIGHEST, preferred_element_type=F32
    )


def sigmoid(v):
    return 0.5 * jnp.tanh(0.5 * v) + 0.5


def halves(v):
    top = v.astype(BF)
    return top, (v - top.astype(F32)).astype(BF)


def three(op, a, b):
    ah, al = halves(a)
    bh, bl = halves(b)
    return op(ah, bh) + op(al, bh) + op(ah, bl)


def fill_expander(ref):
    head = lax.broadcasted_iota(jnp.int32, (LN, DI), 0)
    lane = lax.broadcasted_iota(jnp.int32, (LN, DI), 1)
    e = jnp.where(head == lane // HD, 1.0, 0.0).astype(BF)
    ref[0:LN] = e
    ref[LN:] = e


def expand(v, e2):
    return nn(jnp.concatenate(halves(v), axis=1), e2[...])


def lower_mask(strict):
    row = lax.broadcasted_iota(jnp.int32, (CL, CL), 0)
    col = lax.broadcasted_iota(jnp.int32, (CL, CL), 1)
    return row > col if strict else row >= col


def half_masks():
    lane = lax.broadcasted_iota(jnp.int32, (1, 2 * HD), 1)
    left = jnp.where(lane < HD, 1.0, 0.0).astype(BF)
    right = jnp.where(lane < HD, 0.0, 1.0).astype(BF)
    return left, right


def lanes(j):
    return slice(j * LN, (j + 1) * LN)


def conv_running(ci_ref, j, base, cw, cb):
    total = cb
    for tap in range(DCONV):
        total = total + ci_ref[j, pl.ds(base + 5 + tap, CL), :] * cw[tap : tap + 1]
    return total


MESH_ID = pl.DeviceIdType.MESH
BOTH = slice(None)


class Here:
    def __init__(self, depth):
        dp, seq = lax.axis_index("dp"), lax.axis_index("seq")
        self.depth = depth
        self.levels = depth.bit_length() - 1
        self.z, self.y = dp // 2, dp % 2
        self.x, self.c = seq // 2, seq % 2
        self.rank = dp * 4 + seq

    def device(self, z=None, y=None, x=None, c=None):
        z = self.z if z is None else z
        y = self.y if y is None else y
        x = self.x if x is None else x
        c = self.c if c is None else c
        return (z * 2 + y, x * 2 + c)

    def across(self, level):
        size = 1 << level
        return self.z + size * (1 - 2 * ((self.z // size) % 2))

    def block(self, level):
        size = 1 << level
        return (self.z // size) * size, size

    def block_across(self, level):
        size = 1 << level
        return (self.z // size) * size + size * (1 - 2 * ((self.z // size) % 2)), size

    def partners(self):
        near = [self.device(c=1 - self.c), self.device(x=1 - self.x), self.device(y=1 - self.y)]
        return near + [self.device(z=self.across(level)) for level in range(self.levels)]

    def greet_partners(self):
        barrier = pltpu.get_barrier_semaphore()
        others = self.partners()
        for other in others:
            pl.semaphore_signal(barrier, inc=1, device_id=other, device_id_type=MESH_ID)
        pl.semaphore_wait(barrier, len(others))

    def greet_all(self, ranks):
        barrier = pltpu.get_barrier_semaphore()

        def hail(i, carry):
            other = (self.rank + i) % ranks
            pl.semaphore_signal(barrier, inc=1, device_id=(other // 4, other % 4), device_id_type=MESH_ID)
            return carry

        lax.fori_loop(1, ranks, hail, 0)
        pl.semaphore_wait(barrier, ranks - 1)


class Plan:
    def __init__(self, send, recv):
        self.send, self.recv, self.made, self.segments = send, recv, [], [[]]

    def do(self, action):
        self.segments[-1].append(action)

    def copy(self, i, source, target, device):
        return pltpu.make_async_remote_copy(
            src_ref=source,
            dst_ref=target,
            send_sem=self.send.at[i],
            recv_sem=self.recv.at[i],
            device_id=device,
            device_id_type=MESH_ID,
        )

    def start(self, parts, device):
        waits = []
        for source, target, landing in parts:
            i = len(self.made)
            copy = self.copy(i, source, target, device)
            self.do(copy.start)
            self.made.append(copy)
            waits.append(self.copy(i, source, landing, device))
        return waits

    def arrived(self, waits):
        for w in waits:
            self.do(w.wait_recv)

    def trace(self, streams):
        streams = list(streams)
        while streams:
            for stream in list(streams):
                try:
                    next(stream)
                except StopIteration:
                    streams.remove(stream)
            self.segments.append([])

    def run(self, n):
        for action in self.segments[n]:
            action()

    def run_from(self, n):
        for k in range(n, len(self.segments)):
            self.run(k)
        for copy in self.made:
            copy.wait_send()


def everyone(rank, ranks, source, target, send, recv):
    def one(i):
        other = (rank + i) % ranks
        return pltpu.make_async_remote_copy(
            src_ref=source(other),
            dst_ref=target(rank),
            send_sem=send.at[i],
            recv_sem=recv.at[i],
            device_id=(other // 4, other % 4),
            device_id_type=MESH_ID,
        )

    def begin(i, carry):
        one(i).start()
        return carry

    def end(i, carry):
        copy = one(i)
        copy.wait_send()
        copy.wait_recv()
        return carry

    return (lambda: lax.fori_loop(1, ranks, begin, 0)), (lambda: lax.fori_loop(1, ranks, end, 0))


def gather_stream(here, plan, ref, first):
    z, y, x, c = here.z, here.y, here.x, here.c
    a_dev = here.device(x=1 - x) if first == "x" else here.device(y=1 - y)
    b_dev = here.device(y=1 - y) if first == "x" else here.device(x=1 - x)
    sibling = here.device(c=1 - c)
    cores = []

    def mine(zs, core):
        return ref.at[zs, y, x, core]

    def a_there(zs, core):
        return ref.at[zs, y, 1 - x, core] if first == "x" else ref.at[zs, 1 - y, x, core]

    def line(zs, core):
        return ref.at[zs, y, BOTH, core] if first == "x" else ref.at[zs, BOTH, x, core]

    def line_there(zs, core):
        return ref.at[zs, 1 - y, BOTH, core] if first == "x" else ref.at[zs, BOTH, 1 - x, core]

    def to_core(where, zs):
        cores.extend(plan.start([(where(zs, c), where(zs, c), where(zs, 1 - c))], sibling))

    def start_a(zs):
        waits = plan.start([(mine(zs, c), mine(zs, c), a_there(zs, c))], a_dev)
        to_core(mine, zs)
        return waits

    def start_b(zs, waits):
        plan.arrived(waits)
        out = plan.start([(line(zs, c), line(zs, c), line_there(zs, c))], b_dev)
        to_core(a_there, zs)
        return out

    sets = [pl.ds(z, 1)]
    waiting_a, waiting_b = [], []
    for level in range(here.levels):
        base, size = here.block(level)
        far, _ = here.block_across(level)
        own, theirs = pl.ds(base, size), pl.ds(far, size)
        zwait = plan.start([(mine(own, c), mine(own, c), mine(theirs, c))], here.device(z=here.across(level)))
        waiting_a.append((sets[-1], start_a(sets[-1])))
        sets.append(theirs)
        yield
        if level:
            zs, w = waiting_a.pop(0)
            waiting_b.append((zs, start_b(zs, w)))
        plan.arrived(zwait)
    waiting_a.append((sets[-1], start_a(sets[-1])))
    while waiting_a:
        yield
        zs, w = waiting_a.pop(0)
        waiting_b.append((zs, start_b(zs, w)))
    while waiting_b:
        yield
        zs, w = waiting_b.pop(0)
        plan.arrived(w)
        to_core(line_there, zs)
    yield
    plan.arrived(cores)


def gather_copies(levels):
    return 2 * (levels + 5 * (levels + 1))


def gather_kernel(
    w_in, small_in, xa_out, xb_out, small_out, xa_in, xb_in, send, recv, ssend, srecv, place_sem, *, depth, ranks
):
    here = Here(depth)
    xa_in[...] = w_in[:, DI : DI + XA].astype(BF)
    xb_in[...] = jnp.zeros_like(xb_in)
    xb_in[:, : PROJ - DI - XA] = w_in[:, DI + XA :].astype(BF)
    slot = (here.z, here.y, here.x, here.c)
    own = [
        pltpu.make_async_copy(xa_in, xa_out.at[slot], place_sem.at[0]),
        pltpu.make_async_copy(xb_in, xb_out.at[slot], place_sem.at[1]),
        pltpu.make_async_copy(small_in, small_out.at[here.rank], place_sem.at[2]),
    ]
    here.greet_all(ranks)
    for copy in own:
        copy.start()
    start, finish = everyone(here.rank, ranks, lambda other: small_in, lambda rank: small_out.at[rank], ssend, srecv)
    for copy in own:
        copy.wait()
    plan = Plan(send, recv)
    plan.trace([gather_stream(here, plan, xa_out, "x"), gather_stream(here, plan, xb_out, "y")])
    plan.run(0)
    start()
    plan.run_from(1)
    finish()


ANY = pl.BlockSpec(memory_space=pl.ANY)
IN_VMEM = pl.BlockSpec(memory_space=pltpu.VMEM)


def gather(w_in, small, depth):
    ranks = depth * 8
    rows = w_in.shape[0]
    lead = (depth, 2, 2, 2)
    sds = jax.ShapeDtypeStruct
    n = gather_copies(depth.bit_length() - 1)
    dma = pltpu.SemaphoreType.DMA
    return pl.pallas_call(
        partial(gather_kernel, depth=depth, ranks=ranks),
        in_specs=[IN_VMEM] * 2,
        out_specs=[ANY] * 3,
        out_shape=[
            sds(lead + (rows, XA), BF),
            sds(lead + (rows, XD - XA), BF),
            sds((ranks,) + small.shape, small.dtype),
        ],
        scratch_shapes=[
            pltpu.VMEM((rows, XA), BF),
            pltpu.VMEM((rows, XD - XA), BF),
            dma((n,)),
            dma((n,)),
            dma((ranks,)),
            dma((ranks,)),
            dma((3,)),
        ],
        compiler_params=pltpu.CompilerParams(collective_id=0, has_side_effects=True),
        name="gather",
    )(w_in, small)


def reduce_stream(here, plan, item, first):
    part, acc, core_in, line_in, side_in, z_in, put, own_sem = item
    z, y, x, c = here.z, here.y, here.x, here.c
    one_dev = here.device(y=1 - y) if first == "y" else here.device(x=1 - x)
    two_dev = here.device(x=1 - x) if first == "y" else here.device(y=1 - y)
    sibling = here.device(c=1 - c)
    sets = []
    for level in reversed(range(here.levels)):
        sets.append(here.block_across(level))
    sets.append((z, 1))
    slots = [pl.ds(zs[0], zs[1]) for zs in sets]
    mine = pltpu.make_async_copy(part.at[BOTH, BOTH, BOTH, c], acc, own_sem)
    plan.do(mine.start)

    def add(target, source):
        acc[target] = (acc[target].astype(F32) + source.astype(F32)).astype(BF)

    def line_add(zs):
        for k in range(zs[1]):
            for a in range(2):
                for b in range(2):
                    add((zs[0] + k, a, b), core_in[zs[0] + k, a, b])

    def side_add(zs):
        for k in range(zs[1]):
            for a in range(2):
                add((zs[0] + k, y, a) if first == "y" else (zs[0] + k, a, x), line_in[zs[0] + k, a])

    def last_add(zs):
        for k in range(zs[1]):
            add((zs[0] + k, y, x), side_in[zs[0] + k])

    cores = [plan.start([(part.at[s, BOTH, BOTH, 1 - c], core_in.at[s], core_in.at[s])], sibling) for s in slots]
    plan.do(mine.wait)
    yield
    lines, sides = [], []
    n = len(sets)
    for step in range(n + 2):
        if step < n:
            s = slots[step]
            plan.arrived(cores[step])
            plan.do(partial(line_add, sets[step]))
            give = acc.at[s, 1 - y, BOTH] if first == "y" else acc.at[s, BOTH, 1 - x]
            lines.append(plan.start([(give, line_in.at[s], line_in.at[s])], one_dev))
        if 1 <= step <= n:
            s = slots[step - 1]
            plan.arrived(lines[step - 1])
            plan.do(partial(side_add, sets[step - 1]))
            give = acc.at[s, y, 1 - x] if first == "y" else acc.at[s, 1 - y, x]
            sides.append(plan.start([(give, side_in.at[s], side_in.at[s])], two_dev))
        if step >= 2:
            plan.arrived(sides[step - 2])
            plan.do(partial(last_add, sets[step - 2]))
            if step == 2:
                level = here.levels - 1
                s, size = slots[0], sets[0][1]
                zwait = plan.start(
                    [(acc.at[s, y, x], z_in[0].at[0:size], z_in[0].at[0:size])], here.device(z=here.across(level))
                )
        yield

    def z_add(base, size, got):
        for k in range(size):
            add((base + k, y, x), got[k])

    def z_end(base, got):
        put(got[0].astype(F32) + acc[base, y, x].astype(F32))

    for at_level, level in enumerate(reversed(range(here.levels))):
        base, size = here.block(level)
        plan.arrived(zwait)
        if level:
            plan.do(partial(z_add, base, size, z_in[at_level]))
            far, size = here.block_across(level - 1)
            landing = z_in[at_level + 1].at[0:size]
            zwait = plan.start(
                [(acc.at[pl.ds(far, size), y, x], landing, landing)], here.device(z=here.across(level - 1))
            )
            yield
        else:
            plan.do(partial(z_end, base, z_in[at_level]))


def reduce_copies(levels):
    return 2 * (3 * (levels + 1) + levels)


def reduce_scratch(depth, tile):
    levels = depth.bit_length() - 1
    return [
        pltpu.VMEM((depth, 2, 2) + tile, BF),
        pltpu.VMEM((depth, 2, 2) + tile, BF),
        pltpu.VMEM((depth, 2) + tile, BF),
        pltpu.VMEM((depth,) + tile, BF),
    ] + [pltpu.VMEM((1 << level,) + tile, BF) for level in reversed(range(levels))]


def reduce_items(here, plan, parts, outs, scratch, own_sems):
    each = 4 + here.levels
    streams = []
    for k, first in enumerate(("y", "x")):
        bufs = scratch[k * each : (k + 1) * each]

        def put(v, k=k):
            outs[k][...] = v

        item = (parts[k], *bufs[:4], bufs[4:], put, own_sems.at[k])
        streams.append(reduce_stream(here, plan, item, first))
    plan.trace(streams)


def reduce_kernel(pa, pb, small_in, oa, ob, small_out, send, recv, ssend, srecv, small_got, own_sems, *scratch, depth, ranks):
    here = Here(depth)
    here.greet_all(ranks)
    start, finish = everyone(
        here.rank, ranks, lambda other: small_in.at[other], lambda rank: small_got.at[rank], ssend, srecv
    )
    plan = Plan(send, recv)
    reduce_items(here, plan, (pa, pb), (oa, ob), scratch, own_sems)
    plan.run(0)
    start()
    plan.run_from(1)
    finish()

    def add(i, total):
        return total + jnp.where(i == here.rank, small_in[i], small_got[i])

    small_out[...] = lax.fori_loop(0, ranks, add, jnp.zeros(small_out.shape, F32))


def reduce(pa, pb, small, depth):
    ranks = depth * 8
    sds = jax.ShapeDtypeStruct
    dma = pltpu.SemaphoreType.DMA
    n = reduce_copies(depth.bit_length() - 1)
    scratch = [dma((n,)), dma((n,)), dma((ranks,)), dma((ranks,)), pltpu.VMEM(small.shape, F32), dma((2,))]
    for part in (pa, pb):
        scratch += reduce_scratch(depth, part.shape[-2:])
    return pl.pallas_call(
        partial(reduce_kernel, depth=depth, ranks=ranks),
        in_specs=[ANY, ANY, IN_VMEM],
        out_specs=[IN_VMEM] * 3,
        out_shape=[sds(a.shape[4:], F32) for a in (pa, pb)] + [sds(small.shape[1:], F32)],
        scratch_shapes=scratch,
        compiler_params=pltpu.CompilerParams(collective_id=1, has_side_effects=True, vmem_limit_bytes=LIMIT),
        name="reduce",
    )(pa, pb, small)


def whole(shape):
    return pl.BlockSpec(shape, lambda i: (0,) * len(shape))


def kept(shape):
    return pl.BlockSpec(shape, lambda i: (0,) * len(shape), pipeline_mode=pl.Buffered(1))


def per(shape, first=0):
    rest = (0,) * len(shape)
    return pl.BlockSpec((None,) + shape, lambda i: (first + i,) + rest)


SMEM = pl.BlockSpec(memory_space=pltpu.SMEM)
LIMIT = 67_000_000


def project_kernel(
    vlen_ref,
    x_ref,
    xh_ref,
    g_ref,
    wa_ref,
    wb_ref,
    cw_ref,
    cb_ref,
    dtb_ref,
    rate_ref,
    win_ref,
    wo_ref,
    nrm_ref,
    ci_ref,
    act_ref,
    step_ref,
    l_ref,
    sig_ref,
    sloc_ref,
    s_ref,
    z_out,
    o_out,
    nx,
    xw,
    state,
    e2,
    z_in,
    o_in,
    send,
    recv,
    place_sem,
    *,
    first,
    count,
    depth,
):
    piece = x_ref.shape[0]
    chunks = piece // CL
    section = pl.program_id(0)
    valid = vlen_ref[first + section]
    here = Here(depth)
    slot = (here.z, here.y, here.x, here.c)
    own = [
        pltpu.make_async_copy(z_in, z_out.at[slot], place_sem.at[0]),
        pltpu.make_async_copy(o_in, o_out.at[slot], place_sem.at[1]),
    ]
    plan = Plan(send, recv)
    plan.trace([gather_stream(here, plan, z_out, "x"), gather_stream(here, plan, o_out, "y")])

    @pl.when(section == 0)
    def _():
        z_in[...] = win_ref[:, 0:DI].astype(BF)
        o_in[...] = wo_ref[...].astype(BF)
        here.greet_partners()
        for copy in own:
            copy.start()
        for copy in own:
            copy.wait()
        plan.run(0)

    def norm(v):
        v = v.astype(F32)
        r = lax.rsqrt(jnp.mean(v * v, axis=-1, keepdims=True) + EPSILON)
        return (v * r * g_ref[...]).astype(BF)

    nx[0:16] = norm(xh_ref[...])

    def norm_rows(i, c):
        rows = pl.ds(pl.multiple_of(i * 64, 64), 64)
        v = norm(x_ref[rows, :])
        nx[pl.ds(pl.multiple_of(i * 64 + 16, 16), 64), :] = v
        nrm_ref[rows, :] = v
        return c

    lax.fori_loop(0, piece // 64, norm_rows, 0)

    for j in range(XBC // 256):
        w = wa_ref[:, j * 256 : (j + 1) * 256] if j < XA // 256 else wb_ref[:, j * 256 - XA : (j + 1) * 256 - XA]
        ci = nn(nx[...], w)
        ci_ref[2 * j] = ci[8:, :LN]
        ci_ref[2 * j + 1] = ci[8:, LN:]
    dt_raw = nn(nx[16:], wb_ref[:, XBC - XA :]) + dtb_ref[...]
    row = lax.broadcasted_iota(jnp.int32, (piece, LN), 0)
    mask = jnp.where(row < valid, 1.0, 0.0)
    step_ref[...] = (jnp.maximum(dt_raw, 0.0) + jnp.log1p(jnp.exp(-jnp.abs(dt_raw)))) * mask
    sig_ref[...] = mask / (1.0 + jnp.exp(-dt_raw))

    @pl.when(pl.program_id(0) == 0)
    def _():
        fill_expander(e2)

    tri = jnp.where(lower_mask(False), 1.0, 0.0)
    state[...] = jnp.zeros_like(state)

    slots = count * chunks
    late = slots // 2 + 1
    steps = min(len(plan.segments) - 1, slots - late + 1)

    def chunk(k, total):
        base = pl.multiple_of(k * CL, CL)
        rows = pl.ds(base, CL)
        for n in range(steps):

            @pl.when(section * chunks + k == (late + n - 1 if n else 0))
            def _():
                plan.run(n + 1)

        step = step_ref[rows, :]
        ld = exact_nn(tri, step * rate_ref[...])
        l_ref[rows, :] = ld
        end = ld[CL - 1 :]
        tail = expand(step * jnp.exp(end - ld), e2)
        for j in range(XBC // LN):
            run = conv_running(ci_ref, j, base, cw_ref[:, lanes(j)], cb_ref[:, lanes(j)])
            act = run * sigmoid(run)
            act_ref[rows, lanes(j)] = act
            if j < DI // LN:
                xw[:, lanes(j)] = (act * tail[:, lanes(j)]).astype(BF)
        b = act_ref[rows, DI : DI + NS].astype(BF)
        sloc_ref[k] = state[...].astype(BF)
        keep = expand(jnp.exp(jnp.broadcast_to(end, (8, LN))), e2)[0:1]
        state[...] = keep * state[...] + tn(b, xw[...])
        return total + end

    total = lax.fori_loop(0, chunks, chunk, jnp.zeros((1, LN), F32))
    s_ref[0:NS] = state[...].astype(BF)
    keep = expand(jnp.exp(jnp.broadcast_to(total, (8, LN))), e2)[0:1]
    top, low = halves(keep)
    s_ref[NS : NS + 16] = jnp.concatenate([top, low, jnp.zeros((14, DI), BF)], axis=0)

    @pl.when(section == count - 1)
    def _():
        plan.run_from(steps + 1)


def project(first, count, depth, valid, tokens, halo, gain, wa, wb, cw, cb, dtb, rate, w_in, w_out):
    piece = tokens.shape[1]
    chunks = piece // CL
    lead = (depth, 2, 2, 2)
    n = gather_copies(depth.bit_length() - 1)
    sds = jax.ShapeDtypeStruct
    dma = pltpu.SemaphoreType.DMA
    return pl.pallas_call(
        partial(project_kernel, first=first, count=count, depth=depth),
        grid=(count,),
        in_specs=[
            SMEM,
            per((piece, D), first),
            per((16, D), first),
            whole((1, D)),
            kept((D, XA)),
            kept((D, XD - XA)),
            whole((DCONV, XBC)),
            whole((1, XBC)),
            whole((1, LN)),
            whole((1, LN)),
            kept(w_in.shape),
            kept(w_out.shape),
        ],
        out_specs=[
            per((piece, D)),
            per((XBC // LN, piece + 8, LN)),
            per((piece, XBC)),
            per((piece, LN)),
            per((piece, LN)),
            per((piece, LN)),
            per((chunks, NS, DI)),
            per((SROWS, DI)),
            ANY,
            ANY,
        ],
        out_shape=[
            sds((count, piece, D), BF),
            sds((count, XBC // LN, piece + 8, LN), F32),
            sds((count, piece, XBC), F32),
            sds((count, piece, LN), F32),
            sds((count, piece, LN), F32),
            sds((count, piece, LN), F32),
            sds((count, chunks, NS, DI), BF),
            sds((count, SROWS, DI), BF),
            sds(lead + (w_in.shape[0], DI), BF),
            sds(lead + w_out.shape, BF),
        ],
        scratch_shapes=[
            pltpu.VMEM((piece + 16, D), BF),
            pltpu.VMEM((CL, DI), BF),
            pltpu.VMEM((NS, DI), F32),
            pltpu.VMEM((2 * LN, DI), BF),
            pltpu.VMEM((w_in.shape[0], DI), BF),
            pltpu.VMEM(w_out.shape, BF),
            dma((n,)),
            dma((n,)),
            dma((2,)),
        ],
        compiler_params=pltpu.CompilerParams(vmem_limit_bytes=LIMIT, collective_id=4, has_side_effects=True),
        name="project",
    )(valid, tokens, halo, gain, wa, wb, cw, cb, dtb, rate, w_in, w_out)


class Exchange:
    def __init__(self, own, sib, out, got, swap_send, swap_recv, far_send, far_recv, giver):
        dp, seq = lax.axis_index("dp"), lax.axis_index("seq")
        self.x, self.c = seq // 2, seq % 2
        self.sibling = (dp, self.x * 2 + 1 - self.c)
        self.across = (dp, (1 - self.x) * 2 + self.c)
        self.own, self.sib, self.out, self.got = own, sib, out, got
        self.sems = (swap_send, swap_recv, far_send, far_recv)
        self.giver = giver

    def greet(self):
        barrier = pltpu.get_barrier_semaphore()
        for other in (self.sibling, self.across):
            pl.semaphore_signal(barrier, inc=1, device_id=other, device_id_type=pl.DeviceIdType.MESH)
        pl.semaphore_wait(barrier, 2)

    def swap(self, i):
        return pltpu.make_async_remote_copy(
            src_ref=self.own.at[i],
            dst_ref=self.sib.at[i],
            send_sem=self.sems[0].at[i],
            recv_sem=self.sems[1].at[i],
            device_id=self.sibling,
            device_id_type=pl.DeviceIdType.MESH,
        )

    def far(self, i):
        return pltpu.make_async_remote_copy(
            src_ref=self.out.at[i],
            dst_ref=self.got.at[i],
            send_sem=self.sems[2].at[i],
            recv_sem=self.sems[3].at[i],
            device_id=self.across,
            device_id_type=pl.DeviceIdType.MESH,
        )

    def decay(self, ref, i):
        return ref[i, NS : NS + 1].astype(F32) + ref[i, NS + 1 : NS + 2].astype(F32)

    def begin(self, count):
        for i in range(count):
            self.swap(i).start()

    def hand_over(self, i, coefficients):
        self.swap(i).wait_recv()

        @pl.when(self.x == self.giver)
        def _():
            f, g = coefficients(self.decay(self.own, i), self.decay(self.sib, i))
            self.out[i] = (f * self.own[i, 0:NS].astype(F32) + g * self.sib[i, 0:NS].astype(F32)).astype(BF)
            self.far(i).start()

    def end(self, count):
        for i in range(count):
            self.swap(i).wait_send()

            @pl.when(self.x == self.giver)
            def _():
                self.far(i).wait_send()


def exchange_scratch(count):
    dma = pltpu.SemaphoreType.DMA((count,))
    return [
        pltpu.VMEM((count, SROWS, DI), BF),
        pltpu.VMEM((count, NS, DI), BF),
        pltpu.VMEM((count, NS, DI), BF),
        dma,
        dma,
        dma,
        dma,
    ]


def mix_kernel(
    vlen_ref,
    x_ref,
    cot_ref,
    nrm_ref,
    act_ref,
    step_ref,
    l_ref,
    sloc_ref,
    s_ref,
    wz_ref,
    wo_ref,
    gg_ref,
    dsk_ref,
    out_ref,
    gn_ref,
    dbr_ref,
    dz_ref,
    dy_ref,
    y_ref,
    incoming,
    dsin_ref,
    ggrad_ref,
    zs,
    dgn,
    dsacc,
    yf,
    work,
    e2,
    sib,
    out,
    got,
    *sems,
    first,
    count,
):
    piece = x_ref.shape[0]
    chunks = piece // CL
    section = pl.program_id(0)
    valid = vlen_ref[first + section]
    states = Exchange(s_ref, sib, out, got, *sems, giver=0)
    even = states.c == 0
    weigh = lambda own, sibs: (jnp.where(even, sibs, 1.0), jnp.where(even, 1.0, own))

    @pl.when(section == 0)
    def _():
        ggrad_ref[...] = jnp.zeros_like(ggrad_ref)
        fill_expander(e2)
        states.greet()
        states.begin(count)
        states.hand_over(0, weigh)

    row = lax.broadcasted_iota(jnp.int32, (piece, 1), 0)
    live = row < valid
    dbr_ref[...] = jnp.where(live, cot_ref[...].astype(F32), 0.0).astype(BF)
    for j in range(DI // 256):
        cols = slice(j * 256, (j + 1) * 256)
        zs[:, cols] = nn(nrm_ref[...], wz_ref[:, cols])
        dgn[:, cols] = nt(dbr_ref[...], wo_ref[cols, :])

    @pl.when(states.x == 0)
    def _():
        incoming[...] = jnp.where(even, 0.0, 1.0) * sib[section, 0:NS].astype(F32)

    @pl.when(states.x == 1)
    def _():
        states.far(section).wait_recv()
        f = jnp.where(even, 1.0, states.decay(sib, section))
        incoming[...] = f * got[section].astype(F32) + jnp.where(even, 0.0, 1.0) * sib[section, 0:NS].astype(F32)

    low = lower_mask(False)
    left, right = half_masks()
    dsacc[...] = jnp.zeros_like(dsacc)

    def chunk(k, before):
        base = pl.multiple_of(k * CL, CL)
        rows = pl.ds(base, CL)
        for n in range(1, count):

            @pl.when((section == 0) & (k == n - 1))
            def _():
                states.hand_over(n, weigh)

        step = step_ref[rows, :]
        ld = l_ref[rows, :]
        ldt = ld.T
        start = (before * incoming[...] + sloc_ref[k].astype(F32)).astype(BF)
        step_e = expand(step, e2)
        grow = expand(jnp.exp(ld), e2)
        b = act_ref[rows, DI : DI + NS].astype(BF)
        c, c_low = halves(act_ref[rows, DI + NS :])
        scores = jnp.where(low, nt(c, b), 0.0)
        squares = jnp.zeros((CL, LN), F32)
        for j in range(DI // LN):
            x = act_ref[rows, lanes(j)]
            xd = (x * step_e[:, lanes(j)]).astype(BF)
            mixes = []
            for h in (2 * j, 2 * j + 1):
                gap = jnp.minimum(ld[:, h : h + 1] - ldt[h : h + 1, :], 0.0)
                mixes.append((jnp.exp(gap) * scores).astype(BF))
            block = jnp.concatenate([xd * left, xd * right], axis=0)
            st = start[:, lanes(j)]
            y = nn(jnp.concatenate(mixes, axis=1), block) + (nn(c, st) + nn(c_low, st)) * grow[:, lanes(j)]
            y_ref[rows, lanes(j)] = y
            full = y + dsk_ref[:, lanes(j)] * x
            yf[:, lanes(j)] = full
            z = zs[rows, lanes(j)]
            u = full * (z * sigmoid(z))
            squares = squares + u * u
        r = lax.rsqrt(jnp.sum(squares, axis=-1, keepdims=True) * (1.0 / DI) + EPSILON)
        inner = jnp.zeros((CL, LN), F32)
        for j in range(DI // LN):
            z = zs[rows, lanes(j)]
            v = yf[:, lanes(j)] * (z * sigmoid(z)) * r
            gain = gg_ref[:, lanes(j)]
            gn_ref[rows, lanes(j)] = (v * gain).astype(BF)
            dg = dgn[rows, lanes(j)]
            gv = dg * v
            ggrad_ref[:, lanes(j)] += jnp.sum(gv.reshape(CL // 8, 8, LN), axis=0)
            inner = inner + gv * gain
        q = jnp.sum(inner, axis=-1, keepdims=True) * (1.0 / DI)
        for j in range(DI // LN):
            z = zs[rows, lanes(j)]
            s = sigmoid(z)
            sz = z * s
            full = yf[:, lanes(j)]
            v = full * sz * r
            du = r * (dgn[rows, lanes(j)] * gg_ref[:, lanes(j)] - v * q)
            dy = du * sz
            dy_ref[rows, lanes(j)] = dy
            dz_ref[rows, lanes(j)] = (du * full * (s + sz * (1.0 - s))).astype(BF)
            work[:, lanes(j)] = (dy * grow[:, lanes(j)]).astype(BF)
        dsacc[...] += before * tn(c, work[...])
        return before * grow[CL - 1 :]

    lax.fori_loop(0, chunks, chunk, jnp.ones((1, DI), F32))
    dsin_ref[0:NS] = dsacc[...].astype(BF)
    dsin_ref[NS:] = s_ref[section, NS:]
    for j in range(D // 256):
        cols = slice(j * 256, (j + 1) * 256)
        branch = nn(gn_ref[...], wo_ref[:, cols])
        out_ref[:, cols] = jnp.where(live, x_ref[:, cols].astype(F32) + branch, 0.0).astype(BF)

    @pl.when(section == count - 1)
    def _():
        states.end(count)


def mix(first, count, valid, tokens, cot, normed, act, step, ld, sloc, s, w_z, w_o, gg, dsk):
    piece = tokens.shape[1]
    chunks = piece // CL
    sds = jax.ShapeDtypeStruct
    return pl.pallas_call(
        partial(mix_kernel, first=first, count=count),
        grid=(count,),
        in_specs=[
            SMEM,
            per((piece, D), first),
            per((piece, D), first),
            per((piece, D)),
            per((piece, XBC)),
            per((piece, LN)),
            per((piece, LN)),
            per((chunks, NS, DI)),
            kept((count, SROWS, DI)),
            kept((D, DI)),
            kept((DI, D)),
            whole((1, DI)),
            whole((1, DI)),
        ],
        out_specs=[
            per((piece, D)),
            per((piece, DI)),
            per((piece, D)),
            per((piece, DI)),
            per((piece, DI)),
            per((piece, DI)),
            per((NS, DI)),
            per((SROWS, DI)),
            whole((8, DI)),
        ],
        out_shape=[
            sds((count, piece, D), BF),
            sds((count, piece, DI), BF),
            sds((count, piece, D), BF),
            sds((count, piece, DI), BF),
            sds((count, piece, DI), F32),
            sds((count, piece, DI), F32),
            sds((count, NS, DI), F32),
            sds((count, SROWS, DI), BF),
            sds((8, DI), F32),
        ],
        scratch_shapes=[
            pltpu.VMEM((piece, DI), F32),
            pltpu.VMEM((piece, DI), F32),
            pltpu.VMEM((NS, DI), F32),
            pltpu.VMEM((CL, DI), F32),
            pltpu.VMEM((CL, DI), BF),
            pltpu.VMEM((2 * LN, DI), BF),
        ]
        + exchange_scratch(count),
        compiler_params=pltpu.CompilerParams(vmem_limit_bytes=LIMIT, collective_id=2, has_side_effects=True),
        name="mix",
    )(valid, tokens, cot, normed, act, step, ld, sloc, s, w_z, w_o, gg, dsk)


def scan_back_kernel(
    ci_ref,
    step_ref,
    l_ref,
    sig_ref,
    dy_ref,
    y_ref,
    inc_ref,
    sloc_ref,
    dsin_ref,
    cw_ref,
    cb_ref,
    rate_ref,
    dsk_ref,
    part_a,
    part_b,
    dxa_ref,
    dxb_ref,
    fix_ref,
    edge_ref,
    cgrad_ref,
    hgrad_ref,
    skip_ref,
    shard_a,
    shard_b,
    ds,
    xa,
    dsl,
    dact,
    xdt,
    xt,
    dr,
    e2,
    u_top,
    u_low,
    fs,
    vs,
    dyg,
    start,
    sib,
    out,
    got,
    swap_send,
    swap_recv,
    far_send,
    far_recv,
    send,
    recv,
    own_sems,
    *scratch,
    count,
    depth,
):
    piece = dy_ref.shape[0]
    chunks = piece // CL
    section = pl.program_id(0)
    states = Exchange(dsin_ref, sib, out, got, swap_send, swap_recv, far_send, far_recv, giver=1)
    here = Here(depth)
    plan = Plan(send, recv)
    reduce_items(here, plan, (part_a, part_b), (shard_a, shard_b), scratch, own_sems)
    even = states.c == 0
    one_if_even = jnp.where(even, 1.0, 0.0)
    weigh = lambda own, sibs: (jnp.where(even, 1.0, sibs), jnp.where(even, own, 1.0))

    @pl.when(section == 0)
    def _():
        cgrad_ref[...] = jnp.zeros_like(cgrad_ref)
        hgrad_ref[...] = jnp.zeros_like(hgrad_ref)
        skip_ref[...] = jnp.zeros_like(skip_ref)
        fill_expander(e2)
        here.greet_partners()
        states.begin(count)
        plan.run(0)
        states.hand_over(0, weigh)

    upper = jnp.logical_not(lower_mask(True))
    upper_one = jnp.where(upper, 1.0, 0.0)
    before_one = jnp.where(lower_mask(True), 1.0, 0.0)
    left, right = half_masks()
    dr[:, CL:] = jnp.zeros((XBC // LN, 8, LN), F32)
    steps = min(len(plan.segments) - 1, count * chunks)

    def chunk(i, carry):
        k = chunks - 1 - i
        base = pl.multiple_of(k * CL, CL)
        rows = pl.ds(base, CL)
        for n in range(steps):

            @pl.when(section * chunks + i == n)
            def _():
                plan.run(n + 1)

        for n in range(1, count):

            @pl.when((section == 0) & (i == n))
            def _():
                states.hand_over(n, weigh)

        step = step_ref[rows, :]
        ld = l_ref[rows, :]
        ldt = ld.T
        end = ld[CL - 1 :]
        prefix = jnp.zeros((8, LN), F32)
        for j in range(chunks - 1):
            prefix = prefix + jnp.where(j < k, 1.0, 0.0) * l_ref[j * CL + CL - 1 : j * CL + CL, :]
        before = expand(jnp.exp(prefix), e2)[0:1]
        start[...] = before * inc_ref[...] + sloc_ref[k].astype(F32)
        step_e = expand(step, e2)
        grow = expand(jnp.exp(ld), e2)
        tail = expand(jnp.exp(end - ld), e2)
        keep = grow[CL - 1 :]
        for j in range(XBC // LN):
            run = conv_running(ci_ref, j, base, cw_ref[:, lanes(j)], cb_ref[:, lanes(j)])
            s = sigmoid(run)
            a = run * s
            xa[:, lanes(j)] = a
            dsl[:, lanes(j)] = s + a * (1.0 - s)
            if j < DI // LN:
                xd = a * step_e[:, lanes(j)]
                xdt[:, lanes(j)] = xd
                xt[:, lanes(j)] = xd * tail[:, lanes(j)]

        @pl.when((i == 0) & (states.x == 1))
        def _():
            ds[...] = one_if_even * sib[section, 0:NS].astype(F32)

        @pl.when((i == 0) & (states.x == 0))
        def _():
            states.far(section).wait_recv()
            f = jnp.where(even, states.decay(sib, section), 1.0)
            ds[...] = f * got[section].astype(F32) + one_if_even * sib[section, 0:NS].astype(F32)

        b = xa[:, DI : DI + NS].astype(BF)
        c = xa[:, DI + NS :].astype(BF)
        scores = jnp.where(upper, nt(b, c), 0.0)
        dact[:, 0:DI] = nn(b, ds[...].astype(BF)) * tail
        dscores = jnp.zeros((CL, CL), F32)
        for j in range(DI // LN):
            dyf = dy_ref[rows, lanes(j)]
            dyb, dyl = halves(dyf)
            block = jnp.concatenate([dyb * left, dyb * right], axis=0)
            block_low = jnp.concatenate([dyl * left, dyl * right], axis=0)
            xdb, xdl = halves(xdt[:, lanes(j)])
            dmix = nt(jnp.concatenate([xdb, xdl], axis=1), jnp.concatenate([block, block], axis=1)) + nt(xdb, block_low)
            mixes = []
            for p, h in enumerate((2 * j, 2 * j + 1)):
                gap = jnp.minimum(ldt[h : h + 1, :] - ld[:, h : h + 1], 0.0)
                w = jnp.exp(gap)
                mixes.append((w * scores).astype(BF))
                dscores = dscores + dmix[:, lanes(p)] * w
            diag = nn(jnp.concatenate(mixes, axis=1), block)
            far = dact[:, lanes(j)]
            xdf = xdb.astype(F32)
            u_top[:, lanes(j)], u_low[:, lanes(j)] = halves(dyb.astype(F32) * y_ref[rows, lanes(j)] - xdf * diag)
            fs[:, lanes(j)] = (xdf * far).astype(BF)
            dxd = diag + far
            x = xa[:, lanes(j)]
            vs[:, lanes(j)] = (x * dxd).astype(BF)
            dact[:, lanes(j)] = dxd * step_e[:, lanes(j)] + dsk_ref[:, lanes(j)] * dyf
            skip_ref[:, lanes(j)] += jnp.sum((dyf * x).reshape(CL // 8, 8, LN), axis=0)
            dyg[:, lanes(j)] = dyf * grow[:, lanes(j)]
        e = e2[0:LN]
        const = jnp.sum((start[...] * ds[...]).reshape(NS // 8, 8, DI), axis=0) * keep
        c_top, c_low = halves(const)
        r_c = jnp.sum(nt(c_top, e) + nt(c_low, e), axis=0, keepdims=True)
        r_u = nt(u_top[...], e) + nt(u_low[...], e)
        r_f = nt(fs[...], e)
        r_v = nt(vs[...], e)
        db = three(nt, xt[...], ds[...])
        dc = three(nt, dyg[...], start[...])
        ds[...] = keep * ds[...] + tn(c, dyg[...].astype(BF))
        dsc = jnp.where(upper, dscores, 0.0).astype(BF)
        dact[:, DI : DI + NS] = db + nn(dsc, c)
        dact[:, DI + NS :] = dc + tn(dsc, b)
        da = exact_nn(upper_one, r_u) + exact_nn(before_one, r_f) + r_c
        dstep = r_v + rate_ref[...] * da
        ddt = dstep * sig_ref[rows, :]
        hgrad_ref[0:8] += jnp.sum(ddt.reshape(CL // 8, 8, LN), axis=0)
        hgrad_ref[8:16] += jnp.sum((da * step).reshape(CL // 8, 8, LN), axis=0)
        dxb_ref[rows, XBC - XA :] = ddt.astype(BF)
        for j in range(XBC // LN):
            g = dact[:, lanes(j)] * dsl[:, lanes(j)]
            dr[j, 0:CL] = g
            ci = ci_ref[j, pl.ds(base + 8, CL), :]
            total = g * cw_ref[DCONV - 1 : DCONV, lanes(j)]
            last = 8 * (DCONV - 1)
            cgrad_ref[last : last + 8, lanes(j)] += jnp.sum((g * ci).reshape(CL // 8, 8, LN), axis=0)
            for tap in range(DCONV - 1):
                later = DCONV - 1 - tap
                shifted = dr[j, later : later + CL, :]
                total = total + shifted * cw_ref[tap : tap + 1, lanes(j)]
                cgrad_ref[8 * tap : 8 * tap + 8, lanes(j)] += jnp.sum((shifted * ci).reshape(CL // 8, 8, LN), axis=0)
            cgrad_ref[32:40, lanes(j)] += jnp.sum(g.reshape(CL // 8, 8, LN), axis=0)
            if j < XA // LN:
                dxa_ref[rows, lanes(j)] = total.astype(BF)
            else:
                dxb_ref[rows, lanes(j - XA // LN)] = total.astype(BF)

            @pl.when(i == 0)
            def _():
                fix_ref[:, lanes(j)] = total[CL - 16 :]

            dr[j, CL:] = g[0:8]
        return carry

    lax.fori_loop(0, chunks, chunk, 0)
    for j in range(XBC // LN):
        edge_ref[:, lanes(j)] = dr[j, CL:]
        for tap in range(DCONV - 1):
            later = DCONV - 1 - tap
            part = dr[j, CL : CL + later] * ci_ref[j, 8 - later : 8]
            cgrad_ref[8 * tap : 8 * tap + 1, lanes(j)] += jnp.sum(part, axis=0, keepdims=True)

    @pl.when(section == count - 1)
    def _():
        states.end(count)
        plan.run_from(steps + 1)


def scan_back(count, depth, ci, step, ld, sig, dy, y, inc, sloc, dsin, cw, cb, rate, dsk, part_a, part_b):
    piece = dy.shape[1]
    chunks = piece // CL
    n = reduce_copies(depth.bit_length() - 1)
    sds = jax.ShapeDtypeStruct
    dma = pltpu.SemaphoreType.DMA
    return pl.pallas_call(
        partial(scan_back_kernel, count=count, depth=depth),
        grid=(count,),
        in_specs=[
            per((XBC // LN, piece + 8, LN)),
            per((piece, LN)),
            per((piece, LN)),
            per((piece, LN)),
            per((piece, DI)),
            per((piece, DI)),
            per((NS, DI)),
            per((chunks, NS, DI)),
            kept((count, SROWS, DI)),
            whole((DCONV, XBC)),
            whole((1, XBC)),
            whole((1, LN)),
            whole((1, DI)),
            ANY,
            ANY,
        ],
        out_specs=[
            per((piece, XA)),
            per((piece, XD - XA)),
            per((16, XBC)),
            per((8, XBC)),
            whole((40, XBC)),
            whole((16, LN)),
            whole((8, DI)),
            whole(part_a.shape[4:]),
            whole(part_b.shape[4:]),
        ],
        out_shape=[
            sds((count, piece, XA), BF),
            sds((count, piece, XD - XA), BF),
            sds((count, 16, XBC), F32),
            sds((count, 8, XBC), F32),
            sds((40, XBC), F32),
            sds((16, LN), F32),
            sds((8, DI), F32),
            sds(part_a.shape[4:], F32),
            sds(part_b.shape[4:], F32),
        ],
        scratch_shapes=[
            pltpu.VMEM((NS, DI), F32),
            pltpu.VMEM((CL, XBC), F32),
            pltpu.VMEM((CL, XBC), F32),
            pltpu.VMEM((CL, XBC), F32),
            pltpu.VMEM((CL, DI), F32),
            pltpu.VMEM((CL, DI), F32),
            pltpu.VMEM((XBC // LN, CL + 8, LN), F32),
            pltpu.VMEM((2 * LN, DI), BF),
            pltpu.VMEM((CL, DI), BF),
            pltpu.VMEM((CL, DI), BF),
            pltpu.VMEM((CL, DI), BF),
            pltpu.VMEM((CL, DI), BF),
            pltpu.VMEM((CL, DI), F32),
            pltpu.VMEM((NS, DI), F32),
        ]
        + exchange_scratch(count)
        + [dma((n,)), dma((n,)), dma((2,))]
        + reduce_scratch(depth, part_a.shape[-2:])
        + reduce_scratch(depth, part_b.shape[-2:]),
        compiler_params=pltpu.CompilerParams(vmem_limit_bytes=LIMIT, collective_id=3, has_side_effects=True),
        name="scan_back",
    )(ci, step, ld, sig, dy, y, inc, sloc, dsin, cw, cb, rate, dsk, part_a, part_b)


def patch_kernel(a_ref, b_ref, fix_ref, edge_ref, cw_ref, oa_ref, ob_ref, work):
    work[0:13] = fix_ref[0:13]
    for j in range(DCONV - 1):
        row = fix_ref[13 + j : 14 + j]
        for tap in range(j + 1):
            row = row + cw_ref[tap : tap + 1] * edge_ref[j - tap : j - tap + 1]
        work[13 + j : 14 + j] = row
    oa_ref[...] = work[:, :XA].astype(BF)
    ob_ref[:, : XBC - XA] = work[:, XA:].astype(BF)
    ob_ref[:, XBC - XA :] = b_ref[:, XBC - XA :]


def patch(dxa, dxb, fix, edge, cw):
    count, piece, _ = dxa.shape
    last = piece // 16 - 1
    tail = lambda n: pl.BlockSpec((None, 16, n), lambda i: (i, last, 0))
    return pl.pallas_call(
        patch_kernel,
        grid=(count,),
        in_specs=[tail(XA), tail(XD - XA), per((16, XBC)), per((8, XBC)), whole((DCONV, XBC))],
        out_specs=[tail(XA), tail(XD - XA)],
        out_shape=[jax.ShapeDtypeStruct(a.shape, BF) for a in (dxa, dxb)],
        scratch_shapes=[pltpu.VMEM((16, XBC), F32)],
        input_output_aliases={0: 0, 1: 1},
        name="patch",
    )(dxa, dxb, fix, edge, cw)


def input_grad_kernel(x_ref, dbr_ref, g_ref, dz_ref, dxa_ref, dxb_ref, wz_ref, wa_ref, wb_ref, out_ref, gain_ref, dn):
    piece = x_ref.shape[0]

    @pl.when(pl.program_id(0) == 0)
    def _():
        gain_ref[...] = jnp.zeros_like(gain_ref)

    for j in range(D // 256):
        cols = slice(j * 256, (j + 1) * 256)
        dn[:, cols] = (
            nt(dz_ref[...], wz_ref[cols, :]) + nt(dxa_ref[...], wa_ref[cols, :]) + nt(dxb_ref[...], wb_ref[cols, :])
        )

    def rows_of(i, c):
        rows = pl.ds(pl.multiple_of(i * 64, 64), 64)
        x = x_ref[rows, :].astype(F32)
        d = dn[rows, :]
        r = lax.rsqrt(jnp.mean(x * x, axis=-1, keepdims=True) + EPSILON)
        v = x * r
        gain_ref[...] += jnp.sum((d * v).reshape(8, 8, D), axis=0)
        dv = d * g_ref[...]
        q = jnp.mean(dv * v, axis=-1, keepdims=True)
        out_ref[rows, :] = (dbr_ref[rows, :].astype(F32) + r * (dv - v * q)).astype(BF)
        return c

    lax.fori_loop(0, piece // 64, rows_of, 0)


def input_grad(first, count, tokens, dbr, gain, dz, dxa, dxb, w_z, wa, wb):
    piece = tokens.shape[1]
    sds = jax.ShapeDtypeStruct
    return pl.pallas_call(
        input_grad_kernel,
        grid=(count,),
        in_specs=[
            per((piece, D), first),
            per((piece, D)),
            whole((1, D)),
            per((piece, DI)),
            per((piece, XA)),
            per((piece, XD - XA)),
            kept((D, DI)),
            kept((D, XA)),
            kept((D, XD - XA)),
        ],
        out_specs=[per((piece, D)), whole((8, D))],
        out_shape=[sds((count, piece, D), BF), sds((8, D), F32)],
        scratch_shapes=[pltpu.VMEM((piece, D), F32)],
        compiler_params=pltpu.CompilerParams(vmem_limit_bytes=LIMIT),
        name="input_grad",
    )(tokens, dbr, gain, dz, dxa, dxb, w_z, wa, wb)


def assemble_kernel(z, a, b, o, t, win, wo, g0, g1, g2, g3, h0, h1, h2):
    win[:, 0:DI] = z[...]
    win[:, DI : DI + XA] = a[...]
    win[:, DI + XA :] = b[:, : PROJ - DI - XA]
    wo[...] = o[...]
    g0[...] = t[0:1, : g0.shape[1]]
    g1[...] = t[1:2, : g1.shape[1]]
    g2[...] = t[2:3, : g2.shape[1]]
    g3[...] = t[3 : 3 + DCONV, : g3.shape[1]]
    last = t[7:8, :]
    h0[...] = last[:, 0:NH]
    h1[...] = last[:, NH : 2 * NH]
    h2[...] = last[:, 2 * NH : 3 * NH]


def assemble(z, a, b, o, t, n0, n1, n2):
    shapes = [(z.shape[0], PROJ), o.shape, (1, n0), (1, n1), (1, n2), (DCONV, n2), (1, NH), (1, NH), (1, NH)]
    return pl.pallas_call(
        assemble_kernel,
        in_specs=[IN_VMEM] * 5,
        out_specs=[IN_VMEM] * 9,
        out_shape=[jax.ShapeDtypeStruct(v, F32) for v in shapes],
        name="assemble",
    )(z, a, b, o, t)


def pass_on(block, axis, distance):
    devices = range(lax.axis_size(axis))
    route = [(i - distance, i) for i in devices if i - distance in devices]
    return lax.ppermute(block, axis, route)


def contract_rows(left, right):
    return lax.dot_general(left, right, (((0, 1), (0, 1)), ((), ())), preferred_element_type=F32)


def local(
    tokens,
    norm_gain,
    w_in,
    conv_weight,
    conv_bias,
    dt_bias,
    a_log,
    d_skip,
    gated_gain,
    w_out,
    lengths,
    cotangent,
):
    ranks = lax.axis_size("dp") * lax.axis_size("seq")
    place = lax.axis_index("seq")
    tokens = tokens[:, 0]
    cot = cotangent[:, 0]
    batches, piece, _ = tokens.shape
    rows = w_in.shape[0]

    depth = lax.axis_size("dp") // 2
    n0, n1, n2 = norm_gain.shape[0], gated_gain.shape[0], conv_bias.shape[0]
    widen = lambda v: jnp.pad(v, ((0, 0), (0, LN - v.shape[1])))
    small = [norm_gain[None], gated_gain[None], conv_bias[None], conv_weight]
    small = jnp.pad(jnp.concatenate([widen(v) for v in small]), ((0, 1), (0, 0)))
    wa, wb, small = gather(w_in, small, depth)
    wa, wb = wa.reshape(D, XA), wb.reshape(D, XD - XA)
    gain = small[:, 0, :n0].reshape(1, D)
    gg = small[:, 1, :n1].reshape(1, DI)
    cb = small[:, 2, :n2].reshape(1, XBC)
    cw = small[:, 3 : 3 + DCONV, :n2].transpose(1, 0, 2).reshape(DCONV, XBC)

    halo = pass_on(tokens[:, piece - 16 :], "seq", 1)
    valid = lengths[:, 0].astype(jnp.int32) - place.astype(jnp.int32) * piece
    lane_pad = ((0, 0), (0, LN - NH))
    dtb = jnp.pad(dt_bias[None], lane_pad)
    rate = -jnp.exp(a_log)
    rate_row = jnp.pad(rate[None], lane_pad)
    dsk = jnp.repeat(d_skip, HD)[None]

    first, count = 0, batches
    normed, ci, act, step, ld, sig, sloc, s, w_z, w_o = project(
        first, count, depth, valid, tokens, halo, gain, wa, wb, cw, cb, dtb, rate_row, w_in, w_out
    )
    w_z, w_o = w_z.reshape(D, DI), w_o.reshape(DI, D)
    out, gn, dbr, dz, dy, y, inc, dsin, ggrad = mix(
        first, count, valid, tokens, cot, normed, act, step, ld, sloc, s, w_z, w_o, gg, dsk
    )
    lead = (depth, 2, 2, 2)
    grad_wo = contract_rows(gn, dbr).astype(BF).reshape(lead + (n1, D))
    grad_wz = contract_rows(normed, dz).astype(BF).reshape(lead + (rows, DI))
    dxa, dxb, fix, edge, cgrad, hgrad, skip, shard_wo, shard_wz = scan_back(
        count, depth, ci, step, ld, sig, dy, y, inc, sloc, dsin, cw, cb, rate_row, dsk, grad_wo, grad_wz
    )
    dxa, dxb = patch(dxa, dxb, fix, pass_on(edge, "seq", -1), cw)
    tgrad, gain_grad = input_grad(first, count, tokens, dbr, gain, dz, dxa, dxb, w_z, wa, wb)
    grad_wa = contract_rows(normed, dxa).astype(BF).reshape(lead + (rows, XA))
    grad_wb = contract_rows(normed, dxb).astype(BF).reshape(lead + (rows, XD - XA))

    grad_cw = cgrad[:32].reshape(DCONV, 8, XBC).sum(1)
    heads = hgrad.reshape(2, 8, LN).sum(1)[:, :NH]
    heads = jnp.concatenate([heads[0], heads[1] * rate, skip.sum(0).reshape(NH, HD).sum(1)])
    split = lambda v, n: jnp.pad(v.reshape(-1, ranks, n).transpose(1, 0, 2), ((0, 0), (0, 0), (0, LN - n)))
    packed = jnp.concatenate(
        [
            split(gain_grad.sum(0), n0),
            split(ggrad.sum(0), n1),
            split(cgrad[32:].sum(0), n2),
            split(grad_cw, n2),
            jnp.broadcast_to(jnp.pad(heads, (0, LN - 3 * NH)), (ranks, 1, LN)),
        ],
        axis=1,
    )
    shard_wa, shard_wb, total = reduce(grad_wa, grad_wb, packed, depth)
    shard_win, shard_wo, g0, g1, g2, g3, h0, h1, h2 = assemble(shard_wz, shard_wa, shard_wb, shard_wo, total, n0, n1, n2)
    return (
        out[:, None],
        tgrad[:, None],
        g0.reshape(n0),
        shard_win,
        g3,
        g2.reshape(n2),
        h0.reshape(NH),
        h1.reshape(NH),
        h2.reshape(NH),
        g1.reshape(n1),
        shard_wo,
    )


def solution(mesh):
    shard = P(("dp", "seq"))
    row_shard = P(("dp", "seq"), None)
    col_shard = P(None, ("dp", "seq"))
    acts = P(None, "dp", "seq", None)
    return jax.shard_map(
        local,
        mesh=mesh,
        in_specs=(
            acts,
            shard,
            row_shard,
            col_shard,
            shard,
            P(),
            P(),
            P(),
            shard,
            row_shard,
            P(None, "dp"),
            acts,
        ),
        out_specs=(
            acts,
            acts,
            shard,
            row_shard,
            col_shard,
            shard,
            P(),
            P(),
            P(),
            shard,
            row_shard,
        ),
        check_vma=False,
    )
```

```python
from functools import partial

import jax
import jax.numpy as jnp
from jax import lax
from jax.experimental import pallas as pl
from jax.experimental.pallas import tpu as pltpu
from jax.sharding import PartitionSpec as P

D = 768
NH = 24
HD = 64
NS = 128
DCONV = 4
CL = 128
DI = 1536
XBC = 1792
PROJ = 3352
XD = 1920
XA = 1024
LN = 128
EPSILON = 1e-05

F32 = jnp.float32
BF = jnp.bfloat16
SROWS = 144


def nn(a, b):
    return lax.dot_general(a, b, (((1,), (0,)), ((), ())), preferred_element_type=F32)


def nt(a, b):
    return lax.dot_general(a, b, (((1,), (1,)), ((), ())), preferred_element_type=F32)


def tn(a, b):
    return lax.dot_general(a, b, (((0,), (0,)), ((), ())), preferred_element_type=F32)


def exact_nn(a, b):
    return lax.dot_general(
        a, b, (((1,), (0,)), ((), ())), precision=lax.Precision.HIGHEST, preferred_element_type=F32
    )


def sigmoid(v):
    return 0.5 * jnp.tanh(0.5 * v) + 0.5


def halves(v):
    top = v.astype(BF)
    return top, (v - top.astype(F32)).astype(BF)


def three(op, a, b):
    ah, al = halves(a)
    bh, bl = halves(b)
    return op(ah, bh) + op(al, bh) + op(ah, bl)


def fill_expander(ref):
    head = lax.broadcasted_iota(jnp.int32, (LN, DI), 0)
    lane = lax.broadcasted_iota(jnp.int32, (LN, DI), 1)
    e = jnp.where(head == lane // HD, 1.0, 0.0).astype(BF)
    ref[0:LN] = e
    ref[LN:] = e


def expand(v, e2):
    return nn(jnp.concatenate(halves(v), axis=1), e2[...])


def lower_mask(strict):
    row = lax.broadcasted_iota(jnp.int32, (CL, CL), 0)
    col = lax.broadcasted_iota(jnp.int32, (CL, CL), 1)
    return row > col if strict else row >= col


def half_masks():
    lane = lax.broadcasted_iota(jnp.int32, (1, 2 * HD), 1)
    left = jnp.where(lane < HD, 1.0, 0.0).astype(BF)
    right = jnp.where(lane < HD, 0.0, 1.0).astype(BF)
    return left, right


def lanes(j):
    return slice(j * LN, (j + 1) * LN)


def conv_running(ci_ref, j, base, cw, cb):
    total = cb
    for tap in range(DCONV):
        total = total + ci_ref[j, pl.ds(base + 5 + tap, CL), :] * cw[tap : tap + 1]
    return total


MESH_ID = pl.DeviceIdType.MESH
BOTH = slice(None)


class Here:
    def __init__(self, depth):
        dp, seq = lax.axis_index("dp"), lax.axis_index("seq")
        self.depth = depth
        self.levels = depth.bit_length() - 1
        self.z, self.y = dp // 2, dp % 2
        self.x, self.c = seq // 2, seq % 2
        self.rank = dp * 4 + seq

    def device(self, z=None, y=None, x=None, c=None):
        z = self.z if z is None else z
        y = self.y if y is None else y
        x = self.x if x is None else x
        c = self.c if c is None else c
        return (z * 2 + y, x * 2 + c)

    def across(self, level):
        size = 1 << level
        return self.z + size * (1 - 2 * ((self.z // size) % 2))

    def block(self, level):
        size = 1 << level
        return (self.z // size) * size, size

    def block_across(self, level):
        size = 1 << level
        return (self.z // size) * size + size * (1 - 2 * ((self.z // size) % 2)), size

    def partners(self):
        near = [self.device(c=1 - self.c), self.device(x=1 - self.x), self.device(y=1 - self.y)]
        return near + [self.device(z=self.across(level)) for level in range(self.levels)]

    def greet_partners(self):
        barrier = pltpu.get_barrier_semaphore()
        others = self.partners()
        for other in others:
            pl.semaphore_signal(barrier, inc=1, device_id=other, device_id_type=MESH_ID)
        pl.semaphore_wait(barrier, len(others))

    def greet_all(self, ranks):
        barrier = pltpu.get_barrier_semaphore()

        def hail(i, carry):
            other = (self.rank + i) % ranks
            pl.semaphore_signal(barrier, inc=1, device_id=(other // 4, other % 4), device_id_type=MESH_ID)
            return carry

        lax.fori_loop(1, ranks, hail, 0)
        pl.semaphore_wait(barrier, ranks - 1)


class Plan:
    def __init__(self, send, recv):
        self.send, self.recv, self.made, self.segments = send, recv, [], [[]]

    def do(self, action):
        self.segments[-1].append(action)

    def copy(self, i, source, target, device):
        return pltpu.make_async_remote_copy(
            src_ref=source,
            dst_ref=target,
            send_sem=self.send.at[i],
            recv_sem=self.recv.at[i],
            device_id=device,
            device_id_type=MESH_ID,
        )

    def start(self, parts, device):
        waits = []
        for source, target, landing in parts:
            i = len(self.made)
            copy = self.copy(i, source, target, device)
            self.do(copy.start)
            self.made.append(copy)
            waits.append(self.copy(i, source, landing, device))
        return waits

    def arrived(self, waits):
        for w in waits:
            self.do(w.wait_recv)

    def trace(self, streams):
        streams = list(streams)
        while streams:
            for stream in list(streams):
                try:
                    next(stream)
                except StopIteration:
                    streams.remove(stream)
            self.segments.append([])

    def run(self, n):
        for action in self.segments[n]:
            action()

    def run_from(self, n):
        for k in range(n, len(self.segments)):
            self.run(k)
        for copy in self.made:
            copy.wait_send()


def everyone(rank, ranks, source, target, send, recv):
    def one(i):
        other = (rank + i) % ranks
        return pltpu.make_async_remote_copy(
            src_ref=source(other),
            dst_ref=target(rank),
            send_sem=send.at[i],
            recv_sem=recv.at[i],
            device_id=(other // 4, other % 4),
            device_id_type=MESH_ID,
        )

    def begin(i, carry):
        one(i).start()
        return carry

    def end(i, carry):
        copy = one(i)
        copy.wait_send()
        copy.wait_recv()
        return carry

    return (lambda: lax.fori_loop(1, ranks, begin, 0)), (lambda: lax.fori_loop(1, ranks, end, 0))


def gather_stream(here, plan, ref, first):
    z, y, x, c = here.z, here.y, here.x, here.c
    a_dev = here.device(x=1 - x) if first == "x" else here.device(y=1 - y)
    b_dev = here.device(y=1 - y) if first == "x" else here.device(x=1 - x)
    sibling = here.device(c=1 - c)
    cores = []

    def mine(zs, core):
        return ref.at[zs, y, x, core]

    def a_there(zs, core):
        return ref.at[zs, y, 1 - x, core] if first == "x" else ref.at[zs, 1 - y, x, core]

    def line(zs, core):
        return ref.at[zs, y, BOTH, core] if first == "x" else ref.at[zs, BOTH, x, core]

    def line_there(zs, core):
        return ref.at[zs, 1 - y, BOTH, core] if first == "x" else ref.at[zs, BOTH, 1 - x, core]

    def to_core(where, zs):
        cores.extend(plan.start([(where(zs, c), where(zs, c), where(zs, 1 - c))], sibling))

    def start_a(zs):
        waits = plan.start([(mine(zs, c), mine(zs, c), a_there(zs, c))], a_dev)
        to_core(mine, zs)
        return waits

    def start_b(zs, waits):
        plan.arrived(waits)
        out = plan.start([(line(zs, c), line(zs, c), line_there(zs, c))], b_dev)
        to_core(a_there, zs)
        return out

    sets = [pl.ds(z, 1)]
    waiting_a, waiting_b = [], []
    for level in range(here.levels):
        base, size = here.block(level)
        far, _ = here.block_across(level)
        own, theirs = pl.ds(base, size), pl.ds(far, size)
        zwait = plan.start([(mine(own, c), mine(own, c), mine(theirs, c))], here.device(z=here.across(level)))
        waiting_a.append((sets[-1], start_a(sets[-1])))
        sets.append(theirs)
        yield
        if level:
            zs, w = waiting_a.pop(0)
            waiting_b.append((zs, start_b(zs, w)))
        plan.arrived(zwait)
    waiting_a.append((sets[-1], start_a(sets[-1])))
    while waiting_a:
        yield
        zs, w = waiting_a.pop(0)
        waiting_b.append((zs, start_b(zs, w)))
    while waiting_b:
        yield
        zs, w = waiting_b.pop(0)
        plan.arrived(w)
        to_core(line_there, zs)
    yield
    plan.arrived(cores)


def gather_copies(levels):
    return 2 * (levels + 5 * (levels + 1))


def gather_kernel(
    w_in,
    g_in,
    gg_in,
    cb_in,
    cw_in,
    dtb_in,
    alog_in,
    dsk_in,
    tok_in,
    xa_out,
    xb_out,
    halo,
    gain,
    gg,
    cb,
    cw,
    dtb,
    rate,
    dsk,
    xa_in,
    xb_in,
    small_in,
    small,
    send,
    recv,
    ssend,
    srecv,
    place_sem,
    halo_sem,
    *,
    depth,
    ranks,
):
    here = Here(depth)
    xa_in[...] = w_in[:, DI : DI + XA].astype(BF)
    xb_in[...] = jnp.zeros_like(xb_in)
    xb_in[:, : PROJ - DI - XA] = w_in[:, DI + XA :].astype(BF)
    n0, n1, n2 = g_in.shape[1], gg_in.shape[1], cb_in.shape[1]
    small_in[...] = jnp.zeros_like(small_in)
    small_in[0:1, :n0] = g_in[...]
    small_in[1:2, :n1] = gg_in[...]
    small_in[2:3, :n2] = cb_in[...]
    small_in[3 : 3 + DCONV, :n2] = cw_in[...]
    slot = (here.z, here.y, here.x, here.c)
    own = [
        pltpu.make_async_copy(xa_in, xa_out.at[slot], place_sem.at[0]),
        pltpu.make_async_copy(xb_in, xb_out.at[slot], place_sem.at[1]),
        pltpu.make_async_copy(small_in, small.at[here.rank], place_sem.at[2]),
    ]
    seq = here.x * 2 + here.c
    dp = here.z * 2 + here.y
    piece = tok_in.shape[1]
    after = pltpu.make_async_remote_copy(
        src_ref=tok_in.at[:, pl.ds(piece - 16, 16)],
        dst_ref=halo,
        send_sem=halo_sem.at[0],
        recv_sem=halo_sem.at[1],
        device_id=(dp, (seq + 1) % 4),
        device_id_type=MESH_ID,
    )

    @pl.when(seq == 0)
    def _():
        halo[...] = jnp.zeros_like(halo)

    here.greet_all(ranks)
    for copy in own:
        copy.start()
    start, finish = everyone(here.rank, ranks, lambda other: small_in, lambda rank: small.at[rank], ssend, srecv)
    for copy in own:
        copy.wait()
    plan = Plan(send, recv)
    plan.trace([gather_stream(here, plan, xa_out, "x"), gather_stream(here, plan, xb_out, "y")])
    plan.run(0)
    start()

    @pl.when(seq < 3)
    def _():
        after.start()

    dtb[...] = jnp.zeros_like(dtb)
    dtb[:, 0:NH] = dtb_in[...]
    rate[...] = jnp.zeros_like(rate)
    rate[:, 0:NH] = -jnp.exp(alog_in[...])
    for h in range(NH):
        dsk[:, h * HD : (h + 1) * HD] = jnp.broadcast_to(dsk_in[:, h : h + 1], (1, HD))
    plan.run(1)
    plan.run(2)
    finish()
    for r in range(ranks):
        gain[:, r * n0 : (r + 1) * n0] = small[r, 0:1, :n0]
        gg[:, r * n1 : (r + 1) * n1] = small[r, 1:2, :n1]
        cb[:, r * n2 : (r + 1) * n2] = small[r, 2:3, :n2]
        cw[:, r * n2 : (r + 1) * n2] = small[r, 3 : 3 + DCONV, :n2]

    @pl.when(seq > 0)
    def _():
        after.wait_recv()

    @pl.when(seq < 3)
    def _():
        after.wait_send()

    plan.run_from(3)


ANY = pl.BlockSpec(memory_space=pl.ANY)
IN_VMEM = pl.BlockSpec(memory_space=pltpu.VMEM)


def gather(w_in, gain, gg, cb, cw, dtb, alog, dsk, tokens, depth):
    ranks = depth * 8
    rows = w_in.shape[0]
    lead = (depth, 2, 2, 2)
    sds = jax.ShapeDtypeStruct
    n = gather_copies(depth.bit_length() - 1)
    dma = pltpu.SemaphoreType.DMA
    return pl.pallas_call(
        partial(gather_kernel, depth=depth, ranks=ranks),
        in_specs=[IN_VMEM] * 8 + [ANY],
        out_specs=[ANY] * 2 + [IN_VMEM] * 8,
        out_shape=[
            sds(lead + (rows, XA), BF),
            sds(lead + (rows, XD - XA), BF),
            sds((tokens.shape[0], 16, D), BF),
            sds((1, D), F32),
            sds((1, DI), F32),
            sds((1, XBC), F32),
            sds((DCONV, XBC), F32),
            sds((1, LN), F32),
            sds((1, LN), F32),
            sds((1, DI), F32),
        ],
        scratch_shapes=[
            pltpu.VMEM((rows, XA), BF),
            pltpu.VMEM((rows, XD - XA), BF),
            pltpu.VMEM((8, LN), F32),
            pltpu.VMEM((ranks, 8, LN), F32),
            dma((n,)),
            dma((n,)),
            dma((ranks,)),
            dma((ranks,)),
            dma((3,)),
            dma((2,)),
        ],
        compiler_params=pltpu.CompilerParams(collective_id=0, has_side_effects=True),
        name="gather",
    )(w_in, gain, gg, cb, cw, dtb, alog, dsk, tokens)


def reduce_stream(here, plan, item, first):
    part, acc, core_in, line_in, side_in, z_in, put, own_sem = item
    z, y, x, c = here.z, here.y, here.x, here.c
    one_dev = here.device(y=1 - y) if first == "y" else here.device(x=1 - x)
    two_dev = here.device(x=1 - x) if first == "y" else here.device(y=1 - y)
    sibling = here.device(c=1 - c)
    sets = []
    for level in reversed(range(here.levels)):
        sets.append(here.block_across(level))
    sets.append((z, 1))
    slots = [pl.ds(zs[0], zs[1]) for zs in sets]
    mine = pltpu.make_async_copy(part.at[BOTH, BOTH, BOTH, c], acc, own_sem)
    plan.do(mine.start)

    def add(target, source):
        acc[target] = (acc[target].astype(F32) + source.astype(F32)).astype(BF)

    def line_add(zs):
        for k in range(zs[1]):
            for a in range(2):
                for b in range(2):
                    add((zs[0] + k, a, b), core_in[zs[0] + k, a, b])

    def side_add(zs):
        for k in range(zs[1]):
            for a in range(2):
                add((zs[0] + k, y, a) if first == "y" else (zs[0] + k, a, x), line_in[zs[0] + k, a])

    def last_add(zs):
        for k in range(zs[1]):
            add((zs[0] + k, y, x), side_in[zs[0] + k])

    cores = [plan.start([(part.at[s, BOTH, BOTH, 1 - c], core_in.at[s], core_in.at[s])], sibling) for s in slots]
    plan.do(mine.wait)
    yield
    lines, sides = [], []
    n = len(sets)
    for step in range(n + 2):
        if step < n:
            s = slots[step]
            plan.arrived(cores[step])
            plan.do(partial(line_add, sets[step]))
            give = acc.at[s, 1 - y, BOTH] if first == "y" else acc.at[s, BOTH, 1 - x]
            lines.append(plan.start([(give, line_in.at[s], line_in.at[s])], one_dev))
        if 1 <= step <= n:
            s = slots[step - 1]
            plan.arrived(lines[step - 1])
            plan.do(partial(side_add, sets[step - 1]))
            give = acc.at[s, y, 1 - x] if first == "y" else acc.at[s, 1 - y, x]
            sides.append(plan.start([(give, side_in.at[s], side_in.at[s])], two_dev))
        if step >= 2:
            plan.arrived(sides[step - 2])
            plan.do(partial(last_add, sets[step - 2]))
            if step == 2:
                level = here.levels - 1
                s, size = slots[0], sets[0][1]
                zwait = plan.start(
                    [(acc.at[s, y, x], z_in[0].at[0:size], z_in[0].at[0:size])], here.device(z=here.across(level))
                )
        yield

    def z_add(base, size, got):
        for k in range(size):
            add((base + k, y, x), got[k])

    def z_end(base, got):
        put(got[0].astype(F32) + acc[base, y, x].astype(F32))

    for at_level, level in enumerate(reversed(range(here.levels))):
        base, size = here.block(level)
        plan.arrived(zwait)
        if level:
            plan.do(partial(z_add, base, size, z_in[at_level]))
            far, size = here.block_across(level - 1)
            landing = z_in[at_level + 1].at[0:size]
            zwait = plan.start(
                [(acc.at[pl.ds(far, size), y, x], landing, landing)], here.device(z=here.across(level - 1))
            )
            yield
        else:
            plan.do(partial(z_end, base, z_in[at_level]))


def reduce_copies(levels):
    return 2 * (3 * (levels + 1) + levels)


def reduce_scratch(depth, tile):
    levels = depth.bit_length() - 1
    return [
        pltpu.VMEM((depth, 2, 2) + tile, BF),
        pltpu.VMEM((depth, 2, 2) + tile, BF),
        pltpu.VMEM((depth, 2) + tile, BF),
        pltpu.VMEM((depth,) + tile, BF),
    ] + [pltpu.VMEM((1 << level,) + tile, BF) for level in reversed(range(levels))]


def reduce_items(here, plan, parts, outs, scratch, own_sems):
    each = 4 + here.levels
    streams = []
    for k, first in enumerate(("y", "x")):
        bufs = scratch[k * each : (k + 1) * each]

        def put(v, k=k):
            outs[k][...] = v

        item = (parts[k], *bufs[:4], bufs[4:], put, own_sems.at[k])
        streams.append(reduce_stream(here, plan, item, first))
    plan.trace(streams)


def reduce_kernel(
    pa,
    pb,
    gain_ref,
    gg_ref,
    conv_ref,
    head_ref,
    rate_ref,
    oa,
    ob,
    small_out,
    send,
    recv,
    ssend,
    srecv,
    small_in,
    small_got,
    own_sems,
    *scratch,
    depth,
    ranks,
):
    here = Here(depth)
    here.greet_all(ranks)
    start, finish = everyone(
        here.rank, ranks, lambda other: small_in.at[other], lambda rank: small_got.at[rank], ssend, srecv
    )
    plan = Plan(send, recv)
    reduce_items(here, plan, (pa, pb), (oa, ob), scratch, own_sems)
    plan.run(0)
    small_in[...] = jnp.zeros_like(small_in)
    total = lambda v: jnp.sum(v, axis=0, keepdims=True)
    gain, gg = total(gain_ref[...]), total(gg_ref[...])
    taps = [total(conv_ref[8 * t : 8 * t + 8]) for t in range(DCONV + 1)]
    heads = [
        total(head_ref[0:8])[:, :NH],
        (total(head_ref[8:16]) * rate_ref[...])[:, :NH],
        total(head_ref[16:24])[:, :NH],
    ]
    n0, n1, n2 = D // ranks, DI // ranks, XBC // ranks
    for r in range(ranks):
        small_in[r, 0:1, :n0] = gain[:, r * n0 : (r + 1) * n0]
        small_in[r, 1:2, :n1] = gg[:, r * n1 : (r + 1) * n1]
        small_in[r, 2:3, :n2] = taps[DCONV][:, r * n2 : (r + 1) * n2]
        for t in range(DCONV):
            small_in[r, 3 + t : 4 + t, :n2] = taps[t][:, r * n2 : (r + 1) * n2]
        for k in range(3):
            small_in[r, 7:8, k * NH : (k + 1) * NH] = heads[k]
    plan.run(1)
    start()
    plan.run_from(2)
    finish()

    def add(i, sum_so_far):
        return sum_so_far + jnp.where(i == here.rank, small_in[i], small_got[i])

    small_out[...] = lax.fori_loop(0, ranks, add, jnp.zeros(small_out.shape, F32))


def reduce(pa, pb, gain, gg, conv, head, rate, depth):
    ranks = depth * 8
    sds = jax.ShapeDtypeStruct
    dma = pltpu.SemaphoreType.DMA
    n = reduce_copies(depth.bit_length() - 1)
    small = pltpu.VMEM((ranks, 8, LN), F32)
    scratch = [dma((n,)), dma((n,)), dma((ranks,)), dma((ranks,)), small, small, dma((2,))]
    for part in (pa, pb):
        scratch += reduce_scratch(depth, part.shape[-2:])
    return pl.pallas_call(
        partial(reduce_kernel, depth=depth, ranks=ranks),
        in_specs=[ANY] * 2 + [IN_VMEM] * 5,
        out_specs=[IN_VMEM] * 3,
        out_shape=[sds(a.shape[4:], F32) for a in (pa, pb)] + [sds((8, LN), F32)],
        scratch_shapes=scratch,
        compiler_params=pltpu.CompilerParams(collective_id=1, has_side_effects=True, vmem_limit_bytes=LIMIT),
        name="reduce",
    )(pa, pb, gain, gg, conv, head, rate)


def whole(shape):
    return pl.BlockSpec(shape, lambda i: (0,) * len(shape))


def kept(shape):
    return pl.BlockSpec(shape, lambda i: (0,) * len(shape), pipeline_mode=pl.Buffered(1))


def per(shape, first=0):
    rest = (0,) * len(shape)
    return pl.BlockSpec((None,) + shape, lambda i: (first + i,) + rest)


SMEM = pl.BlockSpec(memory_space=pltpu.SMEM)
LIMIT = 67_000_000


def project_kernel(
    vlen_ref,
    x_ref,
    xh_ref,
    g_ref,
    wa_ref,
    wb_ref,
    cw_ref,
    cb_ref,
    dtb_ref,
    rate_ref,
    win_ref,
    wo_ref,
    nrm_ref,
    ci_ref,
    act_ref,
    step_ref,
    l_ref,
    sig_ref,
    sloc_ref,
    s_ref,
    z_out,
    o_out,
    nx,
    xw,
    state,
    e2,
    z_in,
    o_in,
    send,
    recv,
    place_sem,
    *,
    first,
    count,
    depth,
):
    piece = x_ref.shape[0]
    chunks = piece // CL
    section = pl.program_id(0)
    here = Here(depth)
    valid = vlen_ref[first + section, 0] - (here.x * 2 + here.c) * piece
    slot = (here.z, here.y, here.x, here.c)
    own = [
        pltpu.make_async_copy(z_in, z_out.at[slot], place_sem.at[0]),
        pltpu.make_async_copy(o_in, o_out.at[slot], place_sem.at[1]),
    ]
    plan = Plan(send, recv)
    plan.trace([gather_stream(here, plan, z_out, "x"), gather_stream(here, plan, o_out, "y")])

    @pl.when(section == 0)
    def _():
        z_in[...] = win_ref[:, 0:DI].astype(BF)
        o_in[...] = wo_ref[...].astype(BF)
        here.greet_partners()
        for copy in own:
            copy.start()
        for copy in own:
            copy.wait()
        plan.run(0)

    def norm(v):
        v = v.astype(F32)
        r = lax.rsqrt(jnp.mean(v * v, axis=-1, keepdims=True) + EPSILON)
        return (v * r * g_ref[...]).astype(BF)

    nx[0:16] = norm(xh_ref[...])

    def norm_rows(i, c):
        rows = pl.ds(pl.multiple_of(i * 64, 64), 64)
        v = norm(x_ref[rows, :])
        nx[pl.ds(pl.multiple_of(i * 64 + 16, 16), 64), :] = v
        nrm_ref[rows, :] = v
        return c

    lax.fori_loop(0, piece // 64, norm_rows, 0)

    for j in range(XBC // 256):
        w = wa_ref[:, j * 256 : (j + 1) * 256] if j < XA // 256 else wb_ref[:, j * 256 - XA : (j + 1) * 256 - XA]
        ci = nn(nx[...], w)
        ci_ref[2 * j] = ci[8:, :LN]
        ci_ref[2 * j + 1] = ci[8:, LN:]
    dt_raw = nn(nx[16:], wb_ref[:, XBC - XA :]) + dtb_ref[...]
    row = lax.broadcasted_iota(jnp.int32, (piece, LN), 0)
    mask = jnp.where(row < valid, 1.0, 0.0)
    step_ref[...] = (jnp.maximum(dt_raw, 0.0) + jnp.log1p(jnp.exp(-jnp.abs(dt_raw)))) * mask
    sig_ref[...] = mask / (1.0 + jnp.exp(-dt_raw))

    @pl.when(pl.program_id(0) == 0)
    def _():
        fill_expander(e2)

    tri = jnp.where(lower_mask(False), 1.0, 0.0)
    state[...] = jnp.zeros_like(state)

    slots = count * chunks
    late = slots // 2 + 1
    steps = min(len(plan.segments) - 1, slots - late + 1)

    def chunk(k, total):
        base = pl.multiple_of(k * CL, CL)
        rows = pl.ds(base, CL)
        for n in range(steps):

            @pl.when(section * chunks + k == (late + n - 1 if n else 0))
            def _():
                plan.run(n + 1)

        step = step_ref[rows, :]
        ld = exact_nn(tri, step * rate_ref[...])
        l_ref[rows, :] = ld
        end = ld[CL - 1 :]
        tail = expand(step * jnp.exp(end - ld), e2)
        for j in range(XBC // LN):
            run = conv_running(ci_ref, j, base, cw_ref[:, lanes(j)], cb_ref[:, lanes(j)])
            act = run * sigmoid(run)
            act_ref[rows, lanes(j)] = act
            if j < DI // LN:
                xw[:, lanes(j)] = (act * tail[:, lanes(j)]).astype(BF)
        b = act_ref[rows, DI : DI + NS].astype(BF)
        sloc_ref[k] = state[...].astype(BF)
        keep = expand(jnp.exp(jnp.broadcast_to(end, (8, LN))), e2)[0:1]
        state[...] = keep * state[...] + tn(b, xw[...])
        return total + end

    total = lax.fori_loop(0, chunks, chunk, jnp.zeros((1, LN), F32))
    s_ref[0:NS] = state[...].astype(BF)
    keep = expand(jnp.exp(jnp.broadcast_to(total, (8, LN))), e2)[0:1]
    top, low = halves(keep)
    s_ref[NS : NS + 16] = jnp.concatenate([top, low, jnp.zeros((14, DI), BF)], axis=0)

    @pl.when(section == count - 1)
    def _():
        plan.run_from(steps + 1)


def project(first, count, depth, valid, tokens, halo, gain, wa, wb, cw, cb, dtb, rate, w_in, w_out):
    piece = tokens.shape[1]
    chunks = piece // CL
    lead = (depth, 2, 2, 2)
    n = gather_copies(depth.bit_length() - 1)
    sds = jax.ShapeDtypeStruct
    dma = pltpu.SemaphoreType.DMA
    return pl.pallas_call(
        partial(project_kernel, first=first, count=count, depth=depth),
        grid=(count,),
        in_specs=[
            SMEM,
            per((piece, D), first),
            per((16, D), first),
            whole((1, D)),
            kept((D, XA)),
            kept((D, XD - XA)),
            whole((DCONV, XBC)),
            whole((1, XBC)),
            whole((1, LN)),
            whole((1, LN)),
            kept(w_in.shape),
            kept(w_out.shape),
        ],
        out_specs=[
            per((piece, D)),
            per((XBC // LN, piece + 8, LN)),
            per((piece, XBC)),
            per((piece, LN)),
            per((piece, LN)),
            per((piece, LN)),
            per((chunks, NS, DI)),
            per((SROWS, DI)),
            ANY,
            ANY,
        ],
        out_shape=[
            sds((count, piece, D), BF),
            sds((count, XBC // LN, piece + 8, LN), F32),
            sds((count, piece, XBC), F32),
            sds((count, piece, LN), F32),
            sds((count, piece, LN), F32),
            sds((count, piece, LN), F32),
            sds((count, chunks, NS, DI), BF),
            sds((count, SROWS, DI), BF),
            sds(lead + (w_in.shape[0], DI), BF),
            sds(lead + w_out.shape, BF),
        ],
        scratch_shapes=[
            pltpu.VMEM((piece + 16, D), BF),
            pltpu.VMEM((CL, DI), BF),
            pltpu.VMEM((NS, DI), F32),
            pltpu.VMEM((2 * LN, DI), BF),
            pltpu.VMEM((w_in.shape[0], DI), BF),
            pltpu.VMEM(w_out.shape, BF),
            dma((n,)),
            dma((n,)),
            dma((2,)),
        ],
        compiler_params=pltpu.CompilerParams(vmem_limit_bytes=LIMIT, collective_id=4, has_side_effects=True),
        name="project",
    )(valid, tokens, halo, gain, wa, wb, cw, cb, dtb, rate, w_in, w_out)


class Exchange:
    def __init__(self, own, sib, out, got, swap_send, swap_recv, far_send, far_recv, giver):
        dp, seq = lax.axis_index("dp"), lax.axis_index("seq")
        self.x, self.c = seq // 2, seq % 2
        self.sibling = (dp, self.x * 2 + 1 - self.c)
        self.across = (dp, (1 - self.x) * 2 + self.c)
        self.own, self.sib, self.out, self.got = own, sib, out, got
        self.sems = (swap_send, swap_recv, far_send, far_recv)
        self.giver = giver

    def greet(self):
        barrier = pltpu.get_barrier_semaphore()
        for other in (self.sibling, self.across):
            pl.semaphore_signal(barrier, inc=1, device_id=other, device_id_type=pl.DeviceIdType.MESH)
        pl.semaphore_wait(barrier, 2)

    def swap(self, i):
        return pltpu.make_async_remote_copy(
            src_ref=self.own.at[i],
            dst_ref=self.sib.at[i],
            send_sem=self.sems[0].at[i],
            recv_sem=self.sems[1].at[i],
            device_id=self.sibling,
            device_id_type=pl.DeviceIdType.MESH,
        )

    def far(self, i):
        return pltpu.make_async_remote_copy(
            src_ref=self.out.at[i],
            dst_ref=self.got.at[i],
            send_sem=self.sems[2].at[i],
            recv_sem=self.sems[3].at[i],
            device_id=self.across,
            device_id_type=pl.DeviceIdType.MESH,
        )

    def decay(self, ref, i):
        return ref[i, NS : NS + 1].astype(F32) + ref[i, NS + 1 : NS + 2].astype(F32)

    def begin(self, count):
        for i in range(count):
            self.swap(i).start()

    def hand_over(self, i, coefficients):
        self.swap(i).wait_recv()

        @pl.when(self.x == self.giver)
        def _():
            f, g = coefficients(self.decay(self.own, i), self.decay(self.sib, i))
            self.out[i] = (f * self.own[i, 0:NS].astype(F32) + g * self.sib[i, 0:NS].astype(F32)).astype(BF)
            self.far(i).start()

    def end(self, count):
        for i in range(count):
            self.swap(i).wait_send()

            @pl.when(self.x == self.giver)
            def _():
                self.far(i).wait_send()


def exchange_scratch(count):
    dma = pltpu.SemaphoreType.DMA((count,))
    return [
        pltpu.VMEM((count, SROWS, DI), BF),
        pltpu.VMEM((count, NS, DI), BF),
        pltpu.VMEM((count, NS, DI), BF),
        dma,
        dma,
        dma,
        dma,
    ]


def mix_kernel(
    vlen_ref,
    cot_ref,
    nrm_ref,
    act_ref,
    step_ref,
    l_ref,
    sloc_ref,
    s_ref,
    wz_ref,
    wo_ref,
    gg_ref,
    dsk_ref,
    gn_ref,
    dbr_ref,
    dz_ref,
    dy_ref,
    y_ref,
    incoming,
    dsin_ref,
    ggrad_ref,
    zs,
    dgn,
    dsacc,
    yf,
    work,
    e2,
    sib,
    out,
    got,
    *sems,
    first,
    count,
):
    piece = cot_ref.shape[0]
    chunks = piece // CL
    section = pl.program_id(0)
    valid = vlen_ref[first + section, 0] - lax.axis_index("seq") * piece
    states = Exchange(s_ref, sib, out, got, *sems, giver=0)
    even = states.c == 0
    weigh = lambda own, sibs: (jnp.where(even, sibs, 1.0), jnp.where(even, 1.0, own))

    @pl.when(section == 0)
    def _():
        ggrad_ref[...] = jnp.zeros_like(ggrad_ref)
        fill_expander(e2)
        states.greet()
        states.begin(count)
        states.hand_over(0, weigh)

    row = lax.broadcasted_iota(jnp.int32, (piece, 1), 0)
    live = row < valid
    dbr_ref[...] = jnp.where(live, cot_ref[...].astype(F32), 0.0).astype(BF)
    for j in range(DI // 256):
        cols = slice(j * 256, (j + 1) * 256)
        zs[:, cols] = nn(nrm_ref[...], wz_ref[:, cols])
        dgn[:, cols] = nt(dbr_ref[...], wo_ref[cols, :])

    @pl.when(states.x == 0)
    def _():
        incoming[...] = jnp.where(even, 0.0, 1.0) * sib[section, 0:NS].astype(F32)

    @pl.when(states.x == 1)
    def _():
        states.far(section).wait_recv()
        f = jnp.where(even, 1.0, states.decay(sib, section))
        incoming[...] = f * got[section].astype(F32) + jnp.where(even, 0.0, 1.0) * sib[section, 0:NS].astype(F32)

    low = lower_mask(False)
    left, right = half_masks()
    dsacc[...] = jnp.zeros_like(dsacc)

    def chunk(k, before):
        base = pl.multiple_of(k * CL, CL)
        rows = pl.ds(base, CL)
        for n in range(1, count):

            @pl.when((section == 0) & (k == n - 1))
            def _():
                states.hand_over(n, weigh)

        step = step_ref[rows, :]
        ld = l_ref[rows, :]
        ldt = ld.T
        start = (before * incoming[...] + sloc_ref[k].astype(F32)).astype(BF)
        step_e = expand(step, e2)
        grow = expand(jnp.exp(ld), e2)
        b = act_ref[rows, DI : DI + NS].astype(BF)
        c, c_low = halves(act_ref[rows, DI + NS :])
        scores = jnp.where(low, nt(c, b), 0.0)
        squares = jnp.zeros((CL, LN), F32)
        for j in range(DI // LN):
            x = act_ref[rows, lanes(j)]
            xd = (x * step_e[:, lanes(j)]).astype(BF)
            mixes = []
            for h in (2 * j, 2 * j + 1):
                gap = jnp.minimum(ld[:, h : h + 1] - ldt[h : h + 1, :], 0.0)
                mixes.append((jnp.exp(gap) * scores).astype(BF))
            block = jnp.concatenate([xd * left, xd * right], axis=0)
            st = start[:, lanes(j)]
            y = nn(jnp.concatenate(mixes, axis=1), block) + (nn(c, st) + nn(c_low, st)) * grow[:, lanes(j)]
            y_ref[rows, lanes(j)] = y
            full = y + dsk_ref[:, lanes(j)] * x
            yf[:, lanes(j)] = full
            z = zs[rows, lanes(j)]
            u = full * (z * sigmoid(z))
            squares = squares + u * u
        r = lax.rsqrt(jnp.sum(squares, axis=-1, keepdims=True) * (1.0 / DI) + EPSILON)
        inner = jnp.zeros((CL, LN), F32)
        for j in range(DI // LN):
            z = zs[rows, lanes(j)]
            v = yf[:, lanes(j)] * (z * sigmoid(z)) * r
            gain = gg_ref[:, lanes(j)]
            gn_ref[rows, lanes(j)] = (v * gain).astype(BF)
            dg = dgn[rows, lanes(j)]
            gv = dg * v
            ggrad_ref[:, lanes(j)] += jnp.sum(gv.reshape(CL // 8, 8, LN), axis=0)
            inner = inner + gv * gain
        q = jnp.sum(inner, axis=-1, keepdims=True) * (1.0 / DI)
        for j in range(DI // LN):
            z = zs[rows, lanes(j)]
            s = sigmoid(z)
            sz = z * s
            full = yf[:, lanes(j)]
            v = full * sz * r
            du = r * (dgn[rows, lanes(j)] * gg_ref[:, lanes(j)] - v * q)
            dy = du * sz
            dy_ref[rows, lanes(j)] = dy
            dz_ref[rows, lanes(j)] = (du * full * (s + sz * (1.0 - s))).astype(BF)
            work[:, lanes(j)] = (dy * grow[:, lanes(j)]).astype(BF)
        dsacc[...] += before * tn(c, work[...])
        return before * grow[CL - 1 :]

    lax.fori_loop(0, chunks, chunk, jnp.ones((1, DI), F32))
    dsin_ref[0:NS] = dsacc[...].astype(BF)
    dsin_ref[NS:] = s_ref[section, NS:]
    @pl.when(section == count - 1)
    def _():
        states.end(count)


def mix(first, count, valid, cot, normed, act, step, ld, sloc, s, w_z, w_o, gg, dsk):
    piece = cot.shape[1]
    chunks = piece // CL
    sds = jax.ShapeDtypeStruct
    return pl.pallas_call(
        partial(mix_kernel, first=first, count=count),
        grid=(count,),
        in_specs=[
            SMEM,
            per((piece, D), first),
            per((piece, D)),
            per((piece, XBC)),
            per((piece, LN)),
            per((piece, LN)),
            per((chunks, NS, DI)),
            kept((count, SROWS, DI)),
            kept((D, DI)),
            kept((DI, D)),
            whole((1, DI)),
            whole((1, DI)),
        ],
        out_specs=[
            per((piece, DI)),
            per((piece, D)),
            per((piece, DI)),
            per((piece, DI)),
            per((piece, DI)),
            per((NS, DI)),
            per((SROWS, DI)),
            whole((8, DI)),
        ],
        out_shape=[
            sds((count, piece, DI), BF),
            sds((count, piece, D), BF),
            sds((count, piece, DI), BF),
            sds((count, piece, DI), F32),
            sds((count, piece, DI), F32),
            sds((count, NS, DI), F32),
            sds((count, SROWS, DI), BF),
            sds((8, DI), F32),
        ],
        scratch_shapes=[
            pltpu.VMEM((piece, DI), F32),
            pltpu.VMEM((piece, DI), F32),
            pltpu.VMEM((NS, DI), F32),
            pltpu.VMEM((CL, DI), F32),
            pltpu.VMEM((CL, DI), BF),
            pltpu.VMEM((2 * LN, DI), BF),
        ]
        + exchange_scratch(count),
        compiler_params=pltpu.CompilerParams(vmem_limit_bytes=LIMIT, collective_id=2, has_side_effects=True),
        name="mix",
    )(valid, cot, normed, act, step, ld, sloc, s, w_z, w_o, gg, dsk)


def scan_back_kernel(
    ci_ref,
    step_ref,
    l_ref,
    sig_ref,
    dy_ref,
    y_ref,
    inc_ref,
    sloc_ref,
    dsin_ref,
    cw_ref,
    cb_ref,
    rate_ref,
    dsk_ref,
    part_a,
    part_b,
    dxa_ref,
    dxb_ref,
    fix_ref,
    edge_ref,
    cgrad_ref,
    hgrad_ref,
    shard_a,
    shard_b,
    skip_ref,
    ds,
    xa,
    dsl,
    dact,
    xdt,
    xt,
    dr,
    e2,
    u_top,
    u_low,
    fs,
    vs,
    dyg,
    start,
    sib,
    out,
    got,
    swap_send,
    swap_recv,
    far_send,
    far_recv,
    send,
    recv,
    own_sems,
    *scratch,
    count,
    depth,
):
    piece = dy_ref.shape[0]
    chunks = piece // CL
    section = pl.program_id(0)
    states = Exchange(dsin_ref, sib, out, got, swap_send, swap_recv, far_send, far_recv, giver=1)
    here = Here(depth)
    plan = Plan(send, recv)
    reduce_items(here, plan, (part_a, part_b), (shard_a, shard_b), scratch, own_sems)
    even = states.c == 0
    one_if_even = jnp.where(even, 1.0, 0.0)
    weigh = lambda own, sibs: (jnp.where(even, 1.0, sibs), jnp.where(even, own, 1.0))

    @pl.when(section == 0)
    def _():
        cgrad_ref[...] = jnp.zeros_like(cgrad_ref)
        hgrad_ref[...] = jnp.zeros_like(hgrad_ref)
        skip_ref[...] = jnp.zeros_like(skip_ref)
        fill_expander(e2)
        here.greet_partners()
        states.begin(count)
        plan.run(0)
        states.hand_over(0, weigh)

    upper = jnp.logical_not(lower_mask(True))
    upper_one = jnp.where(upper, 1.0, 0.0)
    before_one = jnp.where(lower_mask(True), 1.0, 0.0)
    left, right = half_masks()
    dr[:, CL:] = jnp.zeros((XBC // LN, 8, LN), F32)
    steps = min(len(plan.segments) - 1, count * chunks)

    def chunk(i, carry):
        k = chunks - 1 - i
        base = pl.multiple_of(k * CL, CL)
        rows = pl.ds(base, CL)
        for n in range(steps):

            @pl.when(section * chunks + i == n)
            def _():
                plan.run(n + 1)

        for n in range(1, count):

            @pl.when((section == 0) & (i == n))
            def _():
                states.hand_over(n, weigh)

        step = step_ref[rows, :]
        ld = l_ref[rows, :]
        ldt = ld.T
        end = ld[CL - 1 :]
        prefix = jnp.zeros((8, LN), F32)
        for j in range(chunks - 1):
            prefix = prefix + jnp.where(j < k, 1.0, 0.0) * l_ref[j * CL + CL - 1 : j * CL + CL, :]
        before = expand(jnp.exp(prefix), e2)[0:1]
        start[...] = before * inc_ref[...] + sloc_ref[k].astype(F32)
        step_e = expand(step, e2)
        grow = expand(jnp.exp(ld), e2)
        tail = expand(jnp.exp(end - ld), e2)
        keep = grow[CL - 1 :]
        for j in range(XBC // LN):
            run = conv_running(ci_ref, j, base, cw_ref[:, lanes(j)], cb_ref[:, lanes(j)])
            s = sigmoid(run)
            a = run * s
            xa[:, lanes(j)] = a
            dsl[:, lanes(j)] = s + a * (1.0 - s)
            if j < DI // LN:
                xd = a * step_e[:, lanes(j)]
                xdt[:, lanes(j)] = xd
                xt[:, lanes(j)] = xd * tail[:, lanes(j)]

        @pl.when((i == 0) & (states.x == 1))
        def _():
            ds[...] = one_if_even * sib[section, 0:NS].astype(F32)

        @pl.when((i == 0) & (states.x == 0))
        def _():
            states.far(section).wait_recv()
            f = jnp.where(even, states.decay(sib, section), 1.0)
            ds[...] = f * got[section].astype(F32) + one_if_even * sib[section, 0:NS].astype(F32)

        b = xa[:, DI : DI + NS].astype(BF)
        c = xa[:, DI + NS :].astype(BF)
        scores = jnp.where(upper, nt(b, c), 0.0)
        dact[:, 0:DI] = nn(b, ds[...].astype(BF)) * tail
        dscores = jnp.zeros((CL, CL), F32)
        for j in range(DI // LN):
            dyf = dy_ref[rows, lanes(j)]
            dyb, dyl = halves(dyf)
            block = jnp.concatenate([dyb * left, dyb * right], axis=0)
            block_low = jnp.concatenate([dyl * left, dyl * right], axis=0)
            xdb, xdl = halves(xdt[:, lanes(j)])
            dmix = nt(jnp.concatenate([xdb, xdl], axis=1), jnp.concatenate([block, block], axis=1)) + nt(xdb, block_low)
            mixes = []
            for p, h in enumerate((2 * j, 2 * j + 1)):
                gap = jnp.minimum(ldt[h : h + 1, :] - ld[:, h : h + 1], 0.0)
                w = jnp.exp(gap)
                mixes.append((w * scores).astype(BF))
                dscores = dscores + dmix[:, lanes(p)] * w
            diag = nn(jnp.concatenate(mixes, axis=1), block)
            far = dact[:, lanes(j)]
            xdf = xdb.astype(F32)
            u_top[:, lanes(j)], u_low[:, lanes(j)] = halves(dyb.astype(F32) * y_ref[rows, lanes(j)] - xdf * diag)
            fs[:, lanes(j)] = (xdf * far).astype(BF)
            dxd = diag + far
            x = xa[:, lanes(j)]
            vs[:, lanes(j)] = (x * dxd).astype(BF)
            dact[:, lanes(j)] = dxd * step_e[:, lanes(j)] + dsk_ref[:, lanes(j)] * dyf
            skip_ref[:, lanes(j)] += jnp.sum((dyf * x).reshape(CL // 8, 8, LN), axis=0)
            dyg[:, lanes(j)] = dyf * grow[:, lanes(j)]
        e = e2[0:LN]
        const = jnp.sum((start[...] * ds[...]).reshape(NS // 8, 8, DI), axis=0) * keep
        c_top, c_low = halves(const)
        r_c = jnp.sum(nt(c_top, e) + nt(c_low, e), axis=0, keepdims=True)
        r_u = nt(u_top[...], e) + nt(u_low[...], e)
        r_f = nt(fs[...], e)
        r_v = nt(vs[...], e)
        db = three(nt, xt[...], ds[...])
        dc = three(nt, dyg[...], start[...])
        ds[...] = keep * ds[...] + tn(c, dyg[...].astype(BF))
        dsc = jnp.where(upper, dscores, 0.0).astype(BF)
        dact[:, DI : DI + NS] = db + nn(dsc, c)
        dact[:, DI + NS :] = dc + tn(dsc, b)
        da = exact_nn(upper_one, r_u) + exact_nn(before_one, r_f) + r_c
        dstep = r_v + rate_ref[...] * da
        ddt = dstep * sig_ref[rows, :]
        hgrad_ref[0:8] += jnp.sum(ddt.reshape(CL // 8, 8, LN), axis=0)
        hgrad_ref[8:16] += jnp.sum((da * step).reshape(CL // 8, 8, LN), axis=0)
        dxb_ref[rows, XBC - XA :] = ddt.astype(BF)
        for j in range(XBC // LN):
            g = dact[:, lanes(j)] * dsl[:, lanes(j)]
            dr[j, 0:CL] = g
            ci = ci_ref[j, pl.ds(base + 8, CL), :]
            total = g * cw_ref[DCONV - 1 : DCONV, lanes(j)]
            last = 8 * (DCONV - 1)
            cgrad_ref[last : last + 8, lanes(j)] += jnp.sum((g * ci).reshape(CL // 8, 8, LN), axis=0)
            for tap in range(DCONV - 1):
                later = DCONV - 1 - tap
                shifted = dr[j, later : later + CL, :]
                total = total + shifted * cw_ref[tap : tap + 1, lanes(j)]
                cgrad_ref[8 * tap : 8 * tap + 8, lanes(j)] += jnp.sum((shifted * ci).reshape(CL // 8, 8, LN), axis=0)
            cgrad_ref[32:40, lanes(j)] += jnp.sum(g.reshape(CL // 8, 8, LN), axis=0)
            if j < XA // LN:
                dxa_ref[rows, lanes(j)] = total.astype(BF)
            else:
                dxb_ref[rows, lanes(j - XA // LN)] = total.astype(BF)

            @pl.when(i == 0)
            def _():
                fix_ref[:, lanes(j)] = total[CL - 16 :]

            dr[j, CL:] = g[0:8]
        return carry

    lax.fori_loop(0, chunks, chunk, 0)
    for j in range(XBC // LN):
        edge_ref[:, lanes(j)] = dr[j, CL:]
        for tap in range(DCONV - 1):
            later = DCONV - 1 - tap
            part = dr[j, CL : CL + later] * ci_ref[j, 8 - later : 8]
            cgrad_ref[8 * tap : 8 * tap + 1, lanes(j)] += jnp.sum(part, axis=0, keepdims=True)

    @pl.when(section == count - 1)
    def _():
        top, low = halves(skip_ref[...])
        hgrad_ref[16:24] = nt(top, e2[0:LN]) + nt(low, e2[0:LN])
        states.end(count)
        plan.run_from(steps + 1)


def scan_back(count, depth, ci, step, ld, sig, dy, y, inc, sloc, dsin, cw, cb, rate, dsk, part_a, part_b):
    piece = dy.shape[1]
    chunks = piece // CL
    n = reduce_copies(depth.bit_length() - 1)
    sds = jax.ShapeDtypeStruct
    dma = pltpu.SemaphoreType.DMA
    return pl.pallas_call(
        partial(scan_back_kernel, count=count, depth=depth),
        grid=(count,),
        in_specs=[
            per((XBC // LN, piece + 8, LN)),
            per((piece, LN)),
            per((piece, LN)),
            per((piece, LN)),
            per((piece, DI)),
            per((piece, DI)),
            per((NS, DI)),
            per((chunks, NS, DI)),
            kept((count, SROWS, DI)),
            whole((DCONV, XBC)),
            whole((1, XBC)),
            whole((1, LN)),
            whole((1, DI)),
            ANY,
            ANY,
        ],
        out_specs=[
            per((piece, XA)),
            per((piece, XD - XA)),
            per((16, XBC)),
            per((8, XBC)),
            whole((40, XBC)),
            whole((24, LN)),
            whole(part_a.shape[4:]),
            whole(part_b.shape[4:]),
        ],
        out_shape=[
            sds((count, piece, XA), BF),
            sds((count, piece, XD - XA), BF),
            sds((count, 16, XBC), F32),
            sds((count, 8, XBC), F32),
            sds((40, XBC), F32),
            sds((24, LN), F32),
            sds(part_a.shape[4:], F32),
            sds(part_b.shape[4:], F32),
        ],
        scratch_shapes=[
            pltpu.VMEM((8, DI), F32),
            pltpu.VMEM((NS, DI), F32),
            pltpu.VMEM((CL, XBC), F32),
            pltpu.VMEM((CL, XBC), F32),
            pltpu.VMEM((CL, XBC), F32),
            pltpu.VMEM((CL, DI), F32),
            pltpu.VMEM((CL, DI), F32),
            pltpu.VMEM((XBC // LN, CL + 8, LN), F32),
            pltpu.VMEM((2 * LN, DI), BF),
            pltpu.VMEM((CL, DI), BF),
            pltpu.VMEM((CL, DI), BF),
            pltpu.VMEM((CL, DI), BF),
            pltpu.VMEM((CL, DI), BF),
            pltpu.VMEM((CL, DI), F32),
            pltpu.VMEM((NS, DI), F32),
        ]
        + exchange_scratch(count)
        + [dma((n,)), dma((n,)), dma((2,))]
        + reduce_scratch(depth, part_a.shape[-2:])
        + reduce_scratch(depth, part_b.shape[-2:]),
        compiler_params=pltpu.CompilerParams(vmem_limit_bytes=LIMIT, collective_id=3, has_side_effects=True),
        name="scan_back",
    )(ci, step, ld, sig, dy, y, inc, sloc, dsin, cw, cb, rate, dsk, part_a, part_b)


def patch_kernel(a_ref, b_ref, fix_ref, edge_ref, cw_ref, oa_ref, ob_ref, work):
    work[0:13] = fix_ref[0:13]
    for j in range(DCONV - 1):
        row = fix_ref[13 + j : 14 + j]
        for tap in range(j + 1):
            row = row + cw_ref[tap : tap + 1] * edge_ref[j - tap : j - tap + 1]
        work[13 + j : 14 + j] = row
    oa_ref[...] = work[:, :XA].astype(BF)
    ob_ref[:, : XBC - XA] = work[:, XA:].astype(BF)
    ob_ref[:, XBC - XA :] = b_ref[:, XBC - XA :]


def patch(dxa, dxb, fix, edge, cw):
    count, piece, _ = dxa.shape
    last = piece // 16 - 1
    tail = lambda n: pl.BlockSpec((None, 16, n), lambda i: (i, last, 0))
    return pl.pallas_call(
        patch_kernel,
        grid=(count,),
        in_specs=[tail(XA), tail(XD - XA), per((16, XBC)), per((8, XBC)), whole((DCONV, XBC))],
        out_specs=[tail(XA), tail(XD - XA)],
        out_shape=[jax.ShapeDtypeStruct(a.shape, BF) for a in (dxa, dxb)],
        scratch_shapes=[pltpu.VMEM((16, XBC), F32)],
        input_output_aliases={0: 0, 1: 1},
        name="patch",
    )(dxa, dxb, fix, edge, cw)


def input_grad_kernel(
    vlen_ref,
    x_ref,
    dbr_ref,
    g_ref,
    gn_ref,
    dz_ref,
    dxa_ref,
    dxb_ref,
    wo_ref,
    wz_ref,
    wa_ref,
    wb_ref,
    block_ref,
    out_ref,
    gain_ref,
    dn,
    *,
    first,
):
    piece = x_ref.shape[0]
    valid = vlen_ref[first + pl.program_id(0), 0] - lax.axis_index("seq") * piece
    live = lax.broadcasted_iota(jnp.int32, (piece, 1), 0) < valid

    @pl.when(pl.program_id(0) == 0)
    def _():
        gain_ref[...] = jnp.zeros_like(gain_ref)

    for j in range(D // 256):
        cols = slice(j * 256, (j + 1) * 256)
        branch = nn(gn_ref[...], wo_ref[:, cols])
        block_ref[:, cols] = jnp.where(live, x_ref[:, cols].astype(F32) + branch, 0.0).astype(BF)
        dn[:, cols] = (
            nt(dz_ref[...], wz_ref[cols, :]) + nt(dxa_ref[...], wa_ref[cols, :]) + nt(dxb_ref[...], wb_ref[cols, :])
        )

    def rows_of(i, c):
        rows = pl.ds(pl.multiple_of(i * 64, 64), 64)
        x = x_ref[rows, :].astype(F32)
        d = dn[rows, :]
        r = lax.rsqrt(jnp.mean(x * x, axis=-1, keepdims=True) + EPSILON)
        v = x * r
        gain_ref[...] += jnp.sum((d * v).reshape(8, 8, D), axis=0)
        dv = d * g_ref[...]
        q = jnp.mean(dv * v, axis=-1, keepdims=True)
        out_ref[rows, :] = (dbr_ref[rows, :].astype(F32) + r * (dv - v * q)).astype(BF)
        return c

    lax.fori_loop(0, piece // 64, rows_of, 0)


def input_grad(first, count, valid, tokens, dbr, gain, gn, dz, dxa, dxb, w_o, w_z, wa, wb):
    piece = tokens.shape[1]
    sds = jax.ShapeDtypeStruct
    return pl.pallas_call(
        partial(input_grad_kernel, first=first),
        grid=(count,),
        in_specs=[
            SMEM,
            per((piece, D), first),
            per((piece, D)),
            whole((1, D)),
            per((piece, DI)),
            per((piece, DI)),
            per((piece, XA)),
            per((piece, XD - XA)),
            kept((DI, D)),
            kept((D, DI)),
            kept((D, XA)),
            kept((D, XD - XA)),
        ],
        out_specs=[per((piece, D)), per((piece, D)), whole((8, D))],
        out_shape=[sds((count, piece, D), BF), sds((count, piece, D), BF), sds((8, D), F32)],
        scratch_shapes=[pltpu.VMEM((piece, D), F32)],
        compiler_params=pltpu.CompilerParams(vmem_limit_bytes=LIMIT),
        name="input_grad",
    )(valid, tokens, dbr, gain, gn, dz, dxa, dxb, w_o, w_z, wa, wb)


def assemble_kernel(z, a, b, o, t, win, wo, g0, g1, g2, g3, h0, h1, h2):
    win[:, 0:DI] = z[...]
    win[:, DI : DI + XA] = a[...]
    win[:, DI + XA :] = b[:, : PROJ - DI - XA]
    wo[...] = o[...]
    g0[...] = t[0:1, : g0.shape[1]]
    g1[...] = t[1:2, : g1.shape[1]]
    g2[...] = t[2:3, : g2.shape[1]]
    g3[...] = t[3 : 3 + DCONV, : g3.shape[1]]
    last = t[7:8, :]
    h0[...] = last[:, 0:NH]
    h1[...] = last[:, NH : 2 * NH]
    h2[...] = last[:, 2 * NH : 3 * NH]


def assemble(z, a, b, o, t, n0, n1, n2):
    shapes = [(z.shape[0], PROJ), o.shape, (1, n0), (1, n1), (1, n2), (DCONV, n2), (1, NH), (1, NH), (1, NH)]
    return pl.pallas_call(
        assemble_kernel,
        in_specs=[IN_VMEM] * 5,
        out_specs=[IN_VMEM] * 9,
        out_shape=[jax.ShapeDtypeStruct(v, F32) for v in shapes],
        name="assemble",
    )(z, a, b, o, t)


def pass_on(block, axis, distance):
    devices = range(lax.axis_size(axis))
    route = [(i - distance, i) for i in devices if i - distance in devices]
    return lax.ppermute(block, axis, route)


def contract_rows(left, right):
    return lax.dot_general(left, right, (((0, 1), (0, 1)), ((), ())), preferred_element_type=F32)


def local(
    tokens,
    norm_gain,
    w_in,
    conv_weight,
    conv_bias,
    dt_bias,
    a_log,
    d_skip,
    gated_gain,
    w_out,
    lengths,
    cotangent,
):
    tokens = tokens[:, 0]
    cot = cotangent[:, 0]
    batches, piece, _ = tokens.shape
    rows = w_in.shape[0]

    depth = lax.axis_size("dp") // 2
    n0, n1, n2 = norm_gain.shape[0], gated_gain.shape[0], conv_bias.shape[0]
    wa, wb, halo, gain, gg, cb, cw, dtb, rate, dsk = gather(
        w_in,
        norm_gain[None],
        gated_gain[None],
        conv_bias[None],
        conv_weight,
        dt_bias[None],
        a_log[None],
        d_skip[None],
        tokens,
        depth,
    )
    wa, wb = wa.reshape(D, XA), wb.reshape(D, XD - XA)

    first, count = 0, batches
    normed, ci, act, step, ld, sig, sloc, s, w_z, w_o = project(
        first, count, depth, lengths, tokens, halo, gain, wa, wb, cw, cb, dtb, rate, w_in, w_out
    )
    w_z, w_o = w_z.reshape(D, DI), w_o.reshape(DI, D)
    gn, dbr, dz, dy, y, inc, dsin, ggrad = mix(
        first, count, lengths, cot, normed, act, step, ld, sloc, s, w_z, w_o, gg, dsk
    )
    lead = (depth, 2, 2, 2)
    grad_wo = contract_rows(gn, dbr).astype(BF).reshape(lead + (n1, D))
    grad_wz = contract_rows(normed, dz).astype(BF).reshape(lead + (rows, DI))
    dxa, dxb, fix, edge, cgrad, hgrad, shard_wo, shard_wz = scan_back(
        count, depth, ci, step, ld, sig, dy, y, inc, sloc, dsin, cw, cb, rate, dsk, grad_wo, grad_wz
    )
    dxa, dxb = patch(dxa, dxb, fix, pass_on(edge, "seq", -1), cw)
    out, tgrad, gain_grad = input_grad(first, count, lengths, tokens, dbr, gain, gn, dz, dxa, dxb, w_o, w_z, wa, wb)
    grad_wa = contract_rows(normed, dxa).astype(BF).reshape(lead + (rows, XA))
    grad_wb = contract_rows(normed, dxb).astype(BF).reshape(lead + (rows, XD - XA))

    shard_wa, shard_wb, total = reduce(grad_wa, grad_wb, gain_grad, ggrad, cgrad, hgrad, rate, depth)
    shard_win, shard_wo, g0, g1, g2, g3, h0, h1, h2 = assemble(shard_wz, shard_wa, shard_wb, shard_wo, total, n0, n1, n2)
    return (
        out[:, None],
        tgrad[:, None],
        g0.reshape(n0),
        shard_win,
        g3,
        g2.reshape(n2),
        h0.reshape(NH),
        h1.reshape(NH),
        h2.reshape(NH),
        g1.reshape(n1),
        shard_wo,
    )


def solution(mesh):
    shard = P(("dp", "seq"))
    row_shard = P(("dp", "seq"), None)
    col_shard = P(None, ("dp", "seq"))
    acts = P(None, "dp", "seq", None)
    return jax.shard_map(
        local,
        mesh=mesh,
        in_specs=(
            acts,
            shard,
            row_shard,
            col_shard,
            shard,
            P(),
            P(),
            P(),
            shard,
            row_shard,
            P(None, "dp"),
            acts,
        ),
        out_specs=(
            acts,
            acts,
            shard,
            row_shard,
            col_shard,
            shard,
            P(),
            P(),
            P(),
            shard,
            row_shard,
        ),
        check_vma=False,
    )
```
